128 devices in a mesh: fsdp: 32 (over z, y, x_hi), sp: 4 (over x_lo, core).
Axes of the slice: x: 4 (x_hi: 2, x_lo: 2; x = x_hi * 2 + x_lo), y: 4, z: 4, core: 2. Of those that a mesh axis runs over, the one named last changes fastest.
Arguments:
- tokens: bfloat16 [32, 512, 1536], P('fsdp', 'sp'), may hold values from -6 to 6
- modulation: float32 [32, 1, 6, 1536], P('fsdp'), may hold values from -4 to 4
- w_qkv: bfloat16 [1, 1536, 3, 1536], P(None, 'fsdp', None, 'sp'), may hold values from -0.15625 to 0.15625
- w_out: bfloat16 [1, 1536, 1536], P(None, 'sp', 'fsdp'), may hold values from -0.15625 to 0.15625
- w_in: bfloat16 [1, 1536, 6144], P(None, 'fsdp', 'sp'), may hold values from -0.15625 to 0.15625
- w_back: bfloat16 [1, 6144, 1536], P(None, 'sp', 'fsdp'), may hold values from -0.078125 to 0.078125
- out_grad: bfloat16 [32, 512, 1536], P('fsdp', 'sp'), may hold values from -6 to 6
Outputs:
- final_out: bfloat16 [32, 512, 1536], P('fsdp', 'sp')
- input_grad: float32 [32, 512, 1536], P('fsdp', 'sp')
- grad_qkv: float32 [1, 1536, 3, 1536], P(None, 'fsdp', None, 'sp')
- grad_out: float32 [1, 1536, 1536], P(None, 'sp', 'fsdp')
- grad_in: float32 [1, 1536, 6144], P(None, 'fsdp', 'sp')
- grad_back: float32 [1, 6144, 1536], P(None, 'sp', 'fsdp')
The draws below stay inside these ranges and needn't reach their ends.
All inputs are finite; a program needn't handle non-finite values.
Results may differ from the reference program's by a relative error of at most 0.03.
Values may be sent and summed in bfloat16 or wider, within the bound.
No kernel may reach another device: no remote copies, remote signals or barrier semaphores. Data moves between devices by JAX's collectives and lax.ppermute only.
A program may use at most 128 MiB of HBM per device.

```python
import math
import jax
import jax.numpy as jnp
from jax import lax

D = 1536
HEAD_DIM = 128
FF = 6144
LAYERS = 1
SEQ = 512
BATCH = 32
N_FSDP = 32


def block_scale(rng, dims, shards, smallest, top_value):
    def one(axis_at, parts):
        heights = jax.random.uniform(jax.random.fold_in(jax.random.fold_in(rng, 6), axis_at), (parts,), jnp.float32, smallest / len(shards), top_value / len(shards))
        return jnp.repeat(jnp.exp(heights), dims[axis_at] // parts).reshape((-1,) + (1,) * (len(dims) - axis_at - 1))

    gain = one(*shards[0])
    for cut in shards[1:]:
        gain = gain * one(*cut)
    return gain


def bell_draw(stream_key, shape, spread, limit, cuts=(), dtype=jnp.bfloat16):
    drawn = spread * jax.random.normal(stream_key, shape, jnp.float32)
    if cuts:
        drawn = drawn * block_scale(stream_key, shape, cuts, -0.22, 0.18)
    return jnp.clip(drawn, -limit, limit).astype(dtype)


def setup_inputs(seed: int = 0) -> dict:
    keys = jax.random.split(jax.random.key(seed), 8)
    tokens = bell_draw(keys[0], (BATCH, SEQ, D), 1.0, 6.0, ((0, 32), (1, 4)))
    modulation = bell_draw(keys[1], (BATCH, LAYERS, 6, D), 1.0, 4.0, ((0, 32),), jnp.float32)
    w_qkv = bell_draw(keys[2], (LAYERS, D, 3, D), D ** -0.5, 0.15625, ((1, 32), (3, 4)))
    w_out = bell_draw(keys[3], (LAYERS, D, D), D ** -0.5, 0.15625, ((1, 4), (2, 32)))
    w_in = bell_draw(keys[4], (LAYERS, D, FF), D ** -0.5, 0.15625, ((1, 32), (2, 4)))
    w_back = bell_draw(keys[5], (LAYERS, FF, D), FF ** -0.5, 0.078125, ((1, 4), (2, 32)))
    out_grad = bell_draw(keys[6], (BATCH, SEQ, D), 1.0, 6.0, ((0, 32), (1, 4)))
    return dict(tokens=tokens, modulation=modulation, w_qkv=w_qkv, w_out=w_out, w_in=w_in, w_back=w_back, out_grad=out_grad)


ln_eps = 1e-06
temper = 2.5
block_limit = 512

def normalize(stream):
    mean_part = lax.optimization_barrier(jnp.mean(stream, axis=-1, keepdims=True))
    centred = stream - mean_part
    rstd = lax.rsqrt(lax.optimization_barrier(jnp.mean(centred * centred, axis=-1, keepdims=True)) + ln_eps)
    return (centred * rstd, rstd)

def norm_back(normed, rstd, incoming):
    first = lax.optimization_barrier(jnp.mean(incoming, axis=-1, keepdims=True))
    second = lax.optimization_barrier(jnp.mean(incoming * normed, axis=-1, keepdims=True))
    return rstd * (incoming - first - normed * second)

def gelu_tanh(hidden):
    return jax.nn.gelu(hidden, approximate=True)

def project(left, weight):
    flat_rows = left.reshape(-1, left.shape[-1])
    result = jnp.dot(flat_rows, weight, preferred_element_type=jnp.float32)
    return result.reshape(left.shape[:-1] + (weight.shape[1],))

def project_back(left, weight):
    flat_rows = left.reshape(-1, left.shape[-1])
    result = lax.dot_general(flat_rows, weight, (((1,), (1,)), ((), ())), preferred_element_type=jnp.float32)
    return result.reshape(left.shape[:-1] + (weight.shape[0],))

def group_grad(left, right, grad_scale):
    width_left = left.shape[-1]
    width_right = right.shape[-1]
    left_groups = left.reshape(N_FSDP, -1, width_left)
    right_groups = right.reshape(N_FSDP, -1, width_right)

    def add_group(total, pair):
        left_part, right_part = pair
        term = lax.dot_general(left_part, right_part, (((0,), (0,)), ((), ())), preferred_element_type=jnp.float32) * grad_scale
        rounded = lax.optimization_barrier(term.astype(jnp.bfloat16))
        return (total + rounded.astype(jnp.float32), None)
    total, unused = lax.scan(add_group, jnp.zeros((width_left, width_right), jnp.float32), (left_groups, right_groups))
    return total

def split_heads(packed, head_count):
    return packed.reshape(packed.shape[:-1] + (head_count, packed.shape[-1] // head_count))

def heads_major(tensor):
    videos, seq_len, head_count, head_width = tensor.shape
    return tensor.transpose(0, 2, 1, 3).reshape(videos * head_count, seq_len, head_width)

def heads_minor(tensor, videos):
    merged, seq_len, head_width = tensor.shape
    return tensor.reshape(videos, merged // videos, seq_len, head_width).transpose(0, 2, 1, 3)

def attend_head(triple):
    queries, key_rows, values = triple
    seq_len, head_width = queries.shape
    block_size = min(block_limit, seq_len)
    score_factor = temper / math.sqrt(head_width)
    values_wide = values.astype(jnp.float32)

    def one_block(query_rows):
        scores = jnp.dot(query_rows, key_rows.T, preferred_element_type=jnp.float32) * score_factor
        softmaxed = jax.nn.softmax(scores, axis=-1)
        return jnp.dot(softmaxed, values_wide, precision=lax.Precision.HIGHEST).astype(jnp.bfloat16)
    attended = lax.map(one_block, queries.reshape(seq_len // block_size, block_size, head_width))
    return attended.reshape(seq_len, head_width)

def attend_back(quadruple):
    queries, key_rows, values, upstream = quadruple
    seq_len, head_width = queries.shape
    block_size = min(block_limit, seq_len)
    score_factor = temper / math.sqrt(head_width)
    keys_wide = key_rows.astype(jnp.float32)

    def one_block(running, block_pair):
        query_rows, grad_rows = block_pair
        scores = jnp.dot(query_rows, key_rows.T, preferred_element_type=jnp.float32) * score_factor
        softmaxed = jax.nn.softmax(scores, axis=-1)
        dprobs = jnp.dot(grad_rows, values.T, preferred_element_type=jnp.float32)
        dscores = softmaxed * (dprobs - lax.optimization_barrier(jnp.sum(softmaxed * dprobs, axis=-1, keepdims=True))) * score_factor
        dquery = jnp.dot(dscores, keys_wide, precision=lax.Precision.HIGHEST)
        grad_keys = running[0] + jnp.dot(dscores.T, query_rows.astype(jnp.float32), precision=lax.Precision.HIGHEST)
        dvalues = running[1] + jnp.dot(softmaxed.T, grad_rows.astype(jnp.float32), precision=lax.Precision.HIGHEST)
        return ((grad_keys, dvalues), dquery)
    zero_rows = jnp.zeros((seq_len, head_width), jnp.float32)
    count = seq_len // block_size
    blocks = (queries.reshape(count, block_size, head_width), upstream.reshape(count, block_size, head_width))
    (grad_keys, dvalues), dquery = lax.scan(one_block, (zero_rows, zero_rows), blocks)
    return (dquery.reshape(seq_len, head_width).astype(jnp.bfloat16), grad_keys.astype(jnp.bfloat16), dvalues.astype(jnp.bfloat16))

def attend_all(queries, key_rows, values):
    attended = lax.map(attend_head, (heads_major(queries), heads_major(key_rows), heads_major(values)))
    return heads_minor(attended, queries.shape[0])

def attend_all_back(queries, key_rows, values, upstream):
    grad_heads = lax.map(attend_back, (heads_major(queries), heads_major(key_rows), heads_major(values), heads_major(upstream)))
    return tuple((heads_minor(grad_piece, queries.shape[0]) for grad_piece in grad_heads))

def reference(tokens, modulation, w_qkv, w_out, w_in, w_back, out_grad):
    videos, seq_len, model_width = tokens.shape
    layers = w_qkv.shape[0]
    head_count = model_width // HEAD_DIM
    grad_scale = 1.0 / math.sqrt(videos * seq_len)
    stream = tokens.astype(jnp.float32)
    stored = []
    for layer_index in range(layers):
        layer_mod = modulation[:, layer_index][:, :, None, :]
        joint = w_qkv[layer_index].reshape(model_width, 3 * model_width)
        normed_first, rstd_first = normalize(stream)
        input_first = (normed_first * (1.0 + layer_mod[:, 1]) + layer_mod[:, 0]).astype(jnp.bfloat16)
        packed = project(input_first, joint).astype(jnp.bfloat16)
        queries = split_heads(packed[..., :model_width], head_count)
        key_rows = split_heads(packed[..., model_width:2 * model_width], head_count)
        values = split_heads(packed[..., 2 * model_width:], head_count)
        attended = attend_all(queries, key_rows, values).reshape(videos, seq_len, model_width)
        middle = stream + layer_mod[:, 2] * project(attended, w_out[layer_index])
        normed_second, rstd_second = normalize(middle)
        input_second = (normed_second * (1.0 + layer_mod[:, 4]) + layer_mod[:, 3]).astype(jnp.bfloat16)
        hidden = project(input_second, w_in[layer_index])
        activated = gelu_tanh(hidden).astype(jnp.bfloat16)
        stream = middle + layer_mod[:, 5] * project(activated, w_back[layer_index])
        stored.append((normed_first, rstd_first, input_first, queries, key_rows, values, attended, normed_second, rstd_second, input_second, hidden, activated))
    final_out = stream.astype(jnp.bfloat16)
    stream_grad = out_grad.astype(jnp.float32)
    results = [None] * layers
    for layer_index in range(layers - 1, -1, -1):
        normed_first, rstd_first, input_first, queries, key_rows, values, attended, normed_second, rstd_second, input_second, hidden, activated = stored[layer_index]
        layer_mod = modulation[:, layer_index][:, :, None, :]
        joint = w_qkv[layer_index].reshape(model_width, 3 * model_width)
        down_grad = (layer_mod[:, 5] * stream_grad).astype(jnp.bfloat16)
        back_hidden = project_back(down_grad, w_back[layer_index])
        unused, pullback = jax.vjp(gelu_tanh, hidden)
        up_grad = pullback(back_hidden)[0].astype(jnp.bfloat16)
        back_second = project_back(up_grad, w_in[layer_index])
        stream_grad = stream_grad + norm_back(normed_second, rstd_second, back_second * (1.0 + layer_mod[:, 4]))
        attn_grad = (layer_mod[:, 2] * stream_grad).astype(jnp.bfloat16)
        mixed_grad = split_heads(project_back(attn_grad, w_out[layer_index]).astype(jnp.bfloat16), head_count)
        grad_query, grad_keys, grad_values = attend_all_back(queries, key_rows, values, mixed_grad)
        packed_grad = jnp.concatenate([grad_query.reshape(videos, seq_len, model_width), grad_keys.reshape(videos, seq_len, model_width), grad_values.reshape(videos, seq_len, model_width)], axis=-1)
        back_first = project_back(packed_grad, joint)
        stream_grad = stream_grad + norm_back(normed_first, rstd_first, back_first * (1.0 + layer_mod[:, 1]))
        results[layer_index] = (group_grad(input_first, packed_grad, grad_scale).reshape(model_width, 3, model_width), group_grad(attended, attn_grad, grad_scale), group_grad(input_second, up_grad, grad_scale), group_grad(activated, down_grad, grad_scale))
    grad_qkv = jnp.stack([results[index][0] for index in range(layers)])
    grad_out = jnp.stack([results[index][1] for index in range(layers)])
    grad_in = jnp.stack([results[index][2] for index in range(layers)])
    grad_back = jnp.stack([results[index][3] for index in range(layers)])
    return (final_out, stream_grad, grad_qkv, grad_out, grad_in, grad_back)
```

```python
import math

import jax
import jax.numpy as jnp
from jax import lax
from jax.experimental import pallas as pl
from jax.experimental.pallas import tpu as pltpu
from jax.sharding import Mesh
from jax.sharding import PartitionSpec as P

HEAD_DIM = 128
FSDP = ("fsdp_zy", "fsdp_x")
SP = ("sp_x", "sp_core")
SWAP = ((0, 1), (1, 0))

ln_eps = 1e-06
temper = 2.5
BF = jnp.bfloat16
F32 = jnp.float32


def normalize(stream):
    mean_part = jnp.mean(stream, axis=-1, keepdims=True)
    centred = stream - mean_part
    rstd = lax.rsqrt(jnp.mean(centred * centred, axis=-1, keepdims=True) + ln_eps)
    return (centred * rstd, rstd)


def norm_back(normed, rstd, incoming):
    first = jnp.mean(incoming, axis=-1, keepdims=True)
    second = jnp.mean(incoming * normed, axis=-1, keepdims=True)
    return rstd * (incoming - first - normed * second)


def gelu_tanh(hidden):
    return jax.nn.gelu(hidden, approximate=True)


def dot_nn(left, right):
    return jnp.dot(left, right, preferred_element_type=F32)


def dot_nt(left, right):
    return lax.dot_general(left, right, (((1,), (1,)), ((), ())), preferred_element_type=F32)


def dot_tn(left, right):
    return lax.dot_general(left, right, (((0,), (0,)), ((), ())), preferred_element_type=F32)


def swap(value, axis):
    return lax.ppermute(value, axis, SWAP)


def near_rows(own):
    return jnp.concatenate([own, swap(own, "sp_core")], axis=0)


def far_rows(own):
    across = swap(own, "sp_x")
    return jnp.concatenate([across, swap(across, "sp_core")], axis=0)


def core_sum(part):
    rows = part.shape[0] // 2
    given = swap(part[rows:].astype(BF), "sp_core")
    return part[:rows] + given.astype(F32)


def far_sum(part):
    return swap(core_sum(part).astype(BF), "sp_x").astype(F32)


def ordered(own, other, axis):
    first = jnp.concatenate([own, other], axis=0)
    second = jnp.concatenate([other, own], axis=0)
    return jnp.where(lax.axis_index(axis) == 0, first, second)


def attend_kernel(q_ref, k_ref, v_ref, o_ref):
    factor = temper / math.sqrt(HEAD_DIM)
    scores = dot_nt(q_ref[...], k_ref[...]) * factor
    lifted = jnp.exp(scores - jnp.max(scores, axis=-1, keepdims=True))
    probs = lifted / jnp.sum(lifted, axis=-1, keepdims=True)
    o_ref[...] = dot_nn(probs.astype(BF), v_ref[...]).astype(BF)


def attend(packed):
    rows, width = packed.shape
    heads = width // (3 * HEAD_DIM)
    block = (rows, HEAD_DIM)
    return pl.pallas_call(
        attend_kernel,
        grid=(heads,),
        in_specs=[
            pl.BlockSpec(block, lambda h: (0, h)),
            pl.BlockSpec(block, lambda h: (0, heads + h)),
            pl.BlockSpec(block, lambda h: (0, 2 * heads + h)),
        ],
        out_specs=pl.BlockSpec(block, lambda h: (0, h)),
        out_shape=jax.ShapeDtypeStruct((rows, heads * HEAD_DIM), BF),
        name="attend",
    )(packed, packed, packed)


def attend_back_kernel(q_ref, k_ref, v_ref, d_ref, o_ref):
    heads = pl.num_programs(0)
    head = pl.program_id(0)
    factor = temper / math.sqrt(HEAD_DIM)
    queries, keys, values, upstream = q_ref[...], k_ref[...], v_ref[...], d_ref[...]
    scores = dot_nt(queries, keys) * factor
    lifted = jnp.exp(scores - jnp.max(scores, axis=-1, keepdims=True))
    probs = lifted / jnp.sum(lifted, axis=-1, keepdims=True)
    dprobs = dot_nt(upstream, values)
    inner = jnp.sum(probs * dprobs, axis=-1, keepdims=True)
    dscores = (probs * (dprobs - inner) * factor).astype(BF)
    probs = probs.astype(BF)

    def put(place, value):
        at = pl.multiple_of((place * heads + head) * HEAD_DIM, HEAD_DIM)
        o_ref[:, pl.ds(at, HEAD_DIM)] = value.astype(BF)

    put(0, dot_nn(dscores, keys))
    put(1, dot_tn(dscores, queries))
    put(2, dot_tn(probs, upstream))


def attend_back(packed, upstream):
    rows, width = packed.shape
    heads = width // (3 * HEAD_DIM)
    block = (rows, HEAD_DIM)
    return pl.pallas_call(
        attend_back_kernel,
        grid=(heads,),
        in_specs=[
            pl.BlockSpec(block, lambda h: (0, h)),
            pl.BlockSpec(block, lambda h: (0, heads + h)),
            pl.BlockSpec(block, lambda h: (0, 2 * heads + h)),
            pl.BlockSpec(block, lambda h: (0, h)),
        ],
        out_specs=pl.BlockSpec((rows, width), lambda h: (0, 0)),
        out_shape=jax.ShapeDtypeStruct((rows, width), BF),
        name="attend_back",
    )(packed, packed, packed, upstream)


def scatter_sum(term):
    rows = lax.psum_scatter(term, "fsdp_zy", scatter_dimension=0, tiled=True)
    half = rows.shape[0] // 2
    low, high = rows[:half], rows[half:]
    at_low = lax.axis_index("fsdp_x") == 0
    given = swap(jnp.where(at_low, high, low), "fsdp_x")
    return jnp.where(at_low, low, high).astype(F32) + given.astype(F32)


def block_pass(tokens, layer_mod, w_qkv, w_out, w_in, w_back, out_grad, grad_scale):
    qkv_width, out_width, in_width = w_qkv.shape[1], w_out.shape[0], w_in.shape[1]
    own_weights = jnp.concatenate([w_qkv, w_out.T, w_in, w_back.T], axis=1)
    pair = ordered(own_weights, swap(own_weights, "fsdp_x"), "fsdp_x")
    cut = qkv_width + out_width
    attn_weights = lax.all_gather(pair[:, :cut], "fsdp_zy", axis=0, tiled=True)
    ffn_weights = lax.all_gather(pair[:, cut:], "fsdp_zy", axis=0, tiled=True)
    joint, out_rows = attn_weights[:, :qkv_width], attn_weights[:, qkv_width:]
    in_rows, back_rows = ffn_weights[:, :in_width], ffn_weights[:, in_width:]

    stream = tokens.astype(F32)
    normed_first, rstd_first = normalize(stream)
    input_first = (normed_first * (1.0 + layer_mod[1]) + layer_mod[0]).astype(BF)
    first_rows = jnp.concatenate([near_rows(input_first), far_rows(input_first)], axis=0)
    packed = dot_nn(first_rows, joint).astype(BF)
    attended = attend(packed)
    half = attended.shape[0] // 2
    attn_part = far_sum(dot_nt(attended[half:], out_rows))
    attn_part = attn_part + core_sum(dot_nt(attended[:half], out_rows))
    middle = stream + layer_mod[2] * attn_part
    normed_second, rstd_second = normalize(middle)
    input_second = (normed_second * (1.0 + layer_mod[4]) + layer_mod[3]).astype(BF)
    second_rows = jnp.concatenate([near_rows(input_second), far_rows(input_second)], axis=0)
    hidden = dot_nn(second_rows, in_rows)
    activated, pullback = jax.vjp(gelu_tanh, hidden)
    activated = activated.astype(BF)
    ffn_part = far_sum(dot_nt(activated[half:], back_rows))
    ffn_part = ffn_part + core_sum(dot_nt(activated[:half], back_rows))
    final_out = (middle + layer_mod[5] * ffn_part).astype(BF)

    stream_grad = out_grad.astype(F32)
    down_grad = (layer_mod[5] * stream_grad).astype(BF)
    down_rows = jnp.concatenate([near_rows(down_grad), far_rows(down_grad)], axis=0)
    up_grad = pullback(dot_nn(down_rows, back_rows))[0].astype(BF)
    back_second = far_sum(dot_nt(up_grad[half:], in_rows))
    back_second = back_second + core_sum(dot_nt(up_grad[:half], in_rows))
    term_back = (dot_tn(down_rows, activated) * grad_scale).astype(BF)
    term_in = (dot_tn(second_rows, up_grad) * grad_scale).astype(BF)
    sum_ffn = scatter_sum(jnp.concatenate([term_in, term_back], axis=1))
    stream_grad = stream_grad + norm_back(
        normed_second, rstd_second, back_second * (1.0 + layer_mod[4])
    )
    attn_grad = (layer_mod[2] * stream_grad).astype(BF)
    attn_rows = jnp.concatenate([near_rows(attn_grad), far_rows(attn_grad)], axis=0)
    mixed_grad = dot_nn(attn_rows, out_rows).astype(BF)
    packed_grad = attend_back(packed, mixed_grad)
    term_out = (dot_tn(attn_rows, attended) * grad_scale).astype(BF)
    term_qkv = (dot_tn(first_rows, packed_grad) * grad_scale).astype(BF)
    sum_attn = scatter_sum(jnp.concatenate([term_qkv, term_out], axis=1))
    back_first = far_sum(dot_nt(packed_grad[half:], joint))
    back_first = back_first + core_sum(dot_nt(packed_grad[:half], joint))
    stream_grad = stream_grad + norm_back(
        normed_first, rstd_first, back_first * (1.0 + layer_mod[1])
    )
    return (
        final_out,
        stream_grad,
        sum_attn[:, :qkv_width],
        sum_attn[:, qkv_width:].T,
        sum_ffn[:, :in_width],
        sum_ffn[:, in_width:].T,
    )


def body(tokens, modulation, w_qkv, w_out, w_in, w_back, out_grad):
    local_seq = tokens.shape[1]
    own_width = w_qkv.shape[3]
    grad_scale = 1.0 / math.sqrt(local_seq * lax.axis_size(FSDP) * lax.axis_size(SP))
    final_out, input_grad, grad_qkv, grad_out, grad_in, grad_back = block_pass(
        tokens[0],
        modulation[0, 0],
        w_qkv[0].reshape(-1, 3 * own_width),
        w_out[0],
        w_in[0],
        w_back[0],
        out_grad[0],
        grad_scale,
    )
    return (
        final_out[None],
        input_grad[None],
        grad_qkv.reshape(1, -1, 3, own_width),
        grad_out[None],
        grad_in[None],
        grad_back[None],
    )


def solution(mesh):
    torus = Mesh(
        mesh.devices.reshape(mesh.shape["fsdp"] // 2, 2, 2, 2),
        ("fsdp_zy", "fsdp_x", "sp_x", "sp_core"),
    )
    return jax.shard_map(
        body,
        mesh=torus,
        in_specs=(
            P(FSDP, SP, None),
            P(FSDP, None, None, None),
            P(None, FSDP, None, SP),
            P(None, SP, FSDP),
            P(None, FSDP, SP),
            P(None, SP, FSDP),
            P(FSDP, SP, None),
        ),
        out_specs=(
            P(FSDP, SP, None),
            P(FSDP, SP, None),
            P(None, FSDP, None, SP),
            P(None, SP, FSDP),
            P(None, FSDP, SP),
            P(None, SP, FSDP),
        ),
        check_vma=False,
    )
```

```python
import math

import jax
import jax.numpy as jnp
from jax import lax
from jax.experimental import pallas as pl
from jax.experimental.pallas import tpu as pltpu
from jax.sharding import Mesh
from jax.sharding import PartitionSpec as P

HEAD_DIM = 128
ZY = ("fsdp_z", "fsdp_y")
FSDP = (*ZY, "fsdp_x")
SP = ("sp_x", "sp_core")
SWAP = ((0, 1), (1, 0))
GRID = (*ZY, "sp_core")
PLACES = 16
FLIPS = (1, 4, 3, 12)
STEPS = len(FLIPS)

ln_eps = 1e-06
temper = 2.5
BF = jnp.bfloat16
F32 = jnp.float32


def normalize(stream):
    mean_part = jnp.mean(stream, axis=-1, keepdims=True)
    centred = stream - mean_part
    rstd = lax.rsqrt(jnp.mean(centred * centred, axis=-1, keepdims=True) + ln_eps)
    return (centred * rstd, rstd)


def norm_back(normed, rstd, incoming):
    first = jnp.mean(incoming, axis=-1, keepdims=True)
    second = jnp.mean(incoming * normed, axis=-1, keepdims=True)
    return rstd * (incoming - first - normed * second)


def gelu_tanh(hidden):
    return jax.nn.gelu(hidden, approximate=True)


def dot_nn(left, right):
    return jnp.dot(left, right, preferred_element_type=F32)


def dot_nt(left, right):
    return lax.dot_general(left, right, (((1,), (1,)), ((), ())), preferred_element_type=F32)


def dot_tn(left, right):
    return lax.dot_general(left, right, (((0,), (0,)), ((), ())), preferred_element_type=F32)


def swap(value, axis):
    return lax.ppermute(value, axis, SWAP)


def near_rows(own):
    return jnp.concatenate([own, swap(own, "sp_core")], axis=0)


def far_rows(own):
    across = swap(own, "sp_x")
    return jnp.concatenate([across, swap(across, "sp_core")], axis=0)


def core_sum(part):
    rows = part.shape[0] // 2
    given = swap(part[rows:].astype(BF), "sp_core")
    return part[:rows] + given.astype(F32)


def far_sum(part):
    return swap(core_sum(part).astype(BF), "sp_x").astype(F32)


def ordered(own, other, axis):
    first = jnp.concatenate([own, other], axis=0)
    second = jnp.concatenate([other, own], axis=0)
    return jnp.where(lax.axis_index(axis) == 0, first, second)


def hop(value, stream, step):
    pairs = []
    for place in range(PLACES):
        for core in range(2):
            flip = FLIPS[(2 * stream + core + step) % STEPS]
            pairs.append((2 * place + core, 2 * (place ^ flip) + core))
    return lax.ppermute(value, GRID, pairs)


def place_of(where_ref, stream):
    turn = 2 * stream + where_ref[1]
    flips = []
    for step in range(STEPS):
        link = lax.rem(turn + step, STEPS)
        low = jnp.where(link == 0, FLIPS[0], FLIPS[1])
        high = jnp.where(link == 2, FLIPS[2], FLIPS[3])
        flips.append(jnp.where(link < 2, low, high))

    def at(rank):
        place = where_ref[0]
        for step in range(STEPS):
            if rank >> step & 1:
                place = place ^ flips[step]
        return place

    return at


def local_call(kernel, name, outs, where, *arrays):
    return pl.pallas_call(
        kernel,
        in_specs=[pl.BlockSpec(memory_space=pltpu.SMEM)]
        + [pl.BlockSpec(memory_space=pltpu.VMEM)] * len(arrays),
        out_specs=[pl.BlockSpec(memory_space=pltpu.VMEM)] * len(outs),
        out_shape=[jax.ShapeDtypeStruct(shape, BF) for shape in outs],
        name=name,
    )(where, *arrays)


def column_cuts(widths):
    at, cuts = 0, []
    for width in widths:
        cuts.append(slice(at, at + width))
        at += width
    return cuts


def lay_out(near, far, where, stream, widths):
    rows = near.shape[0]
    half = PLACES // 2
    block = rows // half

    def kernel(where_ref, near_ref, far_ref, *outs):
        at = place_of(where_ref, stream)
        for rank in range(PLACES):
            source = near_ref if rank < half else far_ref
            inside = pl.ds(rank % half * block, block)
            target = pl.ds(pl.multiple_of(at(rank) * block, block), block)
            for out, cut in zip(outs, column_cuts(widths)):
                out[target, :] = source[inside, cut]

    return local_call(
        kernel, f"lay_out_{stream}", [(2 * rows, w) for w in widths], where, near, far
    )


def gather(own, where, stream, widths):
    held = own
    for step in range(STEPS - 1):
        held = jnp.concatenate([held, hop(held, stream, step)], axis=0)
    return lay_out(held, hop(held, stream, STEPS - 1), where, stream, widths)


def pick_far(terms, where, stream):
    block = terms[0].shape[0] // PLACES
    half = PLACES // 2
    widths = [term.shape[1] for term in terms]

    def kernel(where_ref, *refs):
        at = place_of(where_ref, stream)
        for rank in range(half):
            source = pl.ds(pl.multiple_of(at(rank + half) * block, block), block)
            for term, cut in zip(refs, column_cuts(widths)):
                refs[-1][pl.ds(rank * block, block), cut] = term[source, :]

    (far,) = local_call(
        kernel, f"pick_far_{stream}", [(half * block, sum(widths))], where, *terms
    )
    return far


def add_near(terms, given, where, stream):
    block = terms[0].shape[0] // PLACES
    quarter = PLACES // 4
    widths = [term.shape[1] for term in terms]

    def kernel(where_ref, given_ref, *refs):
        at = place_of(where_ref, stream)
        for rank in range(2 * quarter):
            source = pl.ds(pl.multiple_of(at(rank) * block, block), block)
            out = refs[-2 + rank // quarter]
            for term, cut in zip(refs, column_cuts(widths)):
                total = term[source, :].astype(F32)
                total = total + given_ref[pl.ds(rank * block, block), cut].astype(F32)
                out[pl.ds(rank % quarter * block, block), cut] = total.astype(BF)

    outs = [(quarter * block, sum(widths))] * 2
    return local_call(kernel, f"add_near_{stream}", outs, where, given, *terms)


def scatter(terms, where, stream):
    given = hop(pick_far(terms, where, stream), stream, STEPS - 1)
    keep, send = add_near(terms, given, where, stream)
    for step in range(STEPS - 2, -1, -1):
        given = hop(send, stream, step).astype(F32)
        half = keep.shape[0] // 2
        if step:
            send = (keep[half:].astype(F32) + given[half:]).astype(BF)
            keep = (keep[:half].astype(F32) + given[:half]).astype(BF)
    return keep.astype(F32) + given


def last_sum(sums):
    joined = jnp.concatenate(sums, axis=1)
    half = joined.shape[0] // 2
    low, high = joined[:half], joined[half:]
    at_low = lax.axis_index("fsdp_x") == 0
    given = swap(jnp.where(at_low, high, low).astype(BF), "fsdp_x")
    return jnp.where(at_low, low, high) + given.astype(F32)


def attend_probs(q_ref, k_ref):
    factor = temper / math.sqrt(HEAD_DIM)
    scores = dot_nt(q_ref[...], k_ref[...]) * factor
    lifted = jnp.exp(scores - jnp.max(scores, axis=-1, keepdims=True))
    return lifted / jnp.sum(lifted, axis=-1, keepdims=True)


def attend_kernel(q_ref, k_ref, v_ref, o_ref):
    probs = attend_probs(q_ref, k_ref)
    o_ref[...] = dot_nn(probs.astype(BF), v_ref[...]).astype(BF)


def head_specs(rows, heads):
    block = (rows, HEAD_DIM)
    plain = pl.BlockSpec(block, lambda h: (0, h))
    return plain, pl.BlockSpec(block, lambda h: (0, heads + h))


def attend(queries_keys, values):
    rows, width = values.shape
    plain, keys = head_specs(rows, width // HEAD_DIM)
    return pl.pallas_call(
        attend_kernel,
        grid=(width // HEAD_DIM,),
        in_specs=[plain, keys, plain],
        out_specs=plain,
        out_shape=jax.ShapeDtypeStruct((rows, width), BF),
        name="attend",
    )(queries_keys, queries_keys, values)


def attend_back_kernel(q_ref, k_ref, v_ref, d_ref, dqk_ref, dv_ref):
    heads = pl.num_programs(0)
    head = pl.program_id(0)
    factor = temper / math.sqrt(HEAD_DIM)
    upstream = d_ref[...]
    probs = attend_probs(q_ref, k_ref)
    dprobs = dot_nt(upstream, v_ref[...])
    inner = jnp.sum(probs * dprobs, axis=-1, keepdims=True)
    dscores = (probs * (dprobs - inner) * factor).astype(BF)

    def put(place, value):
        at = pl.multiple_of((place * heads + head) * HEAD_DIM, HEAD_DIM)
        dqk_ref[:, pl.ds(at, HEAD_DIM)] = value.astype(BF)

    put(0, dot_nn(dscores, k_ref[...]))
    put(1, dot_tn(dscores, q_ref[...]))
    dv_ref[...] = dot_tn(probs.astype(BF), upstream).astype(BF)


def attend_back(queries_keys, values, upstream):
    rows, width = values.shape
    plain, keys = head_specs(rows, width // HEAD_DIM)
    return pl.pallas_call(
        attend_back_kernel,
        grid=(width // HEAD_DIM,),
        in_specs=[plain, keys, plain, plain],
        out_specs=[pl.BlockSpec((rows, 2 * width), lambda h: (0, 0)), plain],
        out_shape=[
            jax.ShapeDtypeStruct((rows, 2 * width), BF),
            jax.ShapeDtypeStruct((rows, width), BF),
        ],
        name="attend_back",
    )(queries_keys, queries_keys, values, upstream)


def pair_up(own):
    return ordered(own, swap(own, "fsdp_x"), "fsdp_x")


def block_pass(tokens, layer_mod, w_qkv, w_out, w_in, w_back, out_grad, grad_scale):
    own_width = w_out.shape[0]
    where = jnp.stack([lax.axis_index(ZY), lax.axis_index("sp_core")]).astype(jnp.int32)
    cut = 2 * own_width
    attn_pair = pair_up(jnp.concatenate([w_qkv, w_out.T], axis=1))
    (joint_qk,) = gather(attn_pair[:, :cut], where, 0, (cut,))
    joint_v, out_rows = gather(attn_pair[:, cut:], where, 1, (own_width, own_width))
    ffn_pair = pair_up(jnp.concatenate([w_in, w_back.T], axis=1))
    (in_rows,) = gather(ffn_pair[:, : w_in.shape[1]], where, 0, (w_in.shape[1],))
    (back_rows,) = gather(ffn_pair[:, w_in.shape[1] :], where, 1, (w_back.shape[0],))

    stream = tokens.astype(F32)
    normed_first, rstd_first = normalize(stream)
    input_first = (normed_first * (1.0 + layer_mod[1]) + layer_mod[0]).astype(BF)
    first_rows = jnp.concatenate([near_rows(input_first), far_rows(input_first)], axis=0)
    queries_keys = dot_nn(first_rows, joint_qk).astype(BF)
    values = dot_nn(first_rows, joint_v).astype(BF)
    attended = attend(queries_keys, values)
    half = attended.shape[0] // 2
    attn_part = far_sum(dot_nt(attended[half:], out_rows))
    attn_part = attn_part + core_sum(dot_nt(attended[:half], out_rows))
    middle = stream + layer_mod[2] * attn_part
    normed_second, rstd_second = normalize(middle)
    input_second = (normed_second * (1.0 + layer_mod[4]) + layer_mod[3]).astype(BF)
    second_rows = jnp.concatenate([near_rows(input_second), far_rows(input_second)], axis=0)
    hidden = dot_nn(second_rows, in_rows)
    activated, pullback = jax.vjp(gelu_tanh, hidden)
    activated = activated.astype(BF)
    ffn_part = far_sum(dot_nt(activated[half:], back_rows))
    ffn_part = ffn_part + core_sum(dot_nt(activated[:half], back_rows))
    final_out = (middle + layer_mod[5] * ffn_part).astype(BF)

    stream_grad = out_grad.astype(F32)
    down_grad = (layer_mod[5] * stream_grad).astype(BF)
    down_rows = jnp.concatenate([near_rows(down_grad), far_rows(down_grad)], axis=0)
    up_grad = pullback(dot_nn(down_rows, back_rows))[0].astype(BF)
    back_second = far_sum(dot_nt(up_grad[half:], in_rows))
    back_second = back_second + core_sum(dot_nt(up_grad[:half], in_rows))
    term_back = (dot_tn(down_rows, activated) * grad_scale).astype(BF)
    term_in = (dot_tn(second_rows, up_grad) * grad_scale).astype(BF)
    part_in, part_back = scatter([term_in], where, 0), scatter([term_back], where, 1)
    sum_ffn = last_sum([part_in, part_back])
    stream_grad = stream_grad + norm_back(
        normed_second, rstd_second, back_second * (1.0 + layer_mod[4])
    )
    attn_grad = (layer_mod[2] * stream_grad).astype(BF)
    attn_rows = jnp.concatenate([near_rows(attn_grad), far_rows(attn_grad)], axis=0)
    mixed_grad = dot_nn(attn_rows, out_rows).astype(BF)
    grad_qk, grad_v = attend_back(queries_keys, values, mixed_grad)
    term_qk = (dot_tn(first_rows, grad_qk) * grad_scale).astype(BF)
    term_v = (dot_tn(first_rows, grad_v) * grad_scale).astype(BF)
    term_out = (dot_tn(attn_rows, attended) * grad_scale).astype(BF)
    part_qk, part_vo = scatter([term_qk], where, 0), scatter([term_v, term_out], where, 1)
    sum_attn = last_sum([part_qk, part_vo])

    def back_rows_of(span):
        return dot_nt(grad_qk[span], joint_qk) + dot_nt(grad_v[span], joint_v)

    back_first = far_sum(back_rows_of(slice(half, None)))
    back_first = back_first + core_sum(back_rows_of(slice(None, half)))
    stream_grad = stream_grad + norm_back(
        normed_first, rstd_first, back_first * (1.0 + layer_mod[1])
    )
    return (
        final_out,
        stream_grad,
        sum_attn[:, : 3 * own_width],
        sum_attn[:, 3 * own_width :].T,
        sum_ffn[:, : w_in.shape[1]],
        sum_ffn[:, w_in.shape[1] :].T,
    )


def body(tokens, modulation, w_qkv, w_out, w_in, w_back, out_grad):
    local_seq = tokens.shape[1]
    own_width = w_qkv.shape[3]
    grad_scale = 1.0 / math.sqrt(local_seq * lax.axis_size(FSDP) * lax.axis_size(SP))
    final_out, input_grad, grad_qkv, grad_out, grad_in, grad_back = block_pass(
        tokens[0],
        modulation[0, 0],
        w_qkv[0].reshape(-1, 3 * own_width),
        w_out[0],
        w_in[0],
        w_back[0],
        out_grad[0],
        grad_scale,
    )
    return (
        final_out[None],
        input_grad[None],
        grad_qkv.reshape(1, -1, 3, own_width),
        grad_out[None],
        grad_in[None],
        grad_back[None],
    )


def solution(mesh):
    torus = Mesh(
        mesh.devices.reshape(4, 4, 2, 2, 2),
        (*FSDP, *SP),
    )
    return jax.shard_map(
        body,
        mesh=torus,
        in_specs=(
            P(FSDP, SP, None),
            P(FSDP, None, None, None),
            P(None, FSDP, None, SP),
            P(None, SP, FSDP),
            P(None, FSDP, SP),
            P(None, SP, FSDP),
            P(FSDP, SP, None),
        ),
        out_specs=(
            P(FSDP, SP, None),
            P(FSDP, SP, None),
            P(None, FSDP, None, SP),
            P(None, SP, FSDP),
            P(None, FSDP, SP),
            P(None, SP, FSDP),
        ),
        check_vma=False,
    )
```

```python
import math

import jax
import jax.numpy as jnp
from jax import lax
from jax.experimental import pallas as pl
from jax.experimental.pallas import tpu as pltpu
from jax.sharding import Mesh
from jax.sharding import PartitionSpec as P

HEAD_DIM = 128
ZY = ("fsdp_z", "fsdp_y")
FSDP = (*ZY, "fsdp_x")
SP = ("sp_x", "sp_core")
SWAP = ((0, 1), (1, 0))
GRID = (*ZY, "sp_core")
PLACES = 16
FLIPS = (1, 4, 3, 12)
STEPS = len(FLIPS)

ln_eps = 1e-06
temper = 2.5
BF = jnp.bfloat16
F32 = jnp.float32


def normalize(stream):
    mean_part = jnp.mean(stream, axis=-1, keepdims=True)
    centred = stream - mean_part
    rstd = lax.rsqrt(jnp.mean(centred * centred, axis=-1, keepdims=True) + ln_eps)
    return (centred * rstd, rstd)


def norm_back(normed, rstd, incoming):
    first = jnp.mean(incoming, axis=-1, keepdims=True)
    second = jnp.mean(incoming * normed, axis=-1, keepdims=True)
    return rstd * (incoming - first - normed * second)


def gelu_tanh(hidden):
    return jax.nn.gelu(hidden, approximate=True)


def dot_nn(left, right):
    return jnp.dot(left, right, preferred_element_type=F32)


def dot_nt(left, right):
    return lax.dot_general(left, right, (((1,), (1,)), ((), ())), preferred_element_type=F32)


def dot_tn(left, right):
    return lax.dot_general(left, right, (((0,), (0,)), ((), ())), preferred_element_type=F32)


def swap(value, axis):
    return lax.ppermute(value, axis, SWAP)


def after(value, *earlier):
    return lax.optimization_barrier((value, earlier))[0]


def near_rows(own):
    return jnp.concatenate([own, swap(own, "sp_core")], axis=0)


def far_rows(own):
    across = swap(own, "sp_x")
    return jnp.concatenate([across, swap(across, "sp_core")], axis=0)


def core_sum(part):
    rows = part.shape[0] // 2
    given = swap(part[rows:].astype(BF), "sp_core")
    return part[:rows] + given.astype(F32)


def far_sum(part):
    return swap(core_sum(part).astype(BF), "sp_x").astype(F32)


def ordered(own, other, axis):
    first = jnp.concatenate([own, other], axis=0)
    second = jnp.concatenate([other, own], axis=0)
    return jnp.where(lax.axis_index(axis) == 0, first, second)


def hop(value, stream, step):
    pairs = []
    for place in range(PLACES):
        for core in range(2):
            flip = FLIPS[(2 * stream + core + step) % STEPS]
            pairs.append((2 * place + core, 2 * (place ^ flip) + core))
    return lax.ppermute(value, GRID, pairs)


def place_of(where_ref, stream):
    turn = 2 * stream + where_ref[1]
    flips = []
    for step in range(STEPS):
        link = lax.rem(turn + step, STEPS)
        low = jnp.where(link == 0, FLIPS[0], FLIPS[1])
        high = jnp.where(link == 2, FLIPS[2], FLIPS[3])
        flips.append(jnp.where(link < 2, low, high))

    def at(rank):
        place = where_ref[0]
        for step in range(STEPS):
            if rank >> step & 1:
                place = place ^ flips[step]
        return place

    return at


def local_call(kernel, name, outs, where, *arrays):
    return pl.pallas_call(
        kernel,
        in_specs=[pl.BlockSpec(memory_space=pltpu.SMEM)]
        + [pl.BlockSpec(memory_space=pltpu.VMEM)] * len(arrays),
        out_specs=[pl.BlockSpec(memory_space=pltpu.VMEM)] * len(outs),
        out_shape=[jax.ShapeDtypeStruct(shape, BF) for shape in outs],
        name=name,
    )(where, *arrays)


def column_cuts(widths):
    at, cuts = 0, []
    for width in widths:
        cuts.append(slice(at, at + width))
        at += width
    return cuts


def lay_out(near, far, where, stream, widths):
    rows = near.shape[0]
    half = PLACES // 2
    block = rows // half

    def kernel(where_ref, near_ref, far_ref, *outs):
        at = place_of(where_ref, stream)
        for rank in range(PLACES):
            source = near_ref if rank < half else far_ref
            inside = pl.ds(rank % half * block, block)
            target = pl.ds(pl.multiple_of(at(rank) * block, block), block)
            for out, cut in zip(outs, column_cuts(widths)):
                out[target, :] = source[inside, cut]

    return local_call(
        kernel, f"lay_out_{stream}", [(2 * rows, w) for w in widths], where, near, far
    )


def step_on(held, stream, step):
    return jnp.concatenate([held, hop(held, stream, step)], axis=0)


def pick_far(terms, where, stream):
    block = terms[0].shape[0] // PLACES
    half = PLACES // 2
    widths = [term.shape[1] for term in terms]

    def kernel(where_ref, *refs):
        at = place_of(where_ref, stream)
        for rank in range(half):
            source = pl.ds(pl.multiple_of(at(rank + half) * block, block), block)
            for term, cut in zip(refs, column_cuts(widths)):
                refs[-1][pl.ds(rank * block, block), cut] = term[source, :]

    (far,) = local_call(
        kernel, f"pick_far_{stream}", [(half * block, sum(widths))], where, *terms
    )
    return far


def add_near(terms, given, where, stream):
    block = terms[0].shape[0] // PLACES
    quarter = PLACES // 4
    widths = [term.shape[1] for term in terms]

    def kernel(where_ref, given_ref, *refs):
        at = place_of(where_ref, stream)
        for rank in range(2 * quarter):
            source = pl.ds(pl.multiple_of(at(rank) * block, block), block)
            out = refs[-2 + rank // quarter]
            for term, cut in zip(refs, column_cuts(widths)):
                total = term[source, :].astype(F32)
                total = total + given_ref[pl.ds(rank * block, block), cut].astype(F32)
                out[pl.ds(rank % quarter * block, block), cut] = total.astype(BF)

    outs = [(quarter * block, sum(widths))] * 2
    return local_call(kernel, f"add_near_{stream}", outs, where, given, *terms)


def first_hop(terms, where, stream):
    far = pick_far(terms, where, stream)
    return far, hop(far, stream, STEPS - 1)


def fold(keep, send, stream, step):
    given = hop(send, stream, step).astype(F32)
    half = keep.shape[0] // 2
    if not step:
        return keep.astype(F32) + given
    send = (keep[half:].astype(F32) + given[half:]).astype(BF)
    return (keep[:half].astype(F32) + given[:half]).astype(BF), send


def fold_down(keep, send, stream):
    for step in range(STEPS - 2, 0, -1):
        keep, send = fold(keep, send, stream, step)
    return fold(keep, send, stream, 0)


def last_sum(sums):
    joined = jnp.concatenate(sums, axis=1)
    half = joined.shape[0] // 2
    low, high = joined[:half], joined[half:]
    at_low = lax.axis_index("fsdp_x") == 0
    given = swap(jnp.where(at_low, high, low).astype(BF), "fsdp_x")
    return jnp.where(at_low, low, high) + given.astype(F32)


def attend_probs(q_ref, k_ref):
    factor = temper / math.sqrt(HEAD_DIM)
    scores = dot_nt(q_ref[...], k_ref[...]) * factor
    lifted = jnp.exp(scores - jnp.max(scores, axis=-1, keepdims=True))
    return lifted / jnp.sum(lifted, axis=-1, keepdims=True)


def attend_kernel(q_ref, k_ref, v_ref, o_ref):
    probs = attend_probs(q_ref, k_ref)
    o_ref[...] = dot_nn(probs.astype(BF), v_ref[...]).astype(BF)


def head_specs(rows, heads):
    block = (rows, HEAD_DIM)
    plain = pl.BlockSpec(block, lambda h: (0, h))
    return plain, pl.BlockSpec(block, lambda h: (0, heads + h))


def attend(queries_keys, values):
    rows, width = values.shape
    plain, keys = head_specs(rows, width // HEAD_DIM)
    return pl.pallas_call(
        attend_kernel,
        grid=(width // HEAD_DIM,),
        in_specs=[plain, keys, plain],
        out_specs=plain,
        out_shape=jax.ShapeDtypeStruct((rows, width), BF),
        name="attend",
    )(queries_keys, queries_keys, values)


def attend_back_kernel(q_ref, k_ref, v_ref, d_ref, dqk_ref, dv_ref):
    heads = pl.num_programs(0)
    head = pl.program_id(0)
    factor = temper / math.sqrt(HEAD_DIM)
    upstream = d_ref[...]
    probs = attend_probs(q_ref, k_ref)
    dprobs = dot_nt(upstream, v_ref[...])
    inner = jnp.sum(probs * dprobs, axis=-1, keepdims=True)
    dscores = (probs * (dprobs - inner) * factor).astype(BF)

    def put(place, value):
        at = pl.multiple_of((place * heads + head) * HEAD_DIM, HEAD_DIM)
        dqk_ref[:, pl.ds(at, HEAD_DIM)] = value.astype(BF)

    put(0, dot_nn(dscores, k_ref[...]))
    put(1, dot_tn(dscores, q_ref[...]))
    dv_ref[...] = dot_tn(probs.astype(BF), upstream).astype(BF)


def attend_back(queries_keys, values, upstream):
    rows, width = values.shape
    plain, keys = head_specs(rows, width // HEAD_DIM)
    return pl.pallas_call(
        attend_back_kernel,
        grid=(width // HEAD_DIM,),
        in_specs=[plain, keys, plain, plain],
        out_specs=[pl.BlockSpec((rows, 2 * width), lambda h: (0, 0)), plain],
        out_shape=[
            jax.ShapeDtypeStruct((rows, 2 * width), BF),
            jax.ShapeDtypeStruct((rows, width), BF),
        ],
        name="attend_back",
    )(queries_keys, queries_keys, values, upstream)


def pair_up(own):
    return ordered(own, swap(own, "fsdp_x"), "fsdp_x")


def block_pass(tokens, layer_mod, w_qkv, w_out, w_in, w_back, out_grad, grad_scale):
    own_width, ffn_width = w_out.shape[0], w_in.shape[1]
    where = jnp.stack([lax.axis_index(ZY), lax.axis_index("sp_core")]).astype(jnp.int32)
    cut = 2 * own_width
    attn_pair = pair_up(jnp.concatenate([w_qkv, w_out.T], axis=1))
    ffn_own = after(jnp.concatenate([w_in, w_back.T], axis=1), attn_pair)
    ffn_pair = pair_up(ffn_own)

    stream = tokens.astype(F32)
    normed_first, rstd_first = normalize(stream)
    input_first = (normed_first * (1.0 + layer_mod[1]) + layer_mod[0]).astype(BF)

    attn_held = [attn_pair[:, :cut], attn_pair[:, cut:]]
    for step in (0, 1):
        attn_held = [step_on(held, k, step) for k, held in enumerate(attn_held)]
    input_first = after(input_first, attn_pair)
    first_rows = jnp.concatenate([near_rows(input_first), far_rows(input_first)], axis=0)
    ffn_pair = after(ffn_pair, attn_held)
    attn_held = [step_on(held, k, 2) for k, held in enumerate(attn_held)]
    ffn_held = [ffn_pair[:, :ffn_width], ffn_pair[:, ffn_width:]]
    ffn_held = [step_on(held, k, 0) for k, held in enumerate(ffn_held)]
    ffn_held = [after(held, attn_held) for held in ffn_held]
    attn_far = [hop(held, k, 3) for k, held in enumerate(attn_held)]
    ffn_held = [step_on(held, k, 1) for k, held in enumerate(ffn_held)]

    out_grad = after(out_grad, first_rows)
    stream_grad = out_grad.astype(F32)
    down_grad = (layer_mod[5] * stream_grad).astype(BF)
    down_rows = jnp.concatenate([near_rows(down_grad), far_rows(down_grad)], axis=0)

    attn_far = after(attn_far, down_rows)
    ffn_held = [after(held, attn_far) for held in ffn_held]
    ffn_third = [hop(held, k, 2) for k, held in enumerate(ffn_held)]

    (joint_qk,) = lay_out(attn_held[0], attn_far[0], where, 0, (cut,))
    joint_v, out_rows = lay_out(attn_held[1], attn_far[1], where, 1, (own_width, own_width))
    queries_keys = dot_nn(first_rows, joint_qk).astype(BF)
    values = dot_nn(first_rows, joint_v).astype(BF)
    attended = attend(queries_keys, values)
    half = attended.shape[0] // 2
    far_part = core_sum(dot_nt(attended[half:], out_rows)).astype(BF)
    near_part = dot_nt(attended[:half], out_rows)
    ffn_third = after(ffn_third, far_part, near_part)
    ffn_held = [jnp.concatenate(pair, axis=0) for pair in zip(ffn_held, ffn_third)]
    ffn_far = [hop(held, k, 3) for k, held in enumerate(ffn_held)]
    attn_part = swap(far_part, "sp_x").astype(F32) + core_sum(near_part)
    middle = stream + layer_mod[2] * attn_part
    normed_second, rstd_second = normalize(middle)
    input_second = (normed_second * (1.0 + layer_mod[4]) + layer_mod[3]).astype(BF)
    second_rows = jnp.concatenate([near_rows(input_second), far_rows(input_second)], axis=0)
    ffn_far = after(ffn_far, input_second)
    (in_rows,) = lay_out(ffn_held[0], ffn_far[0], where, 0, (ffn_width,))
    (back_rows,) = lay_out(ffn_held[1], ffn_far[1], where, 1, (ffn_width,))

    hidden = dot_nn(second_rows, in_rows)
    activated, pullback = jax.vjp(gelu_tanh, hidden)
    activated = activated.astype(BF)
    up_grad = pullback(dot_nn(down_rows, back_rows))[0].astype(BF)

    far_part = core_sum(dot_nt(up_grad[half:], in_rows)).astype(BF)
    near_part = dot_nt(up_grad[:half], in_rows)
    up_rows, _ = lax.optimization_barrier((up_grad, (far_part, near_part)))
    term_in = (dot_tn(second_rows, up_rows) * grad_scale).astype(BF)
    picked_in, given_in = first_hop([term_in], where, 0)
    far_part = swap(far_part, "sp_x")
    back_second = after(far_part, picked_in).astype(F32) + core_sum(near_part)
    stream_grad = stream_grad + norm_back(
        normed_second, rstd_second, back_second * (1.0 + layer_mod[4])
    )
    attn_grad = (layer_mod[2] * stream_grad).astype(BF)
    term_back = dot_tn(down_rows, after(activated, attn_grad))
    term_back = (term_back * grad_scale).astype(BF)
    picked_back, given_back = first_hop([term_back], where, 1)
    far_attn = far_rows(attn_grad)
    attn_rows = jnp.concatenate([near_rows(attn_grad), after(far_attn, picked_back)], axis=0)
    mixed_grad = dot_nn(attn_rows, out_rows).astype(BF)
    grad_qk, grad_v = attend_back(queries_keys, values, mixed_grad)

    def back_rows_of(span):
        return dot_nt(grad_qk[span], joint_qk) + dot_nt(grad_v[span], joint_v)

    far_part = core_sum(back_rows_of(slice(half, None))).astype(BF)
    near_part = back_rows_of(slice(None, half))
    qk_rows, v_rows, o_rows = after((grad_qk, grad_v, attended), far_part, near_part)
    term_qk = (dot_tn(first_rows, qk_rows) * grad_scale).astype(BF)
    picked_qk, given_qk = first_hop([term_qk], where, 0)
    term_v = (dot_tn(first_rows, v_rows) * grad_scale).astype(BF)
    term_out = (dot_tn(attn_rows, o_rows) * grad_scale).astype(BF)
    picked_vo, given_vo = first_hop([term_v, term_out], where, 1)
    given_in, given_back = after((given_in, given_back), picked_qk, picked_vo)
    two_in = add_near([term_in], given_in, where, 0)
    two_back = add_near([term_back], given_back, where, 1)
    given_qk, given_vo = after((given_qk, given_vo), two_in, two_back)
    two_qk = add_near([term_qk], given_qk, where, 0)
    two_vo = add_near([term_v, term_out], given_vo, where, 1)

    far_part = swap(far_part, "sp_x")
    back_first = after(far_part, picked_vo).astype(F32) + core_sum(near_part)
    input_grad = stream_grad + norm_back(
        normed_first, rstd_first, back_first * (1.0 + layer_mod[1])
    )

    late = after(activated, two_in, two_back)
    ffn_part = far_sum(dot_nt(late[half:], back_rows))
    ffn_part = ffn_part + core_sum(dot_nt(late[:half], back_rows))
    final_out = (middle + layer_mod[5] * ffn_part).astype(BF)

    sum_ffn = last_sum([fold_down(*two_in, 0), fold_down(*two_back, 1)])
    sum_attn = last_sum([fold_down(*two_qk, 0), fold_down(*two_vo, 1)])
    return (
        final_out,
        input_grad,
        sum_attn[:, : 3 * own_width],
        sum_attn[:, 3 * own_width :].T,
        sum_ffn[:, :ffn_width],
        sum_ffn[:, ffn_width:].T,
    )


def body(tokens, modulation, w_qkv, w_out, w_in, w_back, out_grad):
    local_seq = tokens.shape[1]
    own_width = w_qkv.shape[3]
    grad_scale = 1.0 / math.sqrt(local_seq * lax.axis_size(FSDP) * lax.axis_size(SP))
    final_out, input_grad, grad_qkv, grad_out, grad_in, grad_back = block_pass(
        tokens[0],
        modulation[0, 0],
        w_qkv[0].reshape(-1, 3 * own_width),
        w_out[0],
        w_in[0],
        w_back[0],
        out_grad[0],
        grad_scale,
    )
    return (
        final_out[None],
        input_grad[None],
        grad_qkv.reshape(1, -1, 3, own_width),
        grad_out[None],
        grad_in[None],
        grad_back[None],
    )


def solution(mesh):
    torus = Mesh(
        mesh.devices.reshape(4, 4, 2, 2, 2),
        (*FSDP, *SP),
    )
    return jax.shard_map(
        body,
        mesh=torus,
        in_specs=(
            P(FSDP, SP, None),
            P(FSDP, None, None, None),
            P(None, FSDP, None, SP),
            P(None, SP, FSDP),
            P(None, FSDP, SP),
            P(None, SP, FSDP),
            P(FSDP, SP, None),
        ),
        out_specs=(
            P(FSDP, SP, None),
            P(FSDP, SP, None),
            P(None, FSDP, None, SP),
            P(None, SP, FSDP),
            P(None, FSDP, SP),
            P(None, SP, FSDP),
        ),
        check_vma=False,
    )
```

```python
import math

import jax
import jax.numpy as jnp
from jax import lax
from jax.experimental import pallas as pl
from jax.experimental.pallas import tpu as pltpu
from jax.sharding import Mesh
from jax.sharding import PartitionSpec as P

HEAD_DIM = 128
ZY = ("fsdp_z", "fsdp_y")
FSDP = (*ZY, "fsdp_x")
SP = ("sp_x", "sp_core")
SWAP = ((0, 1), (1, 0))
GRID = (*ZY, "sp_core")
PLACES = 16
FLIPS = (1, 4, 3, 12)
STEPS = len(FLIPS)

ln_eps = 1e-06
temper = 2.5
BF = jnp.bfloat16
F32 = jnp.float32


def normalize(stream):
    mean_part = jnp.mean(stream, axis=-1, keepdims=True)
    centred = stream - mean_part
    rstd = lax.rsqrt(jnp.mean(centred * centred, axis=-1, keepdims=True) + ln_eps)
    return (centred * rstd, rstd)


def norm_back(normed, rstd, incoming):
    first = jnp.mean(incoming, axis=-1, keepdims=True)
    second = jnp.mean(incoming * normed, axis=-1, keepdims=True)
    return rstd * (incoming - first - normed * second)


def dot_nn(left, right):
    return jnp.dot(left, right, preferred_element_type=F32)


def dot_nt(left, right):
    return lax.dot_general(left, right, (((1,), (1,)), ((), ())), preferred_element_type=F32)


def dot_tn(left, right):
    return lax.dot_general(left, right, (((0,), (0,)), ((), ())), preferred_element_type=F32)


def swap(value, axis):
    return lax.ppermute(value, axis, SWAP)


def after(value, *earlier):
    return lax.optimization_barrier((value, earlier))[0]


def spread(own):
    pair = jnp.concatenate([own, swap(own, "sp_x")], axis=0)
    return pair, swap(pair, "sp_core")


def collect_core(keep, give):
    return keep + swap(give, "sp_core").astype(F32)


def collect_x(total):
    rows = total.shape[0] // 2
    return total[:rows], swap(total[rows:].astype(BF), "sp_x")


def ordered(own, other, axis):
    first = jnp.concatenate([own, other], axis=0)
    second = jnp.concatenate([other, own], axis=0)
    return jnp.where(lax.axis_index(axis) == 0, first, second)


def hop(value, stream, step):
    pairs = []
    for place in range(PLACES):
        for core in range(2):
            flip = FLIPS[(2 * stream + core + step) % STEPS]
            pairs.append((2 * place + core, 2 * (place ^ flip) + core))
    return lax.ppermute(value, GRID, pairs)


def place_of(where_ref, stream):
    turn = 2 * stream + where_ref[1]
    flips = []
    for step in range(STEPS):
        link = lax.rem(turn + step, STEPS)
        low = jnp.where(link == 0, FLIPS[0], FLIPS[1])
        high = jnp.where(link == 2, FLIPS[2], FLIPS[3])
        flips.append(jnp.where(link < 2, low, high))

    def at(rank):
        place = where_ref[0]
        for step in range(STEPS):
            if rank >> step & 1:
                place = place ^ flips[step]
        return place

    return at


def local_call(kernel, name, outs, scratch, where, arrays, remote=()):
    vmem, hbm = pl.BlockSpec(memory_space=pltpu.VMEM), pl.BlockSpec(memory_space=pltpu.HBM)
    return pl.pallas_call(
        kernel,
        in_specs=[pl.BlockSpec(memory_space=pltpu.SMEM)]
        + [vmem] * len(arrays)
        + [hbm] * len(remote),
        out_specs=[vmem] * len(outs),
        out_shape=[jax.ShapeDtypeStruct(shape, kind) for shape, kind in outs],
        scratch_shapes=scratch,
        name=name,
        compiler_params=pltpu.CompilerParams(vmem_limit_bytes=56 * 1024 * 1024),
    )(where, *arrays, *remote)


def placed_load(where_ref, held, target, sems, stream):
    near, far = held
    half = PLACES // 2
    block = target.shape[0] // PLACES
    at = place_of(where_ref, stream)
    copies = []
    for rank in range(PLACES):
        source = near if rank < half else far
        copies.append(
            pltpu.make_async_copy(
                source.at[pl.ds(rank % half * block, block), :],
                target.at[pl.ds(pl.multiple_of(at(rank) * block, block), block), :],
                sems.at[rank],
            )
        )
    for copy in copies:
        copy.start()
    return copies


def finish(copies):
    for copy in copies:
        copy.wait()


def column_cuts(widths):
    at, cuts = 0, []
    for width in widths:
        cuts.append(slice(at, at + width))
        at += width
    return cuts


def step_on(held, stream, step):
    return jnp.concatenate([held, hop(held, stream, step)], axis=0)


def term_blocks(name, products, where, stream, grad_scale):
    lefts = [half for left, _ in products for half in left]
    rights = [right for _, right in products]
    height = lefts[0].shape[1]
    cuts = column_cuts([right.shape[1] for right in rights])
    width = cuts[-1].stop
    block = height // PLACES
    half = PLACES // 2
    strip = height // 4

    def kernel(where_ref, *refs):
        left_refs, refs = refs[: len(lefts)], refs[len(lefts) :]
        right_refs, (near_ref, far_ref, whole) = refs[: len(rights)], refs[len(rights) :]
        at = place_of(where_ref, stream)
        for number, cut in enumerate(cuts):
            upper, lower = left_refs[2 * number : 2 * number + 2]
            rows = upper.shape[0]
            for k in range(4):
                part = slice(k * strip, (k + 1) * strip)
                total = dot_tn(upper[:, part], right_refs[number][:rows, :])
                total = total + dot_tn(lower[:, part], right_refs[number][rows:, :])
                whole[part, cut] = (total * grad_scale).astype(BF)
        for rank in range(PLACES):
            source = pl.ds(pl.multiple_of(at(rank) * block, block), block)
            out = near_ref if rank < half else far_ref
            out[pl.ds(rank % half * block, block), :] = whole[source, :]

    outs = [((height // 2, width), BF)] * 2
    scratch = [pltpu.VMEM((height, width), BF)]
    return local_call(kernel, name, outs, scratch, where, (*lefts, *rights))


def fold(near, given):
    half = near.shape[0] // 2
    total = near.astype(F32) + given.astype(F32)
    return total[:half].astype(BF), total[half:].astype(BF)


def last_sum(sums):
    joined = jnp.concatenate(sums, axis=1)
    half = joined.shape[0] // 2
    low, high = joined[:half], joined[half:]
    at_low = lax.axis_index("fsdp_x") == 0
    given = swap(jnp.where(at_low, high, low).astype(BF), "fsdp_x")
    return jnp.where(at_low, low, high) + given.astype(F32)


def split_rows(where_rows, send_ref, keep_ref, value_of):
    half = where_rows // 2
    send_ref[...] = value_of(slice(half, None)).astype(BF)
    keep_ref[...] = value_of(slice(None, half))


def attend_probs(queries, keys):
    factor = temper / math.sqrt(HEAD_DIM)
    scores = dot_nt(queries, keys) * factor
    lifted = jnp.exp(scores - jnp.max(scores, axis=-1, keepdims=True))
    return lifted / jnp.sum(lifted, axis=-1, keepdims=True)


def held_scratch(held):
    return [
        pltpu.VMEM((2 * held[0].shape[0], held[0].shape[1]), BF),
        pltpu.SemaphoreType.DMA((PLACES,)),
    ]


def attention(rows, held_qk, held_vo, where):
    width = held_vo[0].shape[1] // 2
    count = 2 * rows[0].shape[0]
    model = rows[0].shape[1]

    def kernel(where_ref, upper, lower, near0, far0, near1, far1, *refs):
        qk_ref, v_ref, o_ref, send_ref, keep_ref, w0, sems0, w1, sems1 = refs
        first = placed_load(where_ref, (near0, far0), w0, sems0, 0)
        second = placed_load(where_ref, (near1, far1), w1, sems1, 1)
        half = count // 2
        finish(first)
        qk_ref[:half, :] = dot_nn(upper[...], w0[...]).astype(BF)
        qk_ref[half:, :] = dot_nn(lower[...], w0[...]).astype(BF)
        finish(second)
        v_ref[:half, :] = dot_nn(upper[...], w1[:, :width]).astype(BF)
        v_ref[half:, :] = dot_nn(lower[...], w1[:, :width]).astype(BF)
        for at in range(0, width, HEAD_DIM):
            head = slice(at, at + HEAD_DIM)
            probs = attend_probs(qk_ref[:, head], qk_ref[:, width + at : width + at + HEAD_DIM])
            o_ref[:, head] = dot_nn(probs.astype(BF), v_ref[:, head]).astype(BF)
        split_rows(count, send_ref, keep_ref, lambda span: dot_nt(o_ref[span, :], w1[:, width:]))

    outs = [
        ((count, 2 * width), BF),
        ((count, width), BF),
        ((count, width), BF),
        ((count // 2, model), BF),
        ((count // 2, model), F32),
    ]
    scratch = held_scratch(held_qk) + held_scratch(held_vo)
    return local_call(kernel, "attention", outs, scratch, where, rows, (*held_qk, *held_vo))


def attention_back(rows, queries_keys, values, held_qk, held_vo, where):
    width = values.shape[1]
    count = values.shape[0]
    model = rows[0].shape[1]
    factor = temper / math.sqrt(HEAD_DIM)

    def kernel(where_ref, upper, lower, qk_ref, v_ref, near0, far0, near1, far1, *refs):
        dqk_ref, dv_ref, send_ref, keep_ref, mixed, w0, sems0, w1, sems1 = refs
        second = placed_load(where_ref, (near1, far1), w1, sems1, 1)
        first = placed_load(where_ref, (near0, far0), w0, sems0, 0)
        half = count // 2
        finish(second)
        mixed[:half, :] = dot_nn(upper[...], w1[:, width:]).astype(BF)
        mixed[half:, :] = dot_nn(lower[...], w1[:, width:]).astype(BF)
        for at in range(0, width, HEAD_DIM):
            head = slice(at, at + HEAD_DIM)
            key_head = slice(width + at, width + at + HEAD_DIM)
            upstream = mixed[:, head]
            probs = attend_probs(qk_ref[:, head], qk_ref[:, key_head])
            dprobs = dot_nt(upstream, v_ref[:, head])
            inner = jnp.sum(probs * dprobs, axis=-1, keepdims=True)
            dscores = (probs * (dprobs - inner) * factor).astype(BF)
            dqk_ref[:, head] = dot_nn(dscores, qk_ref[:, key_head]).astype(BF)
            dqk_ref[:, key_head] = dot_tn(dscores, qk_ref[:, head]).astype(BF)
            dv_ref[:, head] = dot_tn(probs.astype(BF), upstream).astype(BF)
        finish(first)

        def part(span):
            return dot_nt(dqk_ref[span, :], w0[...]) + dot_nt(dv_ref[span, :], w1[:, :width])

        split_rows(count, send_ref, keep_ref, part)

    outs = [
        ((count, 2 * width), BF),
        ((count, width), BF),
        ((count // 2, model), BF),
        ((count // 2, model), F32),
    ]
    scratch = [pltpu.VMEM((count, width), BF)] + held_scratch(held_qk) + held_scratch(held_vo)
    arrays = (*rows, queries_keys, values)
    return local_call(kernel, "attention_back", outs, scratch, where, arrays, (*held_qk, *held_vo))


def gelu_pair(hidden):
    root, cube = math.sqrt(2.0 / math.pi), 0.044715
    square = hidden * hidden
    curve = jnp.tanh(root * (hidden + cube * (square * hidden)))
    rise = 0.5 * (1.0 + curve)
    slope = 0.5 * hidden * (1.0 - curve * curve) * (root * (1.0 + 3.0 * cube * square))
    return hidden * rise, rise + slope


def feed_forward(rows, down_rows, held_in, held_back, where):
    width = held_in[0].shape[1]
    count = 2 * rows[0].shape[0]
    model = rows[0].shape[1]
    strip = width // 4

    def kernel(where_ref, upper, lower, d_upper, d_lower, near0, far0, near1, far1, *refs):
        act_ref, up_ref, send_ref, keep_ref, w0, sems0, w1, sems1 = refs
        first = placed_load(where_ref, (near0, far0), w0, sems0, 0)
        second = placed_load(where_ref, (near1, far1), w1, sems1, 1)
        half = count // 2
        finish(first)
        finish(second)
        for k in range(4):
            part = slice(k * strip, (k + 1) * strip)
            for at, left, down in ((0, upper, d_upper), (half, lower, d_lower)):
                active, slope = gelu_pair(dot_nn(left[...], w0[:, part]))
                act_ref[at : at + half, part] = active.astype(BF)
                grad = slope * dot_nn(down[...], w1[:, part])
                up_ref[at : at + half, part] = grad.astype(BF)
        split_rows(count, send_ref, keep_ref, lambda span: dot_nt(up_ref[span, :], w0[...]))

    outs = [
        ((count, width), BF),
        ((count, width), BF),
        ((count // 2, model), BF),
        ((count // 2, model), F32),
    ]
    scratch = held_scratch(held_in) + held_scratch(held_back)
    arrays = (*rows, *down_rows)
    return local_call(kernel, "feed_forward", outs, scratch, where, arrays, (*held_in, *held_back))


def down_project(activated, held_back, where):
    count = activated.shape[0]
    model = 2 * held_back[0].shape[0]

    def kernel(where_ref, act_ref, near, far, send_ref, keep_ref, w1, sems):
        finish(placed_load(where_ref, (near, far), w1, sems, 1))
        split_rows(count, send_ref, keep_ref, lambda span: dot_nt(act_ref[span, :], w1[...]))

    outs = [((count // 2, model), BF), ((count // 2, model), F32)]
    scratch = held_scratch(held_back)
    return local_call(kernel, "down_project", outs, scratch, where, (activated,), held_back)


def pair_up(own):
    return ordered(own, swap(own, "fsdp_x"), "fsdp_x")


def block_pass(tokens, layer_mod, w_qkv, w_out, w_in, w_back, out_grad, grad_scale):
    own_width, ffn_width = w_out.shape[0], w_in.shape[1]
    where = jnp.stack([lax.axis_index(ZY), lax.axis_index("sp_core")]).astype(jnp.int32)
    cut = 2 * own_width
    attn_pair = pair_up(jnp.concatenate([w_qkv, w_out.T], axis=1))
    ffn_own = after(jnp.concatenate([w_in, w_back.T], axis=1), attn_pair)
    ffn_pair = pair_up(ffn_own)

    stream = tokens.astype(F32)
    normed_first, rstd_first = normalize(stream)
    input_first = (normed_first * (1.0 + layer_mod[1]) + layer_mod[0]).astype(BF)

    attn_held = [attn_pair[:, :cut], attn_pair[:, cut:]]
    for step in (0, 1):
        attn_held = [step_on(held, k, step) for k, held in enumerate(attn_held)]
    input_first = after(input_first, attn_pair)
    first_rows = spread(input_first)
    ffn_pair = after(ffn_pair, attn_held)
    attn_held = [step_on(held, k, 2) for k, held in enumerate(attn_held)]
    ffn_held = [ffn_pair[:, :ffn_width], ffn_pair[:, ffn_width:]]
    ffn_held = [step_on(held, k, 0) for k, held in enumerate(ffn_held)]
    ffn_held = [after(held, attn_held) for held in ffn_held]
    attn_far = [hop(held, k, 3) for k, held in enumerate(attn_held)]

    out_grad = after(out_grad, first_rows)
    stream_grad = out_grad.astype(F32)
    down_grad = (layer_mod[5] * stream_grad).astype(BF)
    down_rows = spread(down_grad)

    ffn_third = [hop(held, k, 1) for k, held in enumerate(ffn_held)]
    held_qk, held_vo = tuple(zip(attn_held, attn_far))
    queries_keys, values, attended, send, keep = attention(first_rows, held_qk, held_vo, where)
    ffn_third = after(ffn_third, attn_far)
    ffn_held = [jnp.concatenate(pair, axis=0) for pair in zip(ffn_held, ffn_third)]
    ffn_third = [hop(held, k, 2) for k, held in enumerate(ffn_held)]
    total = collect_core(keep, send)
    ffn_third = after(ffn_third, total)
    ffn_held = [jnp.concatenate(pair, axis=0) for pair in zip(ffn_held, ffn_third)]
    ffn_far = [hop(held, k, 3) for k, held in enumerate(ffn_held)]
    mine, given = collect_x(total)
    middle = stream + layer_mod[2] * (mine + given.astype(F32))
    normed_second, rstd_second = normalize(middle)
    input_second = (normed_second * (1.0 + layer_mod[4]) + layer_mod[3]).astype(BF)
    second_rows = spread(input_second)
    ffn_far = after(ffn_far, second_rows)
    held_in, held_back = tuple(zip(ffn_held, ffn_far))

    activated, up_grad, send, keep = feed_forward(second_rows, down_rows, held_in, held_back, where)
    total = collect_core(keep, send)
    mine, given = collect_x(total)
    up_rows = after(up_grad, total)
    near_in, far_in = term_blocks("term_in", [(second_rows, up_rows)], where, 0, grad_scale)
    given_in = hop(far_in, 0, 3)
    back_second = mine + after(given, far_in).astype(F32)
    stream_grad = stream_grad + norm_back(
        normed_second, rstd_second, back_second * (1.0 + layer_mod[4])
    )
    attn_grad = (layer_mod[2] * stream_grad).astype(BF)
    act_rows = after(activated, attn_grad)
    near_back, far_back = term_blocks("term_back", [(down_rows, act_rows)], where, 1, grad_scale)
    given_back = hop(far_back, 1, 3)
    attn_rows = after(spread(attn_grad), far_back)
    grad_qk, grad_v, send, keep = attention_back(
        attn_rows, queries_keys, values, held_qk, held_vo, where
    )
    total = collect_core(keep, send)
    mine, given = collect_x(total)
    grad_qk, grad_v, attended = after((grad_qk, grad_v, attended), total)
    near_qk, far_qk = term_blocks("term_qk", [(first_rows, grad_qk)], where, 0, grad_scale)
    given_qk = hop(far_qk, 0, 3)
    products = [(first_rows, grad_v), (attn_rows, attended)]
    near_vo, far_vo = term_blocks("term_vo", products, where, 1, grad_scale)
    given_vo = hop(far_vo, 1, 3)

    given_in, given_back = after((given_in, given_back), grad_qk)
    two_in, two_back = fold(near_in, given_in), fold(near_back, given_back)
    send_in, send_back = hop(two_in[1], 0, 2), hop(two_back[1], 1, 2)
    given_qk, given_vo = after((given_qk, given_vo), two_in, two_back)
    two_qk, two_vo = fold(near_qk, given_qk), fold(near_vo, given_vo)
    send_qk, send_vo = hop(two_qk[1], 0, 2), hop(two_vo[1], 1, 2)

    back_first = mine + after(given, far_vo).astype(F32)
    input_grad = stream_grad + norm_back(
        normed_first, rstd_first, back_first * (1.0 + layer_mod[1])
    )

    late = after(activated, two_in, two_back, two_qk, two_vo)
    send, keep = down_project(late, held_back, where)
    mine, given = collect_x(collect_core(keep, send))
    final_out = (middle + layer_mod[5] * (mine + given.astype(F32))).astype(BF)

    def rest(two, given, k):
        two = fold(two[0], given)
        two = fold(two[0], hop(two[1], k, 1))
        return two[0].astype(F32), hop(two[1], k, 0)

    done = [
        rest(two_qk, send_qk, 0),
        rest(two_vo, send_vo, 1),
        rest(two_in, send_in, 0),
        rest(two_back, send_back, 1),
    ]
    parts = [near + given.astype(F32) for near, given in done]
    sum_attn, sum_ffn = last_sum(parts[:2]), last_sum(parts[2:])
    return (
        final_out,
        input_grad,
        sum_attn[:, : 3 * own_width],
        sum_attn[:, 3 * own_width :].T,
        sum_ffn[:, :ffn_width],
        sum_ffn[:, ffn_width:].T,
    )


def body(tokens, modulation, w_qkv, w_out, w_in, w_back, out_grad):
    local_seq = tokens.shape[1]
    own_width = w_qkv.shape[3]
    grad_scale = 1.0 / math.sqrt(local_seq * lax.axis_size(FSDP) * lax.axis_size(SP))
    final_out, input_grad, grad_qkv, grad_out, grad_in, grad_back = block_pass(
        tokens[0],
        modulation[0, 0],
        w_qkv[0].reshape(-1, 3 * own_width),
        w_out[0],
        w_in[0],
        w_back[0],
        out_grad[0],
        grad_scale,
    )
    return (
        final_out[None],
        input_grad[None],
        grad_qkv.reshape(1, -1, 3, own_width),
        grad_out[None],
        grad_in[None],
        grad_back[None],
    )


def solution(mesh):
    torus = Mesh(
        mesh.devices.reshape(4, 4, 2, 2, 2),
        (*FSDP, *SP),
    )
    return jax.shard_map(
        body,
        mesh=torus,
        in_specs=(
            P(FSDP, SP, None),
            P(FSDP, None, None, None),
            P(None, FSDP, None, SP),
            P(None, SP, FSDP),
            P(None, FSDP, SP),
            P(None, SP, FSDP),
            P(FSDP, SP, None),
        ),
        out_specs=(
            P(FSDP, SP, None),
            P(FSDP, SP, None),
            P(None, FSDP, None, SP),
            P(None, SP, FSDP),
            P(None, FSDP, SP),
            P(None, SP, FSDP),
        ),
        check_vma=False,
    )
```

```python
import math

import jax
import jax.numpy as jnp
from jax import lax
from jax.experimental import pallas as pl
from jax.experimental.pallas import tpu as pltpu
from jax.sharding import Mesh
from jax.sharding import PartitionSpec as P

HEAD_DIM = 128
ZY = ("fsdp_z", "fsdp_y")
FSDP = (*ZY, "fsdp_x")
SP = ("sp_x", "sp_core")
SWAP = ((0, 1), (1, 0))
GRID = (*ZY, "sp_core")
PLACES = 16
NEAR_FLIPS, WIDE_FLIPS = (1, 4), (3, 12)
STEPS = 4

ln_eps = 1e-06
temper = 2.5
BF = jnp.bfloat16
F32 = jnp.float32


def normalize(stream):
    mean_part = jnp.mean(stream, axis=-1, keepdims=True)
    centred = stream - mean_part
    rstd = lax.rsqrt(jnp.mean(centred * centred, axis=-1, keepdims=True) + ln_eps)
    return (centred * rstd, rstd)


def norm_back(normed, rstd, incoming):
    first = jnp.mean(incoming, axis=-1, keepdims=True)
    second = jnp.mean(incoming * normed, axis=-1, keepdims=True)
    return rstd * (incoming - first - normed * second)


def dot_nn(left, right):
    return jnp.dot(left, right, preferred_element_type=F32)


def dot_nt(left, right):
    return lax.dot_general(left, right, (((1,), (1,)), ((), ())), preferred_element_type=F32)


def dot_tn(left, right):
    return lax.dot_general(left, right, (((0,), (0,)), ((), ())), preferred_element_type=F32)


def swap(value, axis):
    return lax.ppermute(value, axis, SWAP)


def after(value, *earlier):
    return lax.optimization_barrier((value, earlier))[0]


def spread(own):
    pair = jnp.concatenate([own, swap(own, "sp_x")], axis=0)
    return pair, swap(pair, "sp_core")


def collect(keep, give):
    rows = keep.shape[0] // 2
    given = swap(give, "sp_core")
    send = (keep[rows:] + given[rows:].astype(F32)).astype(BF)
    return send, keep[:rows] + given[:rows].astype(F32)


def ordered(own, other, axis):
    first = jnp.concatenate([own, other], axis=0)
    second = jnp.concatenate([other, own], axis=0)
    return jnp.where(lax.axis_index(axis) == 0, first, second)


def flip_of(step, stream, core):
    inner = NEAR_FLIPS if core == (step >= 2) else WIDE_FLIPS
    return inner[(step % 2) ^ (stream if step >= 2 else 0)]


def hop(value, step, stream=0):
    pairs = []
    for place in range(PLACES):
        for core in range(2):
            pairs.append((2 * place + core, 2 * (place ^ flip_of(step, stream, core)) + core))
    return lax.ppermute(value, GRID, pairs)


def place_of(where_ref, stream):
    core = where_ref[1]
    flips = []
    for step in range(STEPS):
        flips.append(
            jnp.where(core == 0, flip_of(step, stream, 0), flip_of(step, stream, 1))
        )

    def at(rank):
        place = where_ref[0]
        for step in range(STEPS):
            if rank >> step & 1:
                place = place ^ flips[step]
        return place

    return at


def local_call(kernel, name, outs, scratch, where, arrays, remote=()):
    vmem, hbm = pl.BlockSpec(memory_space=pltpu.VMEM), pl.BlockSpec(memory_space=pltpu.HBM)
    return pl.pallas_call(
        kernel,
        in_specs=[pl.BlockSpec(memory_space=pltpu.SMEM)]
        + [vmem] * len(arrays)
        + [hbm] * len(remote),
        out_specs=[vmem] * len(outs),
        out_shape=[jax.ShapeDtypeStruct(shape, kind) for shape, kind in outs],
        scratch_shapes=scratch,
        name=name,
        compiler_params=pltpu.CompilerParams(vmem_limit_bytes=56 * 1024 * 1024),
    )(where, *arrays, *remote)


def placed_load(where_ref, held, target, sems, stream):
    near, far = held
    half = PLACES // 2
    block = target.shape[0] // PLACES
    at = place_of(where_ref, stream)
    copies = []
    for rank in range(PLACES):
        source = near if rank < half else far
        copies.append(
            pltpu.make_async_copy(
                source.at[pl.ds(rank % half * block, block), :],
                target.at[pl.ds(pl.multiple_of(at(rank) * block, block), block), :],
                sems.at[rank],
            )
        )
    for copy in copies:
        copy.start()
    return copies


def finish(copies):
    for copy in copies:
        copy.wait()


def column_cuts(widths):
    at, cuts = 0, []
    for width in widths:
        cuts.append(slice(at, at + width))
        at += width
    return cuts


def join(held, given):
    return jnp.concatenate([held, given], axis=0)


def part_join(held, given, cuts):
    return [join(held[:, cut], given[:, cut]) for cut in cuts]


def term_blocks(name, products, where, stream, grad_scale):
    lefts = [half for left, _ in products for half in left]
    rights = [right for _, right in products]
    height = lefts[0].shape[1]
    cuts = column_cuts([right.shape[1] for right in rights])
    width = cuts[-1].stop
    block = height // PLACES
    half = PLACES // 2
    strip = height // 4

    def kernel(where_ref, *refs):
        left_refs, refs = refs[: len(lefts)], refs[len(lefts) :]
        right_refs, (near_ref, far_ref, whole) = refs[: len(rights)], refs[len(rights) :]
        at = place_of(where_ref, stream)
        for number, cut in enumerate(cuts):
            upper, lower = left_refs[2 * number : 2 * number + 2]
            rows = upper.shape[0]
            for k in range(4):
                part = slice(k * strip, (k + 1) * strip)
                total = dot_tn(upper[:, part], right_refs[number][:rows, :])
                total = total + dot_tn(lower[:, part], right_refs[number][rows:, :])
                whole[part, cut] = (total * grad_scale).astype(BF)
        for rank in range(PLACES):
            source = pl.ds(pl.multiple_of(at(rank) * block, block), block)
            out = near_ref if rank < half else far_ref
            out[pl.ds(rank % half * block, block), :] = whole[source, :]

    outs = [((height // 2, width), BF)] * 2
    scratch = [pltpu.VMEM((height, width), BF)]
    return local_call(kernel, name, outs, scratch, where, (*lefts, *rights))


def add(near, given):
    return near.astype(F32) + given.astype(F32)


def fold(near, given):
    half = near.shape[0] // 2
    send = add(near[half:], given[half:]).astype(BF)
    return add(near[:half], given[:half]).astype(BF), send


def fold_joined(nears, givens):
    halves = [fold(near, given) for near, given in zip(nears, givens)]
    return [jnp.concatenate(part, axis=1) for part in zip(*halves)]


def last_sum(joined):
    half = joined.shape[0] // 2
    low, high = joined[:half], joined[half:]
    at_low = lax.axis_index("fsdp_x") == 0
    given = swap(jnp.where(at_low, high, low).astype(BF), "fsdp_x")
    return jnp.where(at_low, low, high) + given.astype(F32)


def split_rows(where_rows, send_ref, keep_ref, value_of):
    half = where_rows // 2
    send_ref[...] = value_of(slice(half, None)).astype(BF)
    keep_ref[...] = value_of(slice(None, half))


def attend_probs(queries, keys):
    factor = temper / math.sqrt(HEAD_DIM)
    scores = dot_nt(queries, keys) * factor
    lifted = jnp.exp(scores - jnp.max(scores, axis=-1, keepdims=True))
    return lifted / jnp.sum(lifted, axis=-1, keepdims=True)


def held_scratch(held):
    return [
        pltpu.VMEM((2 * held[0].shape[0], held[0].shape[1]), BF),
        pltpu.SemaphoreType.DMA((PLACES,)),
    ]


def attention(rows, held_qk, held_vo, where):
    width = held_vo[0].shape[1] // 2
    count = 2 * rows[0].shape[0]
    model = rows[0].shape[1]

    def kernel(where_ref, upper, lower, near0, far0, near1, far1, *refs):
        qk_ref, v_ref, o_ref, send_ref, keep_ref, w0, sems0, w1, sems1 = refs
        first = placed_load(where_ref, (near0, far0), w0, sems0, 0)
        second = placed_load(where_ref, (near1, far1), w1, sems1, 1)
        half = count // 2
        finish(first)
        qk_ref[:half, :] = dot_nn(upper[...], w0[...]).astype(BF)
        qk_ref[half:, :] = dot_nn(lower[...], w0[...]).astype(BF)
        finish(second)
        v_ref[:half, :] = dot_nn(upper[...], w1[:, :width]).astype(BF)
        v_ref[half:, :] = dot_nn(lower[...], w1[:, :width]).astype(BF)
        for at in range(0, width, HEAD_DIM):
            head = slice(at, at + HEAD_DIM)
            probs = attend_probs(qk_ref[:, head], qk_ref[:, width + at : width + at + HEAD_DIM])
            o_ref[:, head] = dot_nn(probs.astype(BF), v_ref[:, head]).astype(BF)
        split_rows(count, send_ref, keep_ref, lambda span: dot_nt(o_ref[span, :], w1[:, width:]))

    outs = [
        ((count, 2 * width), BF),
        ((count, width), BF),
        ((count, width), BF),
        ((count // 2, model), BF),
        ((count // 2, model), F32),
    ]
    scratch = held_scratch(held_qk) + held_scratch(held_vo)
    return local_call(kernel, "attention", outs, scratch, where, rows, (*held_qk, *held_vo))


def attention_back(rows, queries_keys, values, held_qk, held_vo, where):
    width = values.shape[1]
    count = values.shape[0]
    model = rows[0].shape[1]
    factor = temper / math.sqrt(HEAD_DIM)

    def kernel(where_ref, upper, lower, qk_ref, v_ref, near0, far0, near1, far1, *refs):
        dqk_ref, dv_ref, send_ref, keep_ref, mixed, w0, sems0, w1, sems1 = refs
        second = placed_load(where_ref, (near1, far1), w1, sems1, 1)
        first = placed_load(where_ref, (near0, far0), w0, sems0, 0)
        half = count // 2
        finish(second)
        mixed[:half, :] = dot_nn(upper[...], w1[:, width:]).astype(BF)
        mixed[half:, :] = dot_nn(lower[...], w1[:, width:]).astype(BF)
        for at in range(0, width, HEAD_DIM):
            head = slice(at, at + HEAD_DIM)
            key_head = slice(width + at, width + at + HEAD_DIM)
            upstream = mixed[:, head]
            probs = attend_probs(qk_ref[:, head], qk_ref[:, key_head])
            dprobs = dot_nt(upstream, v_ref[:, head])
            inner = jnp.sum(probs * dprobs, axis=-1, keepdims=True)
            dscores = (probs * (dprobs - inner) * factor).astype(BF)
            dqk_ref[:, head] = dot_nn(dscores, qk_ref[:, key_head]).astype(BF)
            dqk_ref[:, key_head] = dot_tn(dscores, qk_ref[:, head]).astype(BF)
            dv_ref[:, head] = dot_tn(probs.astype(BF), upstream).astype(BF)
        finish(first)

        def part(span):
            return dot_nt(dqk_ref[span, :], w0[...]) + dot_nt(dv_ref[span, :], w1[:, :width])

        split_rows(count, send_ref, keep_ref, part)

    outs = [
        ((count, 2 * width), BF),
        ((count, width), BF),
        ((count // 2, model), BF),
        ((count // 2, model), F32),
    ]
    scratch = [pltpu.VMEM((count, width), BF)] + held_scratch(held_qk) + held_scratch(held_vo)
    arrays = (*rows, queries_keys, values)
    return local_call(kernel, "attention_back", outs, scratch, where, arrays, (*held_qk, *held_vo))


def gelu_pair(hidden):
    root, cube = math.sqrt(2.0 / math.pi), 0.044715
    square = hidden * hidden
    curve = jnp.tanh(root * (hidden + cube * (square * hidden)))
    rise = 0.5 * (1.0 + curve)
    slope = 0.5 * hidden * (1.0 - curve * curve) * (root * (1.0 + 3.0 * cube * square))
    return hidden * rise, rise + slope


def feed_forward(rows, down_rows, held_in, held_back, where):
    width = held_in[0].shape[1]
    count = 2 * rows[0].shape[0]
    model = rows[0].shape[1]
    strip = width // 4

    def kernel(where_ref, upper, lower, d_upper, d_lower, near0, far0, near1, far1, *refs):
        act_ref, up_ref, send_ref, keep_ref, w0, sems0, w1, sems1 = refs
        first = placed_load(where_ref, (near0, far0), w0, sems0, 0)
        second = placed_load(where_ref, (near1, far1), w1, sems1, 1)
        half = count // 2
        finish(first)
        finish(second)
        for k in range(4):
            part = slice(k * strip, (k + 1) * strip)
            for at, left, down in ((0, upper, d_upper), (half, lower, d_lower)):
                active, slope = gelu_pair(dot_nn(left[...], w0[:, part]))
                act_ref[at : at + half, part] = active.astype(BF)
                grad = slope * dot_nn(down[...], w1[:, part])
                up_ref[at : at + half, part] = grad.astype(BF)
        split_rows(count, send_ref, keep_ref, lambda span: dot_nt(up_ref[span, :], w0[...]))

    outs = [
        ((count, width), BF),
        ((count, width), BF),
        ((count // 2, model), BF),
        ((count // 2, model), F32),
    ]
    scratch = held_scratch(held_in) + held_scratch(held_back)
    arrays = (*rows, *down_rows)
    return local_call(kernel, "feed_forward", outs, scratch, where, arrays, (*held_in, *held_back))


def down_project(activated, held_back, where):
    count = activated.shape[0]
    model = 2 * held_back[0].shape[0]

    def kernel(where_ref, act_ref, near, far, send_ref, keep_ref, w1, sems):
        finish(placed_load(where_ref, (near, far), w1, sems, 1))
        split_rows(count, send_ref, keep_ref, lambda span: dot_nt(act_ref[span, :], w1[...]))

    outs = [((count // 2, model), BF), ((count // 2, model), F32)]
    scratch = held_scratch(held_back)
    return local_call(kernel, "down_project", outs, scratch, where, (activated,), held_back)


def pair_up(own):
    return ordered(own, swap(own, "fsdp_x"), "fsdp_x")


def block_pass(tokens, layer_mod, w_qkv, w_out, w_in, w_back, out_grad, grad_scale):
    own_width, ffn_width = w_out.shape[0], w_in.shape[1]
    where = jnp.stack([lax.axis_index(ZY), lax.axis_index("sp_core")]).astype(jnp.int32)
    cut = 2 * own_width
    attn_pair = pair_up(jnp.concatenate([w_qkv, w_out.T], axis=1))
    ffn_own = after(jnp.concatenate([w_in, w_back.T], axis=1), attn_pair)
    ffn_pair = pair_up(ffn_own)

    stream = tokens.astype(F32)
    normed_first, rstd_first = normalize(stream)
    input_first = (normed_first * (1.0 + layer_mod[1]) + layer_mod[0]).astype(BF)

    attn_cuts = column_cuts((cut, 2 * own_width))
    ffn_cuts = column_cuts((ffn_width, ffn_width))
    attn_held = join(attn_pair, hop(attn_pair, 0))
    input_first = after(input_first, ffn_pair)
    first_rows = spread(input_first)
    attn_given = hop(attn_held, 1)
    ffn_pair = after(ffn_pair, attn_held)
    ffn_held = join(ffn_pair, hop(ffn_pair, 0))
    attn_held = part_join(attn_held, attn_given, attn_cuts)
    attn_held = [join(held, hop(held, 2, k)) for k, held in enumerate(attn_held)]
    ffn_held = after(ffn_held, attn_held)
    attn_far = [hop(held, 3, k) for k, held in enumerate(attn_held)]
    ffn_given = hop(ffn_held, 1)

    out_grad = after(out_grad, first_rows)
    stream_grad = out_grad.astype(F32)
    down_grad = (layer_mod[5] * stream_grad).astype(BF)
    down_rows = spread(down_grad)

    ffn_given = after(ffn_given, attn_far)
    ffn_held = part_join(ffn_held, ffn_given, ffn_cuts)
    ffn_given = [hop(held, 2, k) for k, held in enumerate(ffn_held)]
    attn_far = after(attn_far, ffn_held)
    held_qk, held_vo = tuple(zip(attn_held, attn_far))
    first_rows = after(first_rows, down_rows)
    queries_keys, values, attended, send, keep = attention(first_rows, held_qk, held_vo, where)
    send, mine = collect(keep, send)
    ffn_given = after(ffn_given, send)
    ffn_held = [join(*pair) for pair in zip(ffn_held, ffn_given)]
    ffn_far = [hop(held, 3, k) for k, held in enumerate(ffn_held)]
    given = swap(send, "sp_x")
    middle = stream + layer_mod[2] * (mine + given.astype(F32))
    normed_second, rstd_second = normalize(middle)
    input_second = (normed_second * (1.0 + layer_mod[4]) + layer_mod[3]).astype(BF)
    second_rows = spread(input_second)
    ffn_far = after(ffn_far, second_rows)
    held_in, held_back = tuple(zip(ffn_held, ffn_far))

    activated, up_grad, send, keep = feed_forward(second_rows, down_rows, held_in, held_back, where)
    send, mine = collect(keep, send)
    up_rows = after(up_grad, send)
    near_in, far_in = term_blocks("term_in", [(second_rows, up_rows)], where, 0, grad_scale)
    given_in = hop(far_in, 3, 0)
    back_second = mine + after(swap(send, "sp_x"), far_in).astype(F32)
    stream_grad = stream_grad + norm_back(
        normed_second, rstd_second, back_second * (1.0 + layer_mod[4])
    )
    attn_grad = (layer_mod[2] * stream_grad).astype(BF)
    act_rows = after(activated, attn_grad)
    near_back, far_back = term_blocks("term_back", [(down_rows, act_rows)], where, 1, grad_scale)
    given_back = hop(far_back, 3, 1)
    attn_rows = after(spread(attn_grad), far_back)
    grad_qk, grad_v, send, keep = attention_back(
        attn_rows, queries_keys, values, held_qk, held_vo, where
    )
    send, mine = collect(keep, send)
    grad_qk, grad_v, attended = after((grad_qk, grad_v, attended), send)
    near_qk, far_qk = term_blocks("term_qk", [(first_rows, grad_qk)], where, 0, grad_scale)
    given_qk = hop(far_qk, 3, 0)
    given_in = after(given_in, far_qk)
    two_in = fold(near_in, given_in)
    send_in = hop(two_in[1], 2, 0)
    grad_v, attended = after((grad_v, attended), two_in)
    products = [(first_rows, grad_v), (attn_rows, attended)]
    near_vo, far_vo = term_blocks("term_vo", products, where, 1, grad_scale)
    given_vo = hop(far_vo, 3, 1)
    given_back = after(given_back, far_vo)
    two_back = fold(near_back, given_back)
    send_back = hop(two_back[1], 2, 1)

    back_first = mine + after(swap(send, "sp_x"), two_back).astype(F32)
    input_grad = stream_grad + norm_back(
        normed_first, rstd_first, back_first * (1.0 + layer_mod[1])
    )
    late = after(activated, two_back, input_grad)
    send, keep = down_project(late, held_back, where)

    given_qk, given_vo = after((given_qk, given_vo), keep)
    two_qk, two_vo = fold(near_qk, given_qk), fold(near_vo, given_vo)
    send_qk, send_vo = hop(two_qk[1], 2, 0), hop(two_vo[1], 2, 1)
    send, mine = collect(keep, send)
    send_in, send_back = after((send_in, send_back), two_qk, two_vo, send)
    near_ffn, send_ffn = fold_joined((two_in[0], two_back[0]), (send_in, send_back))
    given_ffn = hop(send_ffn, 1)
    final_out = (middle + layer_mod[5] * (mine + swap(send, "sp_x").astype(F32))).astype(BF)
    send_qk, send_vo = after((send_qk, send_vo), send_ffn)
    near_attn, send_attn = fold_joined((two_qk[0], two_vo[0]), (send_qk, send_vo))
    given_attn = hop(send_attn, 1)
    near_ffn, send_ffn = fold(near_ffn, after(given_ffn, send_attn))
    given_ffn = hop(send_ffn, 0)
    near_attn, send_attn = fold(near_attn, after(given_attn, send_ffn))
    given_attn = hop(send_attn, 0)
    sum_ffn = last_sum(add(near_ffn, after(given_ffn, send_attn)))
    sum_attn = last_sum(add(near_attn, given_attn))
    return (
        final_out,
        input_grad,
        sum_attn[:, : 3 * own_width],
        sum_attn[:, 3 * own_width :].T,
        sum_ffn[:, :ffn_width],
        sum_ffn[:, ffn_width:].T,
    )


def body(tokens, modulation, w_qkv, w_out, w_in, w_back, out_grad):
    local_seq = tokens.shape[1]
    own_width = w_qkv.shape[3]
    grad_scale = 1.0 / math.sqrt(local_seq * lax.axis_size(FSDP) * lax.axis_size(SP))
    final_out, input_grad, grad_qkv, grad_out, grad_in, grad_back = block_pass(
        tokens[0],
        modulation[0, 0],
        w_qkv[0].reshape(-1, 3 * own_width),
        w_out[0],
        w_in[0],
        w_back[0],
        out_grad[0],
        grad_scale,
    )
    return (
        final_out[None],
        input_grad[None],
        grad_qkv.reshape(1, -1, 3, own_width),
        grad_out[None],
        grad_in[None],
        grad_back[None],
    )


def solution(mesh):
    torus = Mesh(
        mesh.devices.reshape(4, 4, 2, 2, 2),
        (*FSDP, *SP),
    )
    return jax.shard_map(
        body,
        mesh=torus,
        in_specs=(
            P(FSDP, SP, None),
            P(FSDP, None, None, None),
            P(None, FSDP, None, SP),
            P(None, SP, FSDP),
            P(None, FSDP, SP),
            P(None, SP, FSDP),
            P(FSDP, SP, None),
        ),
        out_specs=(
            P(FSDP, SP, None),
            P(FSDP, SP, None),
            P(None, FSDP, None, SP),
            P(None, SP, FSDP),
            P(None, FSDP, SP),
            P(None, SP, FSDP),
        ),
        check_vma=False,
    )
```

```python
import math

import jax
import jax.numpy as jnp
from jax import lax
from jax.experimental import pallas as pl
from jax.experimental.pallas import tpu as pltpu
from jax.sharding import Mesh
from jax.sharding import PartitionSpec as P

HEAD_DIM = 128
ZY = ("fsdp_z", "fsdp_y")
FSDP = (*ZY, "fsdp_x")
SP = ("sp_x", "sp_core")
SWAP = ((0, 1), (1, 0))
GRID = (*ZY, "sp_core")
PLACES = 16
NEAR_FLIPS, WIDE_FLIPS = (1, 4), (3, 12)
STEPS = 4

ln_eps = 1e-06
temper = 2.5
BF = jnp.bfloat16
F32 = jnp.float32


def normalize(stream):
    mean_part = jnp.mean(stream, axis=-1, keepdims=True)
    centred = stream - mean_part
    rstd = lax.rsqrt(jnp.mean(centred * centred, axis=-1, keepdims=True) + ln_eps)
    return (centred * rstd, rstd)


def norm_back(normed, rstd, incoming):
    first = jnp.mean(incoming, axis=-1, keepdims=True)
    second = jnp.mean(incoming * normed, axis=-1, keepdims=True)
    return rstd * (incoming - first - normed * second)


def dot_nn(left, right):
    return jnp.dot(left, right, preferred_element_type=F32)


def dot_nt(left, right):
    return lax.dot_general(left, right, (((1,), (1,)), ((), ())), preferred_element_type=F32)


def dot_tn(left, right):
    return lax.dot_general(left, right, (((0,), (0,)), ((), ())), preferred_element_type=F32)


def swap(value, axis):
    return lax.ppermute(value, axis, SWAP)


def after(value, *earlier):
    return lax.optimization_barrier((value, earlier))[0]


def spread(own):
    pair = jnp.concatenate([own, swap(own, "sp_x")], axis=0)
    return pair, swap(pair, "sp_core")


def collect(keep, give):
    rows = keep.shape[0] // 2
    given = swap(give, "sp_core")
    send = (keep[rows:] + given[rows:].astype(F32)).astype(BF)
    return send, keep[:rows] + given[:rows].astype(F32)


def ordered(own, other, axis):
    first = jnp.concatenate([own, other], axis=0)
    second = jnp.concatenate([other, own], axis=0)
    return jnp.where(lax.axis_index(axis) == 0, first, second)


def flip_of(step, stream, core):
    inner = NEAR_FLIPS if core == (step >= 2) else WIDE_FLIPS
    return inner[(step % 2) ^ (stream if step >= 2 else 0)]


def hop(value, step, stream=0):
    pairs = []
    for place in range(PLACES):
        for core in range(2):
            pairs.append((2 * place + core, 2 * (place ^ flip_of(step, stream, core)) + core))
    return lax.ppermute(value, GRID, pairs)


def place_of(where_ref, stream):
    core = where_ref[1]
    flips = []
    for step in range(STEPS):
        flips.append(
            jnp.where(core == 0, flip_of(step, stream, 0), flip_of(step, stream, 1))
        )

    def at(rank):
        place = where_ref[0]
        for step in range(STEPS):
            if rank >> step & 1:
                place = place ^ flips[step]
        return place

    return at


def local_call(kernel, outs, scratch, where, arrays, remote=()):
    vmem, hbm = pl.BlockSpec(memory_space=pltpu.VMEM), pl.BlockSpec(memory_space=pltpu.HBM)
    return pl.pallas_call(
        kernel,
        in_specs=[pl.BlockSpec(memory_space=pltpu.SMEM)]
        + [vmem] * len(arrays)
        + [hbm] * len(remote),
        out_specs=[vmem] * len(outs),
        out_shape=[jax.ShapeDtypeStruct(shape, kind) for shape, kind in outs],
        scratch_shapes=scratch,
        compiler_params=pltpu.CompilerParams(vmem_limit_bytes=56 * 1024 * 1024),
    )(where, *arrays, *remote)


def placed_load(where_ref, held, target, sems, stream):
    near, far = held
    half = PLACES // 2
    block = target.shape[0] // PLACES
    at = place_of(where_ref, stream)
    copies = []
    for rank in range(PLACES):
        source = near if rank < half else far
        copies.append(
            pltpu.make_async_copy(
                source.at[pl.ds(rank % half * block, block), :],
                target.at[pl.ds(pl.multiple_of(at(rank) * block, block), block), :],
                sems.at[rank],
            )
        )
    for copy in copies:
        copy.start()
    return copies


def finish(copies):
    for copy in copies:
        copy.wait()


def column_cuts(widths):
    at, cuts = 0, []
    for width in widths:
        cuts.append(slice(at, at + width))
        at += width
    return cuts


def join(held, given):
    return jnp.concatenate([held, given], axis=0)


def part_join(held, given, cuts):
    return [join(held[:, cut], given[:, cut]) for cut in cuts]


def term_blocks(products, where, stream, grad_scale):
    lefts = [half for left, _ in products for half in left]
    rights = [right for _, right in products]
    height = lefts[0].shape[1]
    cuts = column_cuts([right.shape[1] for right in rights])
    width = cuts[-1].stop
    block = height // PLACES
    half = PLACES // 2
    strip = height // 4

    def kernel(where_ref, *refs):
        left_refs, refs = refs[: len(lefts)], refs[len(lefts) :]
        right_refs, (near_ref, far_ref, whole) = refs[: len(rights)], refs[len(rights) :]
        at = place_of(where_ref, stream)
        for number, cut in enumerate(cuts):
            upper, lower = left_refs[2 * number : 2 * number + 2]
            rows = upper.shape[0]
            for k in range(4):
                part = slice(k * strip, (k + 1) * strip)
                total = dot_tn(upper[:, part], right_refs[number][:rows, :])
                total = total + dot_tn(lower[:, part], right_refs[number][rows:, :])
                whole[part, cut] = (total * grad_scale).astype(BF)
        for rank in range(PLACES):
            source = pl.ds(pl.multiple_of(at(rank) * block, block), block)
            out = near_ref if rank < half else far_ref
            out[pl.ds(rank % half * block, block), :] = whole[source, :]

    outs = [((height // 2, width), BF)] * 2
    scratch = [pltpu.VMEM((height, width), BF)]
    return local_call(kernel, outs, scratch, where, (*lefts, *rights))


def add(near, given):
    return near.astype(F32) + given.astype(F32)


def fold(near, given):
    half = near.shape[0] // 2
    send = add(near[half:], given[half:]).astype(BF)
    return add(near[:half], given[:half]).astype(BF), send


def fold_joined(nears, givens):
    halves = [fold(near, given) for near, given in zip(nears, givens)]
    return [jnp.concatenate(part, axis=1) for part in zip(*halves)]


def last_sum(joined):
    half = joined.shape[0] // 2
    low, high = joined[:half], joined[half:]
    at_low = lax.axis_index("fsdp_x") == 0
    given = swap(jnp.where(at_low, high, low).astype(BF), "fsdp_x")
    return jnp.where(at_low, low, high) + given.astype(F32)


def split_rows(where_rows, send_ref, keep_ref, value_of):
    half = where_rows // 2
    send_ref[...] = value_of(slice(half, None)).astype(BF)
    keep_ref[...] = value_of(slice(None, half))


def attend_probs(queries, keys):
    factor = temper / math.sqrt(HEAD_DIM)
    scores = dot_nt(queries, keys) * factor
    lifted = jnp.exp(scores - jnp.max(scores, axis=-1, keepdims=True))
    return lifted / jnp.sum(lifted, axis=-1, keepdims=True)


def held_scratch(held):
    return [
        pltpu.VMEM((2 * held[0].shape[0], held[0].shape[1]), BF),
        pltpu.SemaphoreType.DMA((PLACES,)),
    ]


def attention(rows, held_qk, held_vo, where):
    width = held_vo[0].shape[1] // 2
    count = 2 * rows[0].shape[0]
    model = rows[0].shape[1]

    def kernel(where_ref, upper, lower, near0, far0, near1, far1, *refs):
        qk_ref, v_ref, o_ref, send_ref, keep_ref, w0, sems0, w1, sems1 = refs
        first = placed_load(where_ref, (near0, far0), w0, sems0, 0)
        second = placed_load(where_ref, (near1, far1), w1, sems1, 1)
        half = count // 2
        finish(first)
        qk_ref[:half, :] = dot_nn(upper[...], w0[...]).astype(BF)
        qk_ref[half:, :] = dot_nn(lower[...], w0[...]).astype(BF)
        finish(second)
        v_ref[:half, :] = dot_nn(upper[...], w1[:, :width]).astype(BF)
        v_ref[half:, :] = dot_nn(lower[...], w1[:, :width]).astype(BF)
        for at in range(0, width, HEAD_DIM):
            head = slice(at, at + HEAD_DIM)
            probs = attend_probs(qk_ref[:, head], qk_ref[:, width + at : width + at + HEAD_DIM])
            o_ref[:, head] = dot_nn(probs.astype(BF), v_ref[:, head]).astype(BF)
        split_rows(count, send_ref, keep_ref, lambda span: dot_nt(o_ref[span, :], w1[:, width:]))

    outs = [
        ((count, 2 * width), BF),
        ((count, width), BF),
        ((count, width), BF),
        ((count // 2, model), BF),
        ((count // 2, model), F32),
    ]
    scratch = held_scratch(held_qk) + held_scratch(held_vo)
    return local_call(kernel, outs, scratch, where, rows, (*held_qk, *held_vo))


def attention_back(rows, queries_keys, values, held_qk, held_vo, where):
    width = values.shape[1]
    count = values.shape[0]
    model = rows[0].shape[1]
    factor = temper / math.sqrt(HEAD_DIM)

    def kernel(where_ref, upper, lower, qk_ref, v_ref, near0, far0, near1, far1, *refs):
        dqk_ref, dv_ref, send_ref, keep_ref, mixed, w0, sems0, w1, sems1 = refs
        second = placed_load(where_ref, (near1, far1), w1, sems1, 1)
        first = placed_load(where_ref, (near0, far0), w0, sems0, 0)
        half = count // 2
        finish(second)
        mixed[:half, :] = dot_nn(upper[...], w1[:, width:]).astype(BF)
        mixed[half:, :] = dot_nn(lower[...], w1[:, width:]).astype(BF)
        for at in range(0, width, HEAD_DIM):
            head = slice(at, at + HEAD_DIM)
            key_head = slice(width + at, width + at + HEAD_DIM)
            upstream = mixed[:, head]
            probs = attend_probs(qk_ref[:, head], qk_ref[:, key_head])
            dprobs = dot_nt(upstream, v_ref[:, head])
            inner = jnp.sum(probs * dprobs, axis=-1, keepdims=True)
            dscores = (probs * (dprobs - inner) * factor).astype(BF)
            dqk_ref[:, head] = dot_nn(dscores, qk_ref[:, key_head]).astype(BF)
            dqk_ref[:, key_head] = dot_tn(dscores, qk_ref[:, head]).astype(BF)
            dv_ref[:, head] = dot_tn(probs.astype(BF), upstream).astype(BF)
        finish(first)

        def part(span):
            return dot_nt(dqk_ref[span, :], w0[...]) + dot_nt(dv_ref[span, :], w1[:, :width])

        split_rows(count, send_ref, keep_ref, part)

    outs = [
        ((count, 2 * width), BF),
        ((count, width), BF),
        ((count // 2, model), BF),
        ((count // 2, model), F32),
    ]
    scratch = [pltpu.VMEM((count, width), BF)] + held_scratch(held_qk) + held_scratch(held_vo)
    arrays = (*rows, queries_keys, values)
    return local_call(kernel, outs, scratch, where, arrays, (*held_qk, *held_vo))


def gelu_pair(hidden):
    root, cube = math.sqrt(2.0 / math.pi), 0.044715
    square = hidden * hidden
    curve = jnp.tanh(root * (hidden + cube * (square * hidden)))
    rise = 0.5 * (1.0 + curve)
    slope = 0.5 * hidden * (1.0 - curve * curve) * (root * (1.0 + 3.0 * cube * square))
    return hidden * rise, rise + slope


def feed_forward(rows, down_rows, held_in, held_back, where):
    width = held_in[0].shape[1]
    count = 2 * rows[0].shape[0]
    model = rows[0].shape[1]
    strip = width // 4

    def kernel(where_ref, upper, lower, d_upper, d_lower, near0, far0, near1, far1, *refs):
        act_ref, up_ref, send_ref, keep_ref, w0, sems0, w1, sems1 = refs
        first = placed_load(where_ref, (near0, far0), w0, sems0, 0)
        second = placed_load(where_ref, (near1, far1), w1, sems1, 1)
        half = count // 2
        finish(first)
        finish(second)
        for k in range(4):
            part = slice(k * strip, (k + 1) * strip)
            for at, left, down in ((0, upper, d_upper), (half, lower, d_lower)):
                active, slope = gelu_pair(dot_nn(left[...], w0[:, part]))
                act_ref[at : at + half, part] = active.astype(BF)
                grad = slope * dot_nn(down[...], w1[:, part])
                up_ref[at : at + half, part] = grad.astype(BF)
        split_rows(count, send_ref, keep_ref, lambda span: dot_nt(up_ref[span, :], w0[...]))

    outs = [
        ((count, width), BF),
        ((count, width), BF),
        ((count // 2, model), BF),
        ((count // 2, model), F32),
    ]
    scratch = held_scratch(held_in) + held_scratch(held_back)
    arrays = (*rows, *down_rows)
    return local_call(kernel, outs, scratch, where, arrays, (*held_in, *held_back))


def down_project(activated, held_back, where):
    count = activated.shape[0]
    model = 2 * held_back[0].shape[0]

    def kernel(where_ref, act_ref, near, far, send_ref, keep_ref, w1, sems):
        finish(placed_load(where_ref, (near, far), w1, sems, 1))
        split_rows(count, send_ref, keep_ref, lambda span: dot_nt(act_ref[span, :], w1[...]))

    outs = [((count // 2, model), BF), ((count // 2, model), F32)]
    scratch = held_scratch(held_back)
    return local_call(kernel, outs, scratch, where, (activated,), held_back)


def pair_up(own):
    return ordered(own, swap(own, "fsdp_x"), "fsdp_x")


def block_pass(tokens, layer_mod, w_qkv, w_out, w_in, w_back, out_grad, grad_scale):
    own_width, ffn_width = w_out.shape[0], w_in.shape[1]
    where = jnp.stack([lax.axis_index(ZY), lax.axis_index("sp_core")]).astype(jnp.int32)
    cut = 2 * own_width
    attn_pair = pair_up(jnp.concatenate([w_qkv, w_out.T], axis=1))
    ffn_own = after(jnp.concatenate([w_in, w_back.T], axis=1), attn_pair)
    ffn_pair = pair_up(ffn_own)

    stream = tokens.astype(F32)
    normed_first, rstd_first = normalize(stream)
    input_first = (normed_first * (1.0 + layer_mod[1]) + layer_mod[0]).astype(BF)

    attn_cuts = column_cuts((cut, 2 * own_width))
    ffn_cuts = column_cuts((ffn_width, ffn_width))
    attn_held = join(attn_pair, hop(attn_pair, 0))
    input_first = after(input_first, ffn_pair)
    first_rows = spread(input_first)
    attn_given = hop(attn_held, 1)
    attn_held = part_join(attn_held, attn_given, attn_cuts)
    attn_given = [hop(held, 2, k) for k, held in enumerate(attn_held)]
    ffn_pair = after(ffn_pair, attn_held)
    ffn_held = join(ffn_pair, hop(ffn_pair, 0))
    attn_held = [join(*pair) for pair in zip(attn_held, attn_given)]
    attn_far = [hop(held, 3, k) for k, held in enumerate(attn_held)]
    ffn_held = after(ffn_held, attn_held)
    ffn_given = hop(ffn_held, 1)

    out_grad = after(out_grad, first_rows)
    stream_grad = out_grad.astype(F32)
    down_grad = (layer_mod[5] * stream_grad).astype(BF)
    down_rows = spread(down_grad)

    held_qk, held_vo = tuple(zip(attn_held, attn_far))
    first_rows = after(first_rows, down_rows)
    queries_keys, values, attended, send, keep = attention(first_rows, held_qk, held_vo, where)
    ffn_given = after(ffn_given, send)
    ffn_held = part_join(ffn_held, ffn_given, ffn_cuts)
    ffn_given = [hop(held, 2, k) for k, held in enumerate(ffn_held)]
    send, mine = collect(keep, send)
    ffn_given = after(ffn_given, send)
    ffn_held = [join(*pair) for pair in zip(ffn_held, ffn_given)]
    ffn_far = [hop(held, 3, k) for k, held in enumerate(ffn_held)]
    given = swap(send, "sp_x")
    middle = stream + layer_mod[2] * (mine + given.astype(F32))
    normed_second, rstd_second = normalize(middle)
    input_second = (normed_second * (1.0 + layer_mod[4]) + layer_mod[3]).astype(BF)
    second_rows = spread(input_second)
    ffn_far = after(ffn_far, second_rows)
    held_in, held_back = tuple(zip(ffn_held, ffn_far))

    activated, up_grad, send, keep = feed_forward(second_rows, down_rows, held_in, held_back, where)
    send, mine = collect(keep, send)
    up_rows = after(up_grad, send)
    near_in, far_in = term_blocks([(second_rows, up_rows)], where, 0, grad_scale)
    given_in = hop(far_in, 3, 0)
    back_second = mine + after(swap(send, "sp_x"), far_in).astype(F32)
    stream_grad = stream_grad + norm_back(
        normed_second, rstd_second, back_second * (1.0 + layer_mod[4])
    )
    attn_grad = (layer_mod[2] * stream_grad).astype(BF)
    act_rows = after(activated, attn_grad)
    near_back, far_back = term_blocks([(down_rows, act_rows)], where, 1, grad_scale)
    given_back = hop(far_back, 3, 1)
    attn_rows = after(spread(attn_grad), far_back)
    grad_qk, grad_v, send, keep = attention_back(
        attn_rows, queries_keys, values, held_qk, held_vo, where
    )
    given_in = after(given_in, send)
    two_in = fold(near_in, given_in)
    send_in = hop(two_in[1], 2, 0)
    send, mine = collect(keep, send)
    grad_qk, grad_v, attended = after((grad_qk, grad_v, attended), send)
    near_qk, far_qk = term_blocks([(first_rows, grad_qk)], where, 0, grad_scale)
    given_qk = hop(far_qk, 3, 0)
    given_back = after(given_back, far_qk)
    two_back = fold(near_back, given_back)
    send_back = hop(two_back[1], 2, 1)
    grad_v, attended = after((grad_v, attended), two_back)
    products = [(first_rows, grad_v), (attn_rows, attended)]
    near_vo, far_vo = term_blocks(products, where, 1, grad_scale)
    given_vo = hop(far_vo, 3, 1)

    back_first = mine + after(swap(send, "sp_x"), far_vo).astype(F32)
    input_grad = stream_grad + norm_back(
        normed_first, rstd_first, back_first * (1.0 + layer_mod[1])
    )
    late = after(activated, input_grad)
    send, keep = down_project(late, held_back, where)

    send_in, send_back = after((send_in, send_back), keep)
    near_ffn, send_ffn = fold_joined((two_in[0], two_back[0]), (send_in, send_back))
    given_ffn = hop(send_ffn, 1)
    given_qk, given_vo = after((given_qk, given_vo), send_ffn)
    two_qk, two_vo = fold(near_qk, given_qk), fold(near_vo, given_vo)
    send_qk, send_vo = hop(two_qk[1], 2, 0), hop(two_vo[1], 2, 1)
    send, mine = collect(keep, after(send, two_qk, two_vo))
    near_ffn, send_ffn = fold(near_ffn, after(given_ffn, send))
    given_ffn = hop(send_ffn, 0)
    send_qk, send_vo = after((send_qk, send_vo), send_ffn)
    near_attn, send_attn = fold_joined((two_qk[0], two_vo[0]), (send_qk, send_vo))
    given_attn = hop(send_attn, 1)
    total_ffn = add(near_ffn, after(given_ffn, send_attn))
    sum_ffn = last_sum(total_ffn)
    given = after(swap(send, "sp_x"), total_ffn)
    final_out = (middle + layer_mod[5] * (mine + given.astype(F32))).astype(BF)
    near_attn, send_attn = fold(near_attn, after(given_attn, final_out))
    given_attn = hop(send_attn, 0)
    sum_attn = last_sum(add(near_attn, given_attn))
    return (
        final_out,
        input_grad,
        sum_attn[:, : 3 * own_width],
        sum_attn[:, 3 * own_width :].T,
        sum_ffn[:, :ffn_width],
        sum_ffn[:, ffn_width:].T,
    )


def body(tokens, modulation, w_qkv, w_out, w_in, w_back, out_grad):
    local_seq = tokens.shape[1]
    own_width = w_qkv.shape[3]
    grad_scale = 1.0 / math.sqrt(local_seq * lax.axis_size(FSDP) * lax.axis_size(SP))
    final_out, input_grad, grad_qkv, grad_out, grad_in, grad_back = block_pass(
        tokens[0],
        modulation[0, 0],
        w_qkv[0].reshape(-1, 3 * own_width),
        w_out[0],
        w_in[0],
        w_back[0],
        out_grad[0],
        grad_scale,
    )
    return (
        final_out[None],
        input_grad[None],
        grad_qkv.reshape(1, -1, 3, own_width),
        grad_out[None],
        grad_in[None],
        grad_back[None],
    )


def solution(mesh):
    torus = Mesh(
        mesh.devices.reshape(4, 4, 2, 2, 2),
        (*FSDP, *SP),
    )
    return jax.shard_map(
        body,
        mesh=torus,
        in_specs=(
            P(FSDP, SP, None),
            P(FSDP, None, None, None),
            P(None, FSDP, None, SP),
            P(None, SP, FSDP),
            P(None, FSDP, SP),
            P(None, SP, FSDP),
            P(FSDP, SP, None),
        ),
        out_specs=(
            P(FSDP, SP, None),
            P(FSDP, SP, None),
            P(None, FSDP, None, SP),
            P(None, SP, FSDP),
            P(None, FSDP, SP),
            P(None, SP, FSDP),
        ),
        check_vma=False,
    )
```

```python
import math

import jax
import jax.numpy as jnp
from jax import lax
from jax.experimental import pallas as pl
from jax.experimental.pallas import tpu as pltpu
from jax.sharding import Mesh
from jax.sharding import PartitionSpec as P

HEAD_DIM = 128
ZY = ("fsdp_z", "fsdp_y")
FSDP = (*ZY, "fsdp_x")
SP = ("sp_x", "sp_core")
SWAP = ((0, 1), (1, 0))
GRID = (*ZY, "sp_core")
PLACES = 16
FLIPS = (1, 4, 3, 12)
STEPS = 4

ln_eps = 1e-06
temper = 2.5
BF = jnp.bfloat16
F32 = jnp.float32


def normalize(stream):
    mean_part = jnp.mean(stream, axis=-1, keepdims=True)
    centred = stream - mean_part
    rstd = lax.rsqrt(jnp.mean(centred * centred, axis=-1, keepdims=True) + ln_eps)
    return (centred * rstd, rstd)


def norm_back(normed, rstd, incoming):
    first = jnp.mean(incoming, axis=-1, keepdims=True)
    second = jnp.mean(incoming * normed, axis=-1, keepdims=True)
    return rstd * (incoming - first - normed * second)


def dot_nn(left, right):
    return jnp.dot(left, right, preferred_element_type=F32)


def dot_nt(left, right):
    return lax.dot_general(left, right, (((1,), (1,)), ((), ())), preferred_element_type=F32)


def dot_tn(left, right):
    return lax.dot_general(left, right, (((0,), (0,)), ((), ())), preferred_element_type=F32)


def swap(value, axis):
    return lax.ppermute(value, axis, SWAP)


def after(value, *earlier):
    return lax.optimization_barrier((value, earlier))[0]


def spread(own, *earlier):
    across = after(swap(own, "sp_x"), earlier)
    pair = jnp.concatenate([own, across], axis=0)
    return pair, swap(pair, "sp_core")


def collect(keep, give):
    rows = keep.shape[0] // 2
    given = swap(give, "sp_core")
    send = (keep[rows:] + given[rows:].astype(F32)).astype(BF)
    return send, keep[:rows] + given[:rows].astype(F32)


def ordered(own, other, axis):
    first = jnp.concatenate([own, other], axis=0)
    second = jnp.concatenate([other, own], axis=0)
    return jnp.where(lax.axis_index(axis) == 0, first, second)


def flip_of(turning, step, stream, core):
    if turning:
        return FLIPS[(2 * stream + core + step) % STEPS]
    inner = FLIPS[:2] if core == (step >= 2) else FLIPS[2:]
    return inner[(step % 2) ^ (stream if step >= 2 else 0)]


def hop(value, step, stream=0, turning=False):
    pairs = []
    for place in range(PLACES):
        for core in range(2):
            other = place ^ flip_of(turning, step, stream, core)
            pairs.append((2 * place + core, 2 * other + core))
    return lax.ppermute(value, GRID, pairs)


def place_of(where_ref, stream, turning):
    flips = []
    for step in range(STEPS):
        first, second = (flip_of(turning, step, stream, core) for core in range(2))
        flips.append(jnp.where(where_ref[1] == 0, first, second))

    def at(rank):
        place = where_ref[0]
        for step in range(STEPS):
            if rank >> step & 1:
                place = place ^ flips[step]
        return place

    return at


def local_call(kernel, outs, scratch, where, arrays, remote=()):
    vmem, hbm = pl.BlockSpec(memory_space=pltpu.VMEM), pl.BlockSpec(memory_space=pltpu.HBM)
    return pl.pallas_call(
        kernel,
        in_specs=[pl.BlockSpec(memory_space=pltpu.SMEM)]
        + [vmem] * len(arrays)
        + [hbm] * len(remote),
        out_specs=[vmem] * len(outs),
        out_shape=[jax.ShapeDtypeStruct(shape, kind) for shape, kind in outs],
        scratch_shapes=scratch,
        compiler_params=pltpu.CompilerParams(vmem_limit_bytes=56 * 1024 * 1024),
    )(where, *arrays, *remote)


def placed_load(where_ref, held, target, sems, stream, turning=False):
    near, far = held
    half = PLACES // 2
    block = target.shape[0] // PLACES
    at = place_of(where_ref, stream, turning)
    copies = []
    for rank in range(PLACES):
        source = near if rank < half else far
        copies.append(
            pltpu.make_async_copy(
                source.at[pl.ds(rank % half * block, block), :],
                target.at[pl.ds(pl.multiple_of(at(rank) * block, block), block), :],
                sems.at[rank],
            )
        )
    for copy in copies:
        copy.start()
    return copies


def finish(copies):
    for copy in copies:
        copy.wait()


def column_cuts(widths):
    at, cuts = 0, []
    for width in widths:
        cuts.append(slice(at, at + width))
        at += width
    return cuts


def join(held, given):
    return jnp.concatenate([held, given], axis=0)


def part_join(held, given, cuts):
    return [join(held[:, cut], given[:, cut]) for cut in cuts]


def term_blocks(products, where, stream, grad_scale, turning=False):
    lefts = [half for left, _ in products for half in left]
    rights = [right for _, right in products]
    height = lefts[0].shape[1]
    cuts = column_cuts([right.shape[1] for right in rights])
    width = cuts[-1].stop
    block = height // PLACES
    half = PLACES // 2
    strip = height // 4

    def kernel(where_ref, *refs):
        left_refs, refs = refs[: len(lefts)], refs[len(lefts) :]
        right_refs, (near_ref, far_ref, whole) = refs[: len(rights)], refs[len(rights) :]
        at = place_of(where_ref, stream, turning)
        for number, cut in enumerate(cuts):
            upper, lower = left_refs[2 * number : 2 * number + 2]
            rows = upper.shape[0]
            for k in range(4):
                part = slice(k * strip, (k + 1) * strip)
                total = dot_tn(upper[:, part], right_refs[number][:rows, :])
                total = total + dot_tn(lower[:, part], right_refs[number][rows:, :])
                whole[part, cut] = (total * grad_scale).astype(BF)
        for rank in range(PLACES):
            source = pl.ds(pl.multiple_of(at(rank) * block, block), block)
            out = near_ref if rank < half else far_ref
            out[pl.ds(rank % half * block, block), :] = whole[source, :]

    outs = [((height // 2, width), BF)] * 2
    scratch = [pltpu.VMEM((height, width), BF)]
    return local_call(kernel, outs, scratch, where, (*lefts, *rights))


def add(near, given):
    return near.astype(F32) + given.astype(F32)


def fold(near, given):
    half = near.shape[0] // 2
    send = add(near[half:], given[half:]).astype(BF)
    return add(near[:half], given[:half]).astype(BF), send


def fold_joined(nears, givens):
    halves = [fold(near, given) for near, given in zip(nears, givens)]
    return [jnp.concatenate(part, axis=1) for part in zip(*halves)]


def last_sum(joined):
    half = joined.shape[0] // 2
    low, high = joined[:half], joined[half:]
    at_low = lax.axis_index("fsdp_x") == 0
    given = swap(jnp.where(at_low, high, low).astype(BF), "fsdp_x")
    return jnp.where(at_low, low, high) + given.astype(F32)


def split_rows(where_rows, send_ref, keep_ref, value_of):
    half = where_rows // 2
    send_ref[...] = value_of(slice(half, None)).astype(BF)
    keep_ref[...] = value_of(slice(None, half))


def attend_probs(queries, keys):
    factor = temper / math.sqrt(HEAD_DIM)
    scores = dot_nt(queries, keys) * factor
    lifted = jnp.exp(scores - jnp.max(scores, axis=-1, keepdims=True))
    return lifted / jnp.sum(lifted, axis=-1, keepdims=True)


def held_scratch(held):
    return [
        pltpu.VMEM((2 * held[0].shape[0], held[0].shape[1]), BF),
        pltpu.SemaphoreType.DMA((PLACES,)),
    ]


def attention(rows, held_qk, held_vo, where):
    width = held_vo[0].shape[1] // 2
    count = 2 * rows[0].shape[0]
    model = rows[0].shape[1]

    def kernel(where_ref, upper, lower, near0, far0, near1, far1, *refs):
        qk_ref, v_ref, o_ref, send_ref, keep_ref, w0, sems0, w1, sems1 = refs
        first = placed_load(where_ref, (near0, far0), w0, sems0, 0)
        second = placed_load(where_ref, (near1, far1), w1, sems1, 1)
        half = count // 2
        finish(first)
        qk_ref[:half, :] = dot_nn(upper[...], w0[...]).astype(BF)
        qk_ref[half:, :] = dot_nn(lower[...], w0[...]).astype(BF)
        finish(second)
        v_ref[:half, :] = dot_nn(upper[...], w1[:, :width]).astype(BF)
        v_ref[half:, :] = dot_nn(lower[...], w1[:, :width]).astype(BF)
        for at in range(0, width, HEAD_DIM):
            head = slice(at, at + HEAD_DIM)
            probs = attend_probs(qk_ref[:, head], qk_ref[:, width + at : width + at + HEAD_DIM])
            o_ref[:, head] = dot_nn(probs.astype(BF), v_ref[:, head]).astype(BF)
        split_rows(count, send_ref, keep_ref, lambda span: dot_nt(o_ref[span, :], w1[:, width:]))

    outs = [
        ((count, 2 * width), BF),
        ((count, width), BF),
        ((count, width), BF),
        ((count // 2, model), BF),
        ((count // 2, model), F32),
    ]
    scratch = held_scratch(held_qk) + held_scratch(held_vo)
    return local_call(kernel, outs, scratch, where, rows, (*held_qk, *held_vo))


def attention_back(rows, queries_keys, values, held_qk, held_vo, where):
    width = values.shape[1]
    count = values.shape[0]
    model = rows[0].shape[1]
    factor = temper / math.sqrt(HEAD_DIM)

    def kernel(where_ref, upper, lower, qk_ref, v_ref, near0, far0, near1, far1, *refs):
        dqk_ref, dv_ref, send_ref, keep_ref, mixed, w0, sems0, w1, sems1 = refs
        second = placed_load(where_ref, (near1, far1), w1, sems1, 1)
        first = placed_load(where_ref, (near0, far0), w0, sems0, 0)
        half = count // 2
        finish(second)
        mixed[:half, :] = dot_nn(upper[...], w1[:, width:]).astype(BF)
        mixed[half:, :] = dot_nn(lower[...], w1[:, width:]).astype(BF)
        for at in range(0, width, HEAD_DIM):
            head = slice(at, at + HEAD_DIM)
            key_head = slice(width + at, width + at + HEAD_DIM)
            upstream = mixed[:, head]
            probs = attend_probs(qk_ref[:, head], qk_ref[:, key_head])
            dprobs = dot_nt(upstream, v_ref[:, head])
            inner = jnp.sum(probs * dprobs, axis=-1, keepdims=True)
            dscores = (probs * (dprobs - inner) * factor).astype(BF)
            dqk_ref[:, head] = dot_nn(dscores, qk_ref[:, key_head]).astype(BF)
            dqk_ref[:, key_head] = dot_tn(dscores, qk_ref[:, head]).astype(BF)
            dv_ref[:, head] = dot_tn(probs.astype(BF), upstream).astype(BF)
        finish(first)

        def part(span):
            return dot_nt(dqk_ref[span, :], w0[...]) + dot_nt(dv_ref[span, :], w1[:, :width])

        split_rows(count, send_ref, keep_ref, part)

    outs = [
        ((count, 2 * width), BF),
        ((count, width), BF),
        ((count // 2, model), BF),
        ((count // 2, model), F32),
    ]
    scratch = [pltpu.VMEM((count, width), BF)] + held_scratch(held_qk) + held_scratch(held_vo)
    arrays = (*rows, queries_keys, values)
    return local_call(kernel, outs, scratch, where, arrays, (*held_qk, *held_vo))


def gelu_pair(hidden):
    root, cube = math.sqrt(2.0 / math.pi), 0.044715
    square = hidden * hidden
    curve = jnp.tanh(root * (hidden + cube * (square * hidden)))
    rise = 0.5 * (1.0 + curve)
    slope = 0.5 * hidden * (1.0 - curve * curve) * (root * (1.0 + 3.0 * cube * square))
    return hidden * rise, rise + slope


def feed_forward(rows, down_rows, held_in, held_back, where):
    width = held_in[0].shape[1]
    count = 2 * rows[0].shape[0]
    model = rows[0].shape[1]
    strip = width // 4

    def kernel(where_ref, upper, lower, d_upper, d_lower, near0, far0, near1, far1, *refs):
        act_ref, up_ref, send_ref, keep_ref, w0, sems0, w1, sems1 = refs
        first = placed_load(where_ref, (near0, far0), w0, sems0, 0, True)
        second = placed_load(where_ref, (near1, far1), w1, sems1, 1, True)
        half = count // 2
        finish(first)
        finish(second)
        for k in range(4):
            part = slice(k * strip, (k + 1) * strip)
            for at, left, down in ((0, upper, d_upper), (half, lower, d_lower)):
                active, slope = gelu_pair(dot_nn(left[...], w0[:, part]))
                act_ref[at : at + half, part] = active.astype(BF)
                grad = slope * dot_nn(down[...], w1[:, part])
                up_ref[at : at + half, part] = grad.astype(BF)
        split_rows(count, send_ref, keep_ref, lambda span: dot_nt(up_ref[span, :], w0[...]))

    outs = [
        ((count, width), BF),
        ((count, width), BF),
        ((count // 2, model), BF),
        ((count // 2, model), F32),
    ]
    scratch = held_scratch(held_in) + held_scratch(held_back)
    arrays = (*rows, *down_rows)
    return local_call(kernel, outs, scratch, where, arrays, (*held_in, *held_back))


def down_project(activated, held_back, where):
    count = activated.shape[0]
    model = 2 * held_back[0].shape[0]

    def kernel(where_ref, act_ref, near, far, send_ref, keep_ref, w1, sems):
        finish(placed_load(where_ref, (near, far), w1, sems, 1, True))
        split_rows(count, send_ref, keep_ref, lambda span: dot_nt(act_ref[span, :], w1[...]))

    outs = [((count // 2, model), BF), ((count // 2, model), F32)]
    scratch = held_scratch(held_back)
    return local_call(kernel, outs, scratch, where, (activated,), held_back)


def pair_up(own):
    return ordered(own, swap(own, "fsdp_x"), "fsdp_x")


def block_pass(tokens, layer_mod, w_qkv, w_out, w_in, w_back, out_grad, grad_scale):
    own_width, ffn_width = w_out.shape[0], w_in.shape[1]
    where = jnp.stack([lax.axis_index(ZY), lax.axis_index("sp_core")]).astype(jnp.int32)
    cut = 2 * own_width
    attn_pair = pair_up(jnp.concatenate([w_qkv, w_out.T], axis=1))
    ffn_own = after(jnp.concatenate([w_in, w_back.T], axis=1), attn_pair)
    ffn_given = swap(ffn_own, "fsdp_x")

    stream = tokens.astype(F32)
    normed_first, rstd_first = normalize(stream)
    input_first = (normed_first * (1.0 + layer_mod[1]) + layer_mod[0]).astype(BF)

    attn_cuts = column_cuts((cut, 2 * own_width))
    ffn_cuts = column_cuts((ffn_width, ffn_width))
    attn_held = join(attn_pair, hop(attn_pair, 0))
    attn_given = hop(attn_held, 1)
    input_first = after(input_first, attn_held)
    attn_held = part_join(attn_held, attn_given, attn_cuts)
    ffn_given = after(ffn_given, attn_held)
    ffn_pair = ordered(ffn_own, ffn_given, "fsdp_x")
    ffn_held = [ffn_pair[:, part] for part in ffn_cuts]
    first_rows = spread(input_first, attn_held, ffn_pair)
    attn_given = [hop(held, 2, k) for k, held in enumerate(attn_held)]
    ffn_given = [hop(held, 0, k, True) for k, held in enumerate(ffn_held)]
    attn_held = [join(*pair) for pair in zip(attn_held, attn_given)]
    attn_far = [hop(held, 3, k) for k, held in enumerate(attn_held)]
    ffn_given = after(ffn_given, attn_held)
    ffn_held = [join(*pair) for pair in zip(ffn_held, ffn_given)]
    ffn_given = [hop(held, 1, k, True) for k, held in enumerate(ffn_held)]

    out_grad = after(out_grad, first_rows)
    stream_grad = out_grad.astype(F32)
    down_grad = (layer_mod[5] * stream_grad).astype(BF)
    down_rows = spread(down_grad, ffn_held)

    held_qk, held_vo = tuple(zip(attn_held, attn_far))
    first_rows = after(first_rows, down_rows)
    ffn_given = after(ffn_given, attn_far)
    ffn_held = [join(*pair) for pair in zip(ffn_held, ffn_given)]
    ffn_given = [hop(held, 2, k, True) for k, held in enumerate(ffn_held)]
    queries_keys, values, attended, send, keep = attention(first_rows, held_qk, held_vo, where)
    send, mine = collect(keep, send)
    ffn_given = after(ffn_given, send)
    ffn_held = [join(*pair) for pair in zip(ffn_held, ffn_given)]
    ffn_far = [hop(held, 3, k, True) for k, held in enumerate(ffn_held)]
    given = swap(send, "sp_x")
    middle = stream + layer_mod[2] * (mine + given.astype(F32))
    normed_second, rstd_second = normalize(middle)
    input_second = (normed_second * (1.0 + layer_mod[4]) + layer_mod[3]).astype(BF)
    second_rows = spread(input_second)
    ffn_far = after(ffn_far, second_rows)
    held_in, held_back = tuple(zip(ffn_held, ffn_far))

    activated, up_grad, send, keep = feed_forward(second_rows, down_rows, held_in, held_back, where)
    send, mine = collect(keep, send)
    up_rows = after(up_grad, send)
    near_in, far_in = term_blocks([(second_rows, up_rows)], where, 0, grad_scale, True)
    given_in = hop(far_in, 3, 0, True)
    back_second = mine + after(swap(send, "sp_x"), far_in).astype(F32)
    stream_grad = stream_grad + norm_back(
        normed_second, rstd_second, back_second * (1.0 + layer_mod[4])
    )
    attn_grad = (layer_mod[2] * stream_grad).astype(BF)
    act_rows = after(activated, attn_grad)
    near_back, far_back = term_blocks([(down_rows, act_rows)], where, 1, grad_scale, True)
    given_back = hop(far_back, 3, 1, True)
    attn_rows = after(spread(attn_grad), far_back)
    grad_qk, grad_v, send, keep = attention_back(
        attn_rows, queries_keys, values, held_qk, held_vo, where
    )
    given_in = after(given_in, send)
    two_in = fold(near_in, given_in)
    send_in = hop(two_in[1], 2, 0, True)
    send, mine = collect(keep, send)
    grad_qk, grad_v, attended = after((grad_qk, grad_v, attended), send)
    near_qk, far_qk = term_blocks([(first_rows, grad_qk)], where, 0, grad_scale)
    given_qk = hop(far_qk, 3, 0)
    given_back = after(given_back, far_qk)
    two_back = fold(near_back, given_back)
    send_back = hop(two_back[1], 2, 1, True)
    grad_v, attended = after((grad_v, attended), two_back)
    products = [(first_rows, grad_v), (attn_rows, attended)]
    near_vo, far_vo = term_blocks(products, where, 1, grad_scale)
    given_vo = hop(far_vo, 3, 1)

    back_first = mine + after(swap(send, "sp_x"), far_vo).astype(F32)
    input_grad = stream_grad + norm_back(
        normed_first, rstd_first, back_first * (1.0 + layer_mod[1])
    )
    late = after(activated, input_grad)
    send, keep = down_project(late, held_back, where)

    send_in, send_back = after((send_in, send_back), keep)
    two_in, two_back = fold(two_in[0], send_in), fold(two_back[0], send_back)
    send_in = hop(two_in[1], 1, 0, True)
    send_back = hop(two_back[1], 1, 1, True)
    given_qk, given_vo = after((given_qk, given_vo), two_in, two_back)
    two_qk, two_vo = fold(near_qk, given_qk), fold(near_vo, given_vo)
    send_qk, send_vo = hop(two_qk[1], 2, 0), hop(two_vo[1], 2, 1)
    send, mine = collect(keep, after(send, two_qk, two_vo))
    send_in, send_back = after((send_in, send_back), send)
    two_in, two_back = fold(two_in[0], send_in), fold(two_back[0], send_back)
    send_in = hop(two_in[1], 0, 0, True)
    send_back = hop(two_back[1], 0, 1, True)
    send_qk, send_vo = after((send_qk, send_vo), two_in, two_back)
    near_attn, send_attn = fold_joined((two_qk[0], two_vo[0]), (send_qk, send_vo))
    given_attn = hop(send_attn, 1)
    send_in, send_back = after((send_in, send_back), send_attn)
    total_ffn = jnp.concatenate([add(two_in[0], send_in), add(two_back[0], send_back)], axis=1)
    sum_ffn = last_sum(total_ffn)
    given = after(swap(send, "sp_x"), total_ffn)
    final_out = (middle + layer_mod[5] * (mine + given.astype(F32))).astype(BF)
    near_attn, send_attn = fold(near_attn, after(given_attn, final_out))
    given_attn = hop(send_attn, 0)
    sum_attn = last_sum(add(near_attn, given_attn))
    return (
        final_out,
        input_grad,
        sum_attn[:, : 3 * own_width],
        sum_attn[:, 3 * own_width :].T,
        sum_ffn[:, :ffn_width],
        sum_ffn[:, ffn_width:].T,
    )


def body(tokens, modulation, w_qkv, w_out, w_in, w_back, out_grad):
    local_seq = tokens.shape[1]
    own_width = w_qkv.shape[3]
    grad_scale = 1.0 / math.sqrt(local_seq * lax.axis_size(FSDP) * lax.axis_size(SP))
    final_out, input_grad, grad_qkv, grad_out, grad_in, grad_back = block_pass(
        tokens[0],
        modulation[0, 0],
        w_qkv[0].reshape(-1, 3 * own_width),
        w_out[0],
        w_in[0],
        w_back[0],
        out_grad[0],
        grad_scale,
    )
    return (
        final_out[None],
        input_grad[None],
        grad_qkv.reshape(1, -1, 3, own_width),
        grad_out[None],
        grad_in[None],
        grad_back[None],
    )


def solution(mesh):
    torus = Mesh(
        mesh.devices.reshape(4, 4, 2, 2, 2),
        (*FSDP, *SP),
    )
    return jax.shard_map(
        body,
        mesh=torus,
        in_specs=(
            P(FSDP, SP, None),
            P(FSDP, None, None, None),
            P(None, FSDP, None, SP),
            P(None, SP, FSDP),
            P(None, FSDP, SP),
            P(None, SP, FSDP),
            P(FSDP, SP, None),
        ),
        out_specs=(
            P(FSDP, SP, None),
            P(FSDP, SP, None),
            P(None, FSDP, None, SP),
            P(None, SP, FSDP),
            P(None, FSDP, SP),
            P(None, SP, FSDP),
        ),
        check_vma=False,
    )
```

```python
import math

import jax
import jax.numpy as jnp
from jax import lax
from jax.experimental import pallas as pl
from jax.experimental.pallas import tpu as pltpu
from jax.sharding import Mesh
from jax.sharding import PartitionSpec as P

HEAD_DIM = 128
ZY = ("fsdp_z", "fsdp_y")
FSDP = (*ZY, "fsdp_x")
SP = ("sp_x", "sp_core")
SWAP = ((0, 1), (1, 0))
GRID = (*ZY, "sp_core")
PLACES = 16
FLIPS = (1, 4, 3, 12)
STEPS = 4

ln_eps = 1e-06
temper = 2.5
BF = jnp.bfloat16
F32 = jnp.float32


def normalize(stream):
    mean_part = jnp.mean(stream, axis=-1, keepdims=True)
    centred = stream - mean_part
    rstd = lax.rsqrt(jnp.mean(centred * centred, axis=-1, keepdims=True) + ln_eps)
    return (centred * rstd, rstd)


def norm_back(normed, rstd, incoming):
    first = jnp.mean(incoming, axis=-1, keepdims=True)
    second = jnp.mean(incoming * normed, axis=-1, keepdims=True)
    return rstd * (incoming - first - normed * second)


def dot_nn(left, right):
    return jnp.dot(left, right, preferred_element_type=F32)


def dot_nt(left, right):
    return lax.dot_general(left, right, (((1,), (1,)), ((), ())), preferred_element_type=F32)


def dot_tn(left, right):
    return lax.dot_general(left, right, (((0,), (0,)), ((), ())), preferred_element_type=F32)


def swap(value, axis):
    return lax.ppermute(value, axis, SWAP)


def after(value, *earlier):
    return lax.optimization_barrier((value, earlier))[0]


def spread(own, *earlier):
    across = after(swap(own, "sp_x"), earlier)
    pair = jnp.concatenate([own, across], axis=0)
    return pair, swap(pair, "sp_core")


def collect(keep, give):
    rows = keep.shape[0] // 2
    given = swap(give, "sp_core")
    send = (keep[rows:] + given[rows:].astype(F32)).astype(BF)
    return send, keep[:rows] + given[:rows].astype(F32)


def ordered(own, other, axis):
    first = jnp.concatenate([own, other], axis=0)
    second = jnp.concatenate([other, own], axis=0)
    return jnp.where(lax.axis_index(axis) == 0, first, second)


def flip_of(turning, step, stream, core):
    if turning:
        return FLIPS[(2 * stream + core + step) % STEPS]
    inner = FLIPS[:2] if core == (step >= 2) else FLIPS[2:]
    return inner[(step % 2) ^ (stream if step >= 2 else 0)]


def hop(value, step, stream=0, turning=False):
    pairs = []
    for place in range(PLACES):
        for core in range(2):
            other = place ^ flip_of(turning, step, stream, core)
            pairs.append((2 * place + core, 2 * other + core))
    return lax.ppermute(value, GRID, pairs)


def place_of(where_ref, stream, turning):
    flips = []
    for step in range(STEPS):
        first, second = (flip_of(turning, step, stream, core) for core in range(2))
        flips.append(jnp.where(where_ref[1] == 0, first, second))

    def at(rank):
        place = where_ref[0]
        for step in range(STEPS):
            if rank >> step & 1:
                place = place ^ flips[step]
        return place

    return at


def local_call(kernel, outs, scratch, where, arrays, limit):
    vmem = pl.BlockSpec(memory_space=pltpu.VMEM)
    return pl.pallas_call(
        kernel,
        in_specs=[pl.BlockSpec(memory_space=pltpu.SMEM)] + [vmem] * len(arrays),
        out_specs=[vmem] * len(outs),
        out_shape=[jax.ShapeDtypeStruct(shape, kind) for shape, kind in outs],
        scratch_shapes=scratch,
        compiler_params=pltpu.CompilerParams(vmem_limit_bytes=limit * 1024 * 1024),
    )(where, *arrays)


def put_in_place(where_ref, held, target, stream, turning=False):
    near, far = held
    half = PLACES // 2
    block = target.shape[0] // PLACES
    at = place_of(where_ref, stream, turning)
    for rank in range(PLACES):
        source = near if rank < half else far
        rows = pl.ds(pl.multiple_of(at(rank) * block, block), block)
        target[rows, :] = source[rank % half * block : (rank % half + 1) * block, :]


def column_cuts(widths):
    at, cuts = 0, []
    for width in widths:
        cuts.append(slice(at, at + width))
        at += width
    return cuts


def join(held, given):
    return jnp.concatenate([held, given], axis=0)


def part_join(held, given, cuts):
    return [join(held[:, cut], given[:, cut]) for cut in cuts]


def term_blocks(products, where, stream, grad_scale, turning=False):
    lefts = [half for left, _ in products for half in left]
    rights = [right for _, right in products]
    height = lefts[0].shape[1]
    cuts = column_cuts([right.shape[1] for right in rights])
    width = cuts[-1].stop
    block = height // PLACES
    half = PLACES // 2
    strip = height // 4

    def kernel(where_ref, *refs):
        left_refs, refs = refs[: len(lefts)], refs[len(lefts) :]
        right_refs, (near_ref, far_ref, whole) = refs[: len(rights)], refs[len(rights) :]
        at = place_of(where_ref, stream, turning)
        for number, cut in enumerate(cuts):
            upper, lower = left_refs[2 * number : 2 * number + 2]
            rows = upper.shape[0]
            for k in range(4):
                part = slice(k * strip, (k + 1) * strip)
                total = dot_tn(upper[:, part], right_refs[number][:rows, :])
                total = total + dot_tn(lower[:, part], right_refs[number][rows:, :])
                whole[part, cut] = (total * grad_scale).astype(BF)
        for rank in range(PLACES):
            source = pl.ds(pl.multiple_of(at(rank) * block, block), block)
            out = near_ref if rank < half else far_ref
            out[pl.ds(rank % half * block, block), :] = whole[source, :]

    outs = [((height // 2, width), BF)] * 2
    scratch = [pltpu.VMEM((height, width), BF)]
    return local_call(kernel, outs, scratch, where, (*lefts, *rights), 20)


def add(near, given):
    return near.astype(F32) + given.astype(F32)


def fold(near, given):
    half = near.shape[0] // 2
    send = add(near[half:], given[half:]).astype(BF)
    return add(near[:half], given[:half]).astype(BF), send


def fold_joined(nears, givens):
    halves = [fold(near, given) for near, given in zip(nears, givens)]
    return [jnp.concatenate(part, axis=1) for part in zip(*halves)]


def last_sum(joined):
    half = joined.shape[0] // 2
    low, high = joined[:half], joined[half:]
    at_low = lax.axis_index("fsdp_x") == 0
    given = swap(jnp.where(at_low, high, low).astype(BF), "fsdp_x")
    return jnp.where(at_low, low, high) + given.astype(F32)


def split_rows(where_rows, send_ref, keep_ref, value_of):
    half = where_rows // 2
    send_ref[...] = value_of(slice(half, None)).astype(BF)
    keep_ref[...] = value_of(slice(None, half))


def attend_probs(queries, keys):
    factor = temper / math.sqrt(HEAD_DIM)
    scores = dot_nt(queries, keys) * factor
    lifted = jnp.exp(scores - jnp.max(scores, axis=-1, keepdims=True))
    return lifted / jnp.sum(lifted, axis=-1, keepdims=True)


def held_scratch(held):
    return pltpu.VMEM((2 * held[0].shape[0], held[0].shape[1]), BF)


def attention(rows, held_qk, held_vo, where):
    width = held_vo[0].shape[1] // 2
    count = 2 * rows[0].shape[0]
    model = rows[0].shape[1]

    def kernel(where_ref, upper, lower, near0, far0, near1, far1, *refs):
        qk_ref, v_ref, o_ref, send_ref, keep_ref, w0, w1 = refs
        half = count // 2
        put_in_place(where_ref, (near0, far0), w0, 0)
        qk_ref[:half, :] = dot_nn(upper[...], w0[...]).astype(BF)
        qk_ref[half:, :] = dot_nn(lower[...], w0[...]).astype(BF)
        put_in_place(where_ref, (near1, far1), w1, 1)
        v_ref[:half, :] = dot_nn(upper[...], w1[:, :width]).astype(BF)
        v_ref[half:, :] = dot_nn(lower[...], w1[:, :width]).astype(BF)
        for at in range(0, width, HEAD_DIM):
            head = slice(at, at + HEAD_DIM)
            probs = attend_probs(qk_ref[:, head], qk_ref[:, width + at : width + at + HEAD_DIM])
            o_ref[:, head] = dot_nn(probs.astype(BF), v_ref[:, head]).astype(BF)
        split_rows(count, send_ref, keep_ref, lambda span: dot_nt(o_ref[span, :], w1[:, width:]))

    outs = [
        ((count, 2 * width), BF),
        ((count, width), BF),
        ((count, width), BF),
        ((count // 2, model), BF),
        ((count // 2, model), F32),
    ]
    scratch = [held_scratch(held_qk), held_scratch(held_vo)]
    arrays = (*rows, *held_qk, *held_vo)
    return local_call(kernel, outs, scratch, where, arrays, 28)


def attention_back(rows, queries_keys, values, held_qk, held_vo, where):
    width = values.shape[1]
    count = values.shape[0]
    model = rows[0].shape[1]
    factor = temper / math.sqrt(HEAD_DIM)

    def kernel(where_ref, upper, lower, qk_ref, v_ref, near0, far0, near1, far1, *refs):
        dqk_ref, dv_ref, send_ref, keep_ref, mixed, w0, w1 = refs
        half = count // 2
        put_in_place(where_ref, (near1, far1), w1, 1)
        put_in_place(where_ref, (near0, far0), w0, 0)
        mixed[:half, :] = dot_nn(upper[...], w1[:, width:]).astype(BF)
        mixed[half:, :] = dot_nn(lower[...], w1[:, width:]).astype(BF)
        for at in range(0, width, HEAD_DIM):
            head = slice(at, at + HEAD_DIM)
            key_head = slice(width + at, width + at + HEAD_DIM)
            upstream = mixed[:, head]
            probs = attend_probs(qk_ref[:, head], qk_ref[:, key_head])
            dprobs = dot_nt(upstream, v_ref[:, head])
            inner = jnp.sum(probs * dprobs, axis=-1, keepdims=True)
            dscores = (probs * (dprobs - inner) * factor).astype(BF)
            dqk_ref[:, head] = dot_nn(dscores, qk_ref[:, key_head]).astype(BF)
            dqk_ref[:, key_head] = dot_tn(dscores, qk_ref[:, head]).astype(BF)
            dv_ref[:, head] = dot_tn(probs.astype(BF), upstream).astype(BF)

        def part(span):
            return dot_nt(dqk_ref[span, :], w0[...]) + dot_nt(dv_ref[span, :], w1[:, :width])

        split_rows(count, send_ref, keep_ref, part)

    outs = [
        ((count, 2 * width), BF),
        ((count, width), BF),
        ((count // 2, model), BF),
        ((count // 2, model), F32),
    ]
    scratch = [pltpu.VMEM((count, width), BF), held_scratch(held_qk), held_scratch(held_vo)]
    arrays = (*rows, queries_keys, values, *held_qk, *held_vo)
    return local_call(kernel, outs, scratch, where, arrays, 28)


def gelu_pair(hidden):
    root, cube = math.sqrt(2.0 / math.pi), 0.044715
    square = hidden * hidden
    curve = jnp.tanh(root * (hidden + cube * (square * hidden)))
    rise = 0.5 * (1.0 + curve)
    slope = 0.5 * hidden * (1.0 - curve * curve) * (root * (1.0 + 3.0 * cube * square))
    return hidden * rise, rise + slope


def feed_forward(rows, down_rows, held_in, held_back, where):
    width = held_in[0].shape[1]
    count = 2 * rows[0].shape[0]
    model = rows[0].shape[1]
    strip = width // 4

    def kernel(where_ref, upper, lower, d_upper, d_lower, near0, far0, near1, far1, *refs):
        act_ref, up_ref, send_ref, keep_ref, w0, w1 = refs
        half = count // 2
        put_in_place(where_ref, (near0, far0), w0, 0, True)
        put_in_place(where_ref, (near1, far1), w1, 1, True)
        for k in range(4):
            part = slice(k * strip, (k + 1) * strip)
            for at, left, down in ((0, upper, d_upper), (half, lower, d_lower)):
                active, slope = gelu_pair(dot_nn(left[...], w0[:, part]))
                act_ref[at : at + half, part] = active.astype(BF)
                grad = slope * dot_nn(down[...], w1[:, part])
                up_ref[at : at + half, part] = grad.astype(BF)
        split_rows(count, send_ref, keep_ref, lambda span: dot_nt(up_ref[span, :], w0[...]))

    outs = [
        ((count, width), BF),
        ((count, width), BF),
        ((count // 2, model), BF),
        ((count // 2, model), F32),
    ]
    scratch = [held_scratch(held_in), held_scratch(held_back)]
    arrays = (*rows, *down_rows, *held_in, *held_back)
    return local_call(kernel, outs, scratch, where, arrays, 32)


def down_project(activated, held_back, where):
    count = activated.shape[0]
    model = 2 * held_back[0].shape[0]

    def kernel(where_ref, act_ref, near, far, send_ref, keep_ref, w1):
        put_in_place(where_ref, (near, far), w1, 1, True)
        split_rows(count, send_ref, keep_ref, lambda span: dot_nt(act_ref[span, :], w1[...]))

    outs = [((count // 2, model), BF), ((count // 2, model), F32)]
    scratch = [held_scratch(held_back)]
    arrays = (activated, *held_back)
    return local_call(kernel, outs, scratch, where, arrays, 20)


def pair_up(own):
    return ordered(own, swap(own, "fsdp_x"), "fsdp_x")


def block_pass(tokens, layer_mod, w_qkv, w_out, w_in, w_back, out_grad, grad_scale):
    own_width, ffn_width = w_out.shape[0], w_in.shape[1]
    where = jnp.stack([lax.axis_index(ZY), lax.axis_index("sp_core")]).astype(jnp.int32)
    cut = 2 * own_width
    attn_pair = pair_up(jnp.concatenate([w_qkv, w_out.T], axis=1))
    ffn_own = after(jnp.concatenate([w_in, w_back.T], axis=1), attn_pair)
    ffn_given = swap(ffn_own, "fsdp_x")

    stream = tokens.astype(F32)
    normed_first, rstd_first = normalize(stream)
    input_first = (normed_first * (1.0 + layer_mod[1]) + layer_mod[0]).astype(BF)

    attn_cuts = column_cuts((cut, 2 * own_width))
    ffn_cuts = column_cuts((ffn_width, ffn_width))
    attn_held = join(attn_pair, hop(attn_pair, 0))
    attn_given = hop(attn_held, 1)
    input_first = after(input_first, attn_held)
    attn_held = part_join(attn_held, attn_given, attn_cuts)
    ffn_given = after(ffn_given, attn_held)
    ffn_pair = ordered(ffn_own, ffn_given, "fsdp_x")
    ffn_held = [ffn_pair[:, part] for part in ffn_cuts]
    attn_given = [hop(held, 2, k) for k, held in enumerate(attn_held)]
    ffn_given = [hop(held, 0, k, True) for k, held in enumerate(ffn_held)]
    attn_held = [join(*pair) for pair in zip(attn_held, attn_given)]
    first_rows = spread(input_first, attn_held)
    attn_far = [hop(held, 3, k) for k, held in enumerate(attn_held)]
    ffn_given = after(ffn_given, attn_held)
    ffn_held = [join(*pair) for pair in zip(ffn_held, ffn_given)]
    ffn_given = [hop(held, 1, k, True) for k, held in enumerate(ffn_held)]

    out_grad = after(out_grad, first_rows)
    stream_grad = out_grad.astype(F32)
    down_grad = (layer_mod[5] * stream_grad).astype(BF)
    down_rows = spread(down_grad)

    held_qk, held_vo = tuple(zip(attn_held, attn_far))
    ffn_given = after(ffn_given, attn_far)
    ffn_held = [join(*pair) for pair in zip(ffn_held, ffn_given)]
    ffn_given = [hop(held, 2, k, True) for k, held in enumerate(ffn_held)]
    queries_keys, values, attended, send, keep = attention(first_rows, held_qk, held_vo, where)
    send, mine = collect(keep, send)
    ffn_given = after(ffn_given, send)
    ffn_held = [join(*pair) for pair in zip(ffn_held, ffn_given)]
    ffn_far = [hop(held, 3, k, True) for k, held in enumerate(ffn_held)]
    given = swap(send, "sp_x")
    middle = stream + layer_mod[2] * (mine + given.astype(F32))
    normed_second, rstd_second = normalize(middle)
    input_second = (normed_second * (1.0 + layer_mod[4]) + layer_mod[3]).astype(BF)
    second_rows = spread(input_second)
    ffn_far = after(ffn_far, second_rows)
    held_in, held_back = tuple(zip(ffn_held, ffn_far))

    activated, up_grad, send, keep = feed_forward(second_rows, down_rows, held_in, held_back, where)
    send, mine = collect(keep, send)
    up_rows = after(up_grad, send)
    near_in, far_in = term_blocks([(second_rows, up_rows)], where, 0, grad_scale, True)
    given_in = hop(far_in, 3, 0, True)
    back_second = mine + after(swap(send, "sp_x"), far_in).astype(F32)
    stream_grad = stream_grad + norm_back(
        normed_second, rstd_second, back_second * (1.0 + layer_mod[4])
    )
    attn_grad = (layer_mod[2] * stream_grad).astype(BF)
    act_rows = after(activated, attn_grad)
    near_back, far_back = term_blocks([(down_rows, act_rows)], where, 1, grad_scale, True)
    given_back = hop(far_back, 3, 1, True)
    attn_rows = after(spread(attn_grad), far_back)
    grad_qk, grad_v, send, keep = attention_back(
        attn_rows, queries_keys, values, held_qk, held_vo, where
    )
    given_in = after(given_in, send)
    two_in = fold(near_in, given_in)
    send_in = hop(two_in[1], 2, 0, True)
    send, mine = collect(keep, send)
    grad_qk, grad_v, attended = after((grad_qk, grad_v, attended), send)
    near_qk, far_qk = term_blocks([(first_rows, grad_qk)], where, 0, grad_scale)
    given_qk = hop(far_qk, 3, 0)
    given_back = after(given_back, far_qk)
    two_back = fold(near_back, given_back)
    send_back = hop(two_back[1], 2, 1, True)
    grad_v, attended = after((grad_v, attended), two_back)
    products = [(first_rows, grad_v), (attn_rows, attended)]
    near_vo, far_vo = term_blocks(products, where, 1, grad_scale)
    given_vo = hop(far_vo, 3, 1)

    back_first = mine + after(swap(send, "sp_x"), far_vo).astype(F32)
    input_grad = stream_grad + norm_back(
        normed_first, rstd_first, back_first * (1.0 + layer_mod[1])
    )
    late = after(activated, input_grad)
    send, keep = down_project(late, held_back, where)

    send_in, send_back = after((send_in, send_back), keep)
    two_in, two_back = fold(two_in[0], send_in), fold(two_back[0], send_back)
    send_in = hop(two_in[1], 1, 0, True)
    send_back = hop(two_back[1], 1, 1, True)
    given_qk, given_vo = after((given_qk, given_vo), two_in, two_back)
    two_qk, two_vo = fold(near_qk, given_qk), fold(near_vo, given_vo)
    send_qk, send_vo = hop(two_qk[1], 2, 0), hop(two_vo[1], 2, 1)
    send, mine = collect(keep, after(send, two_qk, two_vo))
    send_in, send_back = after((send_in, send_back), send)
    two_in, two_back = fold(two_in[0], send_in), fold(two_back[0], send_back)
    send_in = hop(two_in[1], 0, 0, True)
    send_back = hop(two_back[1], 0, 1, True)
    send_qk, send_vo = after((send_qk, send_vo), two_in, two_back)
    near_attn, send_attn = fold_joined((two_qk[0], two_vo[0]), (send_qk, send_vo))
    given_attn = hop(send_attn, 1)
    send_in, send_back = after((send_in, send_back), send_attn)
    total_ffn = jnp.concatenate([add(two_in[0], send_in), add(two_back[0], send_back)], axis=1)
    sum_ffn = last_sum(total_ffn)
    given = after(swap(send, "sp_x"), total_ffn)
    final_out = (middle + layer_mod[5] * (mine + given.astype(F32))).astype(BF)
    near_attn, send_attn = fold(near_attn, after(given_attn, final_out))
    given_attn = hop(send_attn, 0)
    sum_attn = last_sum(add(near_attn, given_attn))
    return (
        final_out,
        input_grad,
        sum_attn[:, : 3 * own_width],
        sum_attn[:, 3 * own_width :].T,
        sum_ffn[:, :ffn_width],
        sum_ffn[:, ffn_width:].T,
    )


def body(tokens, modulation, w_qkv, w_out, w_in, w_back, out_grad):
    local_seq = tokens.shape[1]
    own_width = w_qkv.shape[3]
    grad_scale = 1.0 / math.sqrt(local_seq * lax.axis_size(FSDP) * lax.axis_size(SP))
    final_out, input_grad, grad_qkv, grad_out, grad_in, grad_back = block_pass(
        tokens[0],
        modulation[0, 0],
        w_qkv[0].reshape(-1, 3 * own_width),
        w_out[0],
        w_in[0],
        w_back[0],
        out_grad[0],
        grad_scale,
    )
    return (
        final_out[None],
        input_grad[None],
        grad_qkv.reshape(1, -1, 3, own_width),
        grad_out[None],
        grad_in[None],
        grad_back[None],
    )


def solution(mesh):
    torus = Mesh(
        mesh.devices.reshape(4, 4, 2, 2, 2),
        (*FSDP, *SP),
    )
    return jax.shard_map(
        body,
        mesh=torus,
        in_specs=(
            P(FSDP, SP, None),
            P(FSDP, None, None, None),
            P(None, FSDP, None, SP),
            P(None, SP, FSDP),
            P(None, FSDP, SP),
            P(None, SP, FSDP),
            P(FSDP, SP, None),
        ),
        out_specs=(
            P(FSDP, SP, None),
            P(FSDP, SP, None),
            P(None, FSDP, None, SP),
            P(None, SP, FSDP),
            P(None, FSDP, SP),
            P(None, SP, FSDP),
        ),
        check_vma=False,
    )
```

```python
import math

import jax
import jax.numpy as jnp
from jax import lax
from jax.experimental import pallas as pl
from jax.experimental.pallas import tpu as pltpu
from jax.sharding import Mesh
from jax.sharding import PartitionSpec as P

HEAD_DIM = 128
ZY = ("fsdp_z", "fsdp_y")
FSDP = (*ZY, "fsdp_x")
SP = ("sp_x", "sp_core")
SWAP = ((0, 1), (1, 0))
GRID = (*ZY, "sp_core")
PLACES = 16
FLIPS = (1, 4, 3, 12)
STEPS = 4

ln_eps = 1e-06
temper = 2.5
BF = jnp.bfloat16
F32 = jnp.float32


def normalize(stream):
    mean_part = jnp.mean(stream, axis=-1, keepdims=True)
    centred = stream - mean_part
    rstd = lax.rsqrt(jnp.mean(centred * centred, axis=-1, keepdims=True) + ln_eps)
    return (centred * rstd, rstd)


def norm_back(normed, rstd, incoming):
    first = jnp.mean(incoming, axis=-1, keepdims=True)
    second = jnp.mean(incoming * normed, axis=-1, keepdims=True)
    return rstd * (incoming - first - normed * second)


def dot_nn(left, right):
    return jnp.dot(left, right, preferred_element_type=F32)


def dot_nt(left, right):
    return lax.dot_general(left, right, (((1,), (1,)), ((), ())), preferred_element_type=F32)


def dot_tn(left, right):
    return lax.dot_general(left, right, (((0,), (0,)), ((), ())), preferred_element_type=F32)


def swap(value, axis):
    return lax.ppermute(value, axis, SWAP)


def after(value, *earlier):
    return lax.optimization_barrier((value, earlier))[0]


def spread(own, *earlier):
    across = after(swap(own, "sp_x"), earlier)
    pair = jnp.concatenate([own, across], axis=0)
    return pair, swap(pair, "sp_core")


def collect(keep, give):
    rows = keep.shape[0] // 2
    given = swap(give, "sp_core")
    send = (keep[rows:] + given[rows:].astype(F32)).astype(BF)
    return send, keep[:rows] + given[:rows].astype(F32)


def ordered(own, other, axis):
    first = jnp.concatenate([own, other], axis=0)
    second = jnp.concatenate([other, own], axis=0)
    return jnp.where(lax.axis_index(axis) == 0, first, second)


def flip_of(turning, step, stream, core):
    if turning:
        return FLIPS[(2 * stream + core + step) % STEPS]
    inner = FLIPS[:2] if core == (step >= 2) else FLIPS[2:]
    return inner[(step % 2) ^ (stream if step >= 2 else 0)]


def hop(value, step, stream=0, turning=False):
    pairs = []
    for place in range(PLACES):
        for core in range(2):
            other = place ^ flip_of(turning, step, stream, core)
            pairs.append((2 * place + core, 2 * other + core))
    return lax.ppermute(value, GRID, pairs)


def place_of(where_ref, stream, turning):
    flips = []
    for step in range(STEPS):
        first, second = (flip_of(turning, step, stream, core) for core in range(2))
        flips.append(jnp.where(where_ref[1] == 0, first, second))

    def at(rank):
        place = where_ref[0]
        for step in range(STEPS):
            if rank >> step & 1:
                place = place ^ flips[step]
        return place

    return at


def local_call(kernel, outs, scratch, where, arrays, limit):
    vmem = pl.BlockSpec(memory_space=pltpu.VMEM)
    return pl.pallas_call(
        kernel,
        in_specs=[pl.BlockSpec(memory_space=pltpu.SMEM)] + [vmem] * len(arrays),
        out_specs=[vmem] * len(outs),
        out_shape=[jax.ShapeDtypeStruct(shape, kind) for shape, kind in outs],
        scratch_shapes=scratch,
        compiler_params=pltpu.CompilerParams(vmem_limit_bytes=limit * 1024 * 1024),
    )(where, *arrays)


def put_in_place(where_ref, held, target, stream, turning=False):
    near, far = held
    half = PLACES // 2
    block = target.shape[0] // PLACES
    at = place_of(where_ref, stream, turning)
    for rank in range(PLACES):
        source = near if rank < half else far
        rows = pl.ds(pl.multiple_of(at(rank) * block, block), block)
        target[rows, :] = source[rank % half * block : (rank % half + 1) * block, :]


def column_cuts(widths):
    at, cuts = 0, []
    for width in widths:
        cuts.append(slice(at, at + width))
        at += width
    return cuts


def join(held, given):
    return jnp.concatenate([held, given], axis=0)


def part_join(held, given, cuts):
    return [join(held[:, cut], given[:, cut]) for cut in cuts]


def term_blocks(products, where, stream, grad_scale, turning=False):
    lefts = [half for left, _ in products for half in left]
    rights = [right for _, right in products]
    height = lefts[0].shape[1]
    cuts = column_cuts([right.shape[1] for right in rights])
    width = cuts[-1].stop
    block = height // PLACES
    half = PLACES // 2
    strip = height // 4

    def kernel(where_ref, *refs):
        left_refs, refs = refs[: len(lefts)], refs[len(lefts) :]
        right_refs, (near_ref, far_ref, whole) = refs[: len(rights)], refs[len(rights) :]
        at = place_of(where_ref, stream, turning)
        for number, cut in enumerate(cuts):
            upper, lower = left_refs[2 * number : 2 * number + 2]
            rows = upper.shape[0]
            for k in range(4):
                part = slice(k * strip, (k + 1) * strip)
                total = dot_tn(upper[:, part], right_refs[number][:rows, :])
                total = total + dot_tn(lower[:, part], right_refs[number][rows:, :])
                whole[part, cut] = (total * grad_scale).astype(BF)
        for rank in range(PLACES):
            source = pl.ds(pl.multiple_of(at(rank) * block, block), block)
            out = near_ref if rank < half else far_ref
            out[pl.ds(rank % half * block, block), :] = whole[source, :]

    outs = [((height // 2, width), BF)] * 2
    scratch = [pltpu.VMEM((height, width), BF)]
    return local_call(kernel, outs, scratch, where, (*lefts, *rights), 20)


def add(near, given):
    return near.astype(F32) + given.astype(F32)


def fold(near, given):
    half = near.shape[0] // 2
    send = add(near[half:], given[half:]).astype(BF)
    return add(near[:half], given[:half]).astype(BF), send


def fold_joined(nears, givens):
    halves = [fold(near, given) for near, given in zip(nears, givens)]
    return [jnp.concatenate(part, axis=1) for part in zip(*halves)]


def last_sum(joined):
    half = joined.shape[0] // 2
    low, high = joined[:half], joined[half:]
    at_low = lax.axis_index("fsdp_x") == 0
    given = swap(jnp.where(at_low, high, low).astype(BF), "fsdp_x")
    return jnp.where(at_low, low, high) + given.astype(F32)


def split_rows(where_rows, send_ref, keep_ref, value_of):
    half = where_rows // 2
    send_ref[...] = value_of(slice(half, None)).astype(BF)
    keep_ref[...] = value_of(slice(None, half))


def attend_probs(queries, keys):
    factor = temper / math.sqrt(HEAD_DIM)
    scores = dot_nt(queries, keys) * factor
    lifted = jnp.exp(scores - jnp.max(scores, axis=-1, keepdims=True))
    return lifted / jnp.sum(lifted, axis=-1, keepdims=True)


def held_scratch(held):
    return pltpu.VMEM((2 * held[0].shape[0], held[0].shape[1]), BF)


def attention(rows, held_qk, held_vo, where):
    width = held_vo[0].shape[1] // 2
    count = 2 * rows[0].shape[0]
    model = rows[0].shape[1]

    def kernel(where_ref, upper, lower, near0, far0, near1, far1, *refs):
        qk_ref, v_ref, o_ref, send_ref, keep_ref, w0, w1 = refs
        half = count // 2
        put_in_place(where_ref, (near0, far0), w0, 0)
        qk_ref[:half, :] = dot_nn(upper[...], w0[...]).astype(BF)
        qk_ref[half:, :] = dot_nn(lower[...], w0[...]).astype(BF)
        put_in_place(where_ref, (near1, far1), w1, 1)
        v_ref[:half, :] = dot_nn(upper[...], w1[:, :width]).astype(BF)
        v_ref[half:, :] = dot_nn(lower[...], w1[:, :width]).astype(BF)
        for at in range(0, width, HEAD_DIM):
            head = slice(at, at + HEAD_DIM)
            probs = attend_probs(qk_ref[:, head], qk_ref[:, width + at : width + at + HEAD_DIM])
            o_ref[:, head] = dot_nn(probs.astype(BF), v_ref[:, head]).astype(BF)
        split_rows(count, send_ref, keep_ref, lambda span: dot_nt(o_ref[span, :], w1[:, width:]))

    outs = [
        ((count, 2 * width), BF),
        ((count, width), BF),
        ((count, width), BF),
        ((count // 2, model), BF),
        ((count // 2, model), F32),
    ]
    scratch = [held_scratch(held_qk), held_scratch(held_vo)]
    arrays = (*rows, *held_qk, *held_vo)
    return local_call(kernel, outs, scratch, where, arrays, 28)


def attention_back(rows, queries_keys, values, held_qk, held_vo, where):
    width = values.shape[1]
    count = values.shape[0]
    model = rows[0].shape[1]
    factor = temper / math.sqrt(HEAD_DIM)

    def kernel(where_ref, upper, lower, qk_ref, v_ref, near0, far0, near1, far1, *refs):
        dqk_ref, dv_ref, send_ref, keep_ref, mixed, w0, w1 = refs
        half = count // 2
        put_in_place(where_ref, (near1, far1), w1, 1)
        put_in_place(where_ref, (near0, far0), w0, 0)
        mixed[:half, :] = dot_nn(upper[...], w1[:, width:]).astype(BF)
        mixed[half:, :] = dot_nn(lower[...], w1[:, width:]).astype(BF)
        for at in range(0, width, HEAD_DIM):
            head = slice(at, at + HEAD_DIM)
            key_head = slice(width + at, width + at + HEAD_DIM)
            upstream = mixed[:, head]
            probs = attend_probs(qk_ref[:, head], qk_ref[:, key_head])
            dprobs = dot_nt(upstream, v_ref[:, head])
            inner = jnp.sum(probs * dprobs, axis=-1, keepdims=True)
            dscores = (probs * (dprobs - inner) * factor).astype(BF)
            dqk_ref[:, head] = dot_nn(dscores, qk_ref[:, key_head]).astype(BF)
            dqk_ref[:, key_head] = dot_tn(dscores, qk_ref[:, head]).astype(BF)
            dv_ref[:, head] = dot_tn(probs.astype(BF), upstream).astype(BF)

        def part(span):
            return dot_nt(dqk_ref[span, :], w0[...]) + dot_nt(dv_ref[span, :], w1[:, :width])

        split_rows(count, send_ref, keep_ref, part)

    outs = [
        ((count, 2 * width), BF),
        ((count, width), BF),
        ((count // 2, model), BF),
        ((count // 2, model), F32),
    ]
    scratch = [pltpu.VMEM((count, width), BF), held_scratch(held_qk), held_scratch(held_vo)]
    arrays = (*rows, queries_keys, values, *held_qk, *held_vo)
    return local_call(kernel, outs, scratch, where, arrays, 28)


def gelu_pair(hidden):
    root, cube = math.sqrt(2.0 / math.pi), 0.044715
    square = hidden * hidden
    curve = jnp.tanh(root * (hidden + cube * (square * hidden)))
    rise = 0.5 * (1.0 + curve)
    slope = 0.5 * hidden * (1.0 - curve * curve) * (root * (1.0 + 3.0 * cube * square))
    return hidden * rise, rise + slope


def feed_forward(rows, down_rows, held_in, held_back, where):
    width = held_in[0].shape[1]
    count = 2 * rows[0].shape[0]
    model = rows[0].shape[1]
    strip = width // 4

    def kernel(where_ref, upper, lower, d_upper, d_lower, near0, far0, near1, far1, *refs):
        act_ref, up_ref, send_ref, keep_ref, w0, w1 = refs
        half = count // 2
        put_in_place(where_ref, (near0, far0), w0, 0, True)
        put_in_place(where_ref, (near1, far1), w1, 1, True)
        for k in range(4):
            part = slice(k * strip, (k + 1) * strip)
            for at, left, down in ((0, upper, d_upper), (half, lower, d_lower)):
                active, slope = gelu_pair(dot_nn(left[...], w0[:, part]))
                act_ref[at : at + half, part] = active.astype(BF)
                grad = slope * dot_nn(down[...], w1[:, part])
                up_ref[at : at + half, part] = grad.astype(BF)
        split_rows(count, send_ref, keep_ref, lambda span: dot_nt(up_ref[span, :], w0[...]))

    outs = [
        ((count, width), BF),
        ((count, width), BF),
        ((count // 2, model), BF),
        ((count // 2, model), F32),
    ]
    scratch = [held_scratch(held_in), held_scratch(held_back)]
    arrays = (*rows, *down_rows, *held_in, *held_back)
    return local_call(kernel, outs, scratch, where, arrays, 32)


def down_project(activated, held_back, where):
    count = activated.shape[0]
    model = 2 * held_back[0].shape[0]

    def kernel(where_ref, act_ref, near, far, send_ref, keep_ref, w1):
        put_in_place(where_ref, (near, far), w1, 1, True)
        split_rows(count, send_ref, keep_ref, lambda span: dot_nt(act_ref[span, :], w1[...]))

    outs = [((count // 2, model), BF), ((count // 2, model), F32)]
    scratch = [held_scratch(held_back)]
    arrays = (activated, *held_back)
    return local_call(kernel, outs, scratch, where, arrays, 20)


def pair_up(own):
    return ordered(own, swap(own, "fsdp_x"), "fsdp_x")


def block_pass(tokens, layer_mod, w_qkv, w_out, w_in, w_back, out_grad, grad_scale):
    own_width, ffn_width = w_out.shape[0], w_in.shape[1]
    where = jnp.stack([lax.axis_index(ZY), lax.axis_index("sp_core")]).astype(jnp.int32)
    cut = 2 * own_width
    attn_pair = pair_up(jnp.concatenate([w_qkv, w_out.T], axis=1))
    ffn_own = jnp.concatenate([w_in, w_back.T], axis=1)
    ffn_given = after(swap(ffn_own, "fsdp_x"), attn_pair)
    ffn_pair = ordered(ffn_own, ffn_given, "fsdp_x")

    stream = tokens.astype(F32)
    normed_first, rstd_first = normalize(stream)
    input_first = (normed_first * (1.0 + layer_mod[1]) + layer_mod[0]).astype(BF)

    attn_cuts = column_cuts((cut, 2 * own_width))
    ffn_cuts = column_cuts((ffn_width, ffn_width))
    ffn_held = [ffn_pair[:, part] for part in ffn_cuts]
    ffn_given = [hop(held, 0, k, True) for k, held in enumerate(ffn_held)]
    attn_held = join(attn_pair, hop(attn_pair, 0))
    attn_given = hop(attn_held, 1)
    ffn_given = after(ffn_given, attn_held)
    ffn_held = [join(*pair) for pair in zip(ffn_held, ffn_given)]
    ffn_given = [hop(held, 1, k, True) for k, held in enumerate(ffn_held)]
    input_first = after(input_first, attn_pair)
    attn_held = part_join(attn_held, attn_given, attn_cuts)
    attn_given = [hop(held, 2, k) for k, held in enumerate(attn_held)]
    attn_held = [join(*pair) for pair in zip(attn_held, attn_given)]
    first_rows = spread(input_first, attn_held)
    attn_far = [hop(held, 3, k) for k, held in enumerate(attn_held)]
    ffn_given = after(ffn_given, attn_held)
    ffn_held = [join(*pair) for pair in zip(ffn_held, ffn_given)]
    ffn_given = [hop(held, 2, k, True) for k, held in enumerate(ffn_held)]

    out_grad = after(out_grad, first_rows)
    stream_grad = out_grad.astype(F32)
    down_grad = (layer_mod[5] * stream_grad).astype(BF)
    down_rows = spread(down_grad)

    held_qk, held_vo = tuple(zip(attn_held, attn_far))
    queries_keys, values, attended, send, keep = attention(first_rows, held_qk, held_vo, where)
    send, mine = collect(keep, send)
    ffn_given = after(ffn_given, send)
    ffn_held = [join(*pair) for pair in zip(ffn_held, ffn_given)]
    ffn_far = [hop(held, 3, k, True) for k, held in enumerate(ffn_held)]
    given = after(swap(send, "sp_x"), ffn_held)
    middle = stream + layer_mod[2] * (mine + given.astype(F32))
    normed_second, rstd_second = normalize(middle)
    input_second = (normed_second * (1.0 + layer_mod[4]) + layer_mod[3]).astype(BF)
    second_rows = spread(input_second)
    ffn_far = after(ffn_far, second_rows)
    held_in, held_back = tuple(zip(ffn_held, ffn_far))

    activated, up_grad, send, keep = feed_forward(second_rows, down_rows, held_in, held_back, where)
    send, mine = collect(keep, send)
    up_rows = after(up_grad, send)
    near_in, far_in = term_blocks([(second_rows, up_rows)], where, 0, grad_scale, True)
    given_in = hop(far_in, 3, 0, True)
    back_second = mine + after(swap(send, "sp_x"), far_in).astype(F32)
    stream_grad = stream_grad + norm_back(
        normed_second, rstd_second, back_second * (1.0 + layer_mod[4])
    )
    attn_grad = (layer_mod[2] * stream_grad).astype(BF)
    act_rows = after(activated, attn_grad)
    near_back, far_back = term_blocks([(down_rows, act_rows)], where, 1, grad_scale, True)
    given_back = hop(far_back, 3, 1, True)
    attn_rows = after(spread(attn_grad), far_back)
    grad_qk, grad_v, send, keep = attention_back(
        attn_rows, queries_keys, values, held_qk, held_vo, where
    )
    near_qk, far_qk = term_blocks([(first_rows, grad_qk)], where, 0, grad_scale)
    given_qk = hop(far_qk, 3, 0)
    grad_v, attended = after((grad_v, attended), far_qk)
    products = [(first_rows, grad_v), (attn_rows, attended)]
    near_vo, far_vo = term_blocks(products, where, 1, grad_scale)
    given_vo = hop(far_vo, 3, 1)
    given_in = after(given_in, far_vo)
    two_in = fold(near_in, given_in)
    send_in = hop(two_in[1], 2, 0, True)
    given_back, send = after((given_back, send), two_in)
    two_back = fold(near_back, given_back)
    send_back = hop(two_back[1], 2, 1, True)
    send, mine = collect(keep, send)
    given_first = swap(send, "sp_x")

    send, keep = down_project(after(activated, send, two_back), held_back, where)
    given_qk, given_vo = after((given_qk, given_vo), keep)
    two_qk, two_vo = fold(near_qk, given_qk), fold(near_vo, given_vo)
    send_qk, send_vo = hop(two_qk[1], 2, 0), hop(two_vo[1], 2, 1)
    send, out_mine = collect(keep, after(send, two_qk, two_vo))
    send_in, send_back = after((send_in, send_back), send)
    two_in, two_back = fold(two_in[0], send_in), fold(two_back[0], send_back)
    send_in = hop(two_in[1], 1, 0, True)
    send_back = hop(two_back[1], 1, 1, True)

    back_first = mine + after(given_first, two_in, two_back).astype(F32)
    input_grad = stream_grad + norm_back(
        normed_first, rstd_first, back_first * (1.0 + layer_mod[1])
    )
    send_qk, send_vo = after((send_qk, send_vo), input_grad)
    near_attn, send_attn = fold_joined((two_qk[0], two_vo[0]), (send_qk, send_vo))
    given_attn = hop(send_attn, 1)
    send_in, send_back = after((send_in, send_back), send_attn)
    two_in, two_back = fold(two_in[0], send_in), fold(two_back[0], send_back)
    send_in = hop(two_in[1], 0, 0, True)
    send_back = hop(two_back[1], 0, 1, True)
    given = after(swap(send, "sp_x"), two_in, two_back)
    final_out = (middle + layer_mod[5] * (out_mine + given.astype(F32))).astype(BF)
    near_attn, send_attn = fold(near_attn, after(given_attn, final_out))
    given_attn = hop(send_attn, 0)
    send_in, send_back = after((send_in, send_back), send_attn)
    total_ffn = jnp.concatenate([add(two_in[0], send_in), add(two_back[0], send_back)], axis=1)
    sum_ffn = last_sum(total_ffn)
    sum_attn = last_sum(add(near_attn, after(given_attn, total_ffn)))
    return (
        final_out,
        input_grad,
        sum_attn[:, : 3 * own_width],
        sum_attn[:, 3 * own_width :].T,
        sum_ffn[:, :ffn_width],
        sum_ffn[:, ffn_width:].T,
    )


def body(tokens, modulation, w_qkv, w_out, w_in, w_back, out_grad):
    local_seq = tokens.shape[1]
    own_width = w_qkv.shape[3]
    grad_scale = 1.0 / math.sqrt(local_seq * lax.axis_size(FSDP) * lax.axis_size(SP))
    final_out, input_grad, grad_qkv, grad_out, grad_in, grad_back = block_pass(
        tokens[0],
        modulation[0, 0],
        w_qkv[0].reshape(-1, 3 * own_width),
        w_out[0],
        w_in[0],
        w_back[0],
        out_grad[0],
        grad_scale,
    )
    return (
        final_out[None],
        input_grad[None],
        grad_qkv.reshape(1, -1, 3, own_width),
        grad_out[None],
        grad_in[None],
        grad_back[None],
    )


def solution(mesh):
    torus = Mesh(
        mesh.devices.reshape(4, 4, 2, 2, 2),
        (*FSDP, *SP),
    )
    return jax.shard_map(
        body,
        mesh=torus,
        in_specs=(
            P(FSDP, SP, None),
            P(FSDP, None, None, None),
            P(None, FSDP, None, SP),
            P(None, SP, FSDP),
            P(None, FSDP, SP),
            P(None, SP, FSDP),
            P(FSDP, SP, None),
        ),
        out_specs=(
            P(FSDP, SP, None),
            P(FSDP, SP, None),
            P(None, FSDP, None, SP),
            P(None, SP, FSDP),
            P(None, FSDP, SP),
            P(None, SP, FSDP),
        ),
        check_vma=False,
    )
```

```python
import math

import jax
import jax.numpy as jnp
from jax import lax
from jax.experimental import pallas as pl
from jax.experimental.pallas import tpu as pltpu
from jax.sharding import Mesh
from jax.sharding import PartitionSpec as P

HEAD_DIM = 128
ZY = ("fsdp_z", "fsdp_y")
FSDP = (*ZY, "fsdp_x")
SP = ("sp_x", "sp_core")
SWAP = ((0, 1), (1, 0))
GRID = (*ZY, "sp_core")
PLACES = 16
FLIPS = (1, 4, 3, 12)
STEPS = 4

ln_eps = 1e-06
temper = 2.5
BF = jnp.bfloat16
F32 = jnp.float32


def normalize(stream):
    mean_part = jnp.mean(stream, axis=-1, keepdims=True)
    centred = stream - mean_part
    rstd = lax.rsqrt(jnp.mean(centred * centred, axis=-1, keepdims=True) + ln_eps)
    return (centred * rstd, rstd)


def norm_back(normed, rstd, incoming):
    first = jnp.mean(incoming, axis=-1, keepdims=True)
    second = jnp.mean(incoming * normed, axis=-1, keepdims=True)
    return rstd * (incoming - first - normed * second)


def dot_nn(left, right):
    return jnp.dot(left, right, preferred_element_type=F32)


def dot_nt(left, right):
    return lax.dot_general(left, right, (((1,), (1,)), ((), ())), preferred_element_type=F32)


def dot_tn(left, right):
    return lax.dot_general(left, right, (((0,), (0,)), ((), ())), preferred_element_type=F32)


def swap(value, axis):
    return lax.ppermute(value, axis, SWAP)


def after(value, *earlier):
    return lax.optimization_barrier((value, earlier))[0]


def spread(own, *earlier):
    across = after(swap(own, "sp_x"), earlier)
    pair = jnp.concatenate([own, across], axis=0)
    return pair, swap(pair, "sp_core")


def collect(keep, give):
    rows = keep.shape[0] // 2
    given = swap(give, "sp_core")
    send = (keep[rows:] + given[rows:].astype(F32)).astype(BF)
    return send, keep[:rows] + given[:rows].astype(F32)


def ordered(own, other, axis):
    first = jnp.concatenate([own, other], axis=0)
    second = jnp.concatenate([other, own], axis=0)
    return jnp.where(lax.axis_index(axis) == 0, first, second)


def flip_of(turning, step, stream, core):
    if turning:
        return FLIPS[(2 * stream + core + step) % STEPS]
    inner = FLIPS[:2] if core == (step >= 2) else FLIPS[2:]
    return inner[(step % 2) ^ (stream if step >= 2 else 0)]


def hop(value, step, stream=0, turning=False):
    pairs = []
    for place in range(PLACES):
        for core in range(2):
            other = place ^ flip_of(turning, step, stream, core)
            pairs.append((2 * place + core, 2 * other + core))
    return lax.ppermute(value, GRID, pairs)


def place_of(where_ref, stream, turning):
    flips = []
    for step in range(STEPS):
        first, second = (flip_of(turning, step, stream, core) for core in range(2))
        flips.append(jnp.where(where_ref[1] == 0, first, second))

    def at(rank):
        place = where_ref[0]
        for step in range(STEPS):
            if rank >> step & 1:
                place = place ^ flips[step]
        return place

    return at


def local_call(kernel, outs, scratch, where, arrays, limit):
    vmem = pl.BlockSpec(memory_space=pltpu.VMEM)
    return pl.pallas_call(
        kernel,
        in_specs=[pl.BlockSpec(memory_space=pltpu.SMEM)] + [vmem] * len(arrays),
        out_specs=[vmem] * len(outs),
        out_shape=[jax.ShapeDtypeStruct(shape, kind) for shape, kind in outs],
        scratch_shapes=scratch,
        compiler_params=pltpu.CompilerParams(vmem_limit_bytes=limit * 1024 * 1024),
    )(where, *arrays)


def put_in_place(where_ref, held, target, stream, turning=False):
    near, far = held
    half = PLACES // 2
    block = target.shape[0] // PLACES
    at = place_of(where_ref, stream, turning)
    for rank in range(PLACES):
        source = near if rank < half else far
        rows = pl.ds(pl.multiple_of(at(rank) * block, block), block)
        target[rows, :] = source[rank % half * block : (rank % half + 1) * block, :]


def column_cuts(widths):
    at, cuts = 0, []
    for width in widths:
        cuts.append(slice(at, at + width))
        at += width
    return cuts


def join(held, given):
    return jnp.concatenate([held, given], axis=0)


def part_join(held, given, cuts):
    return [join(held[:, cut], given[:, cut]) for cut in cuts]


def term_blocks(products, where, stream, grad_scale, turning=False):
    lefts = [half for left, _ in products for half in left]
    rights = [right for _, right in products]
    height = lefts[0].shape[1]
    cuts = column_cuts([right.shape[1] for right in rights])
    width = cuts[-1].stop
    block = height // PLACES
    half = PLACES // 2
    strip = height // 4

    def kernel(where_ref, *refs):
        left_refs, refs = refs[: len(lefts)], refs[len(lefts) :]
        right_refs, (near_ref, far_ref, whole) = refs[: len(rights)], refs[len(rights) :]
        at = place_of(where_ref, stream, turning)
        for number, cut in enumerate(cuts):
            upper, lower = left_refs[2 * number : 2 * number + 2]
            rows = upper.shape[0]
            for k in range(4):
                part = slice(k * strip, (k + 1) * strip)
                total = dot_tn(upper[:, part], right_refs[number][:rows, :])
                total = total + dot_tn(lower[:, part], right_refs[number][rows:, :])
                whole[part, cut] = (total * grad_scale).astype(BF)
        for rank in range(PLACES):
            source = pl.ds(pl.multiple_of(at(rank) * block, block), block)
            out = near_ref if rank < half else far_ref
            out[pl.ds(rank % half * block, block), :] = whole[source, :]

    outs = [((height // 2, width), BF)] * 2
    scratch = [pltpu.VMEM((height, width), BF)]
    return local_call(kernel, outs, scratch, where, (*lefts, *rights), 20)


def add(near, given):
    return near.astype(F32) + given.astype(F32)


def fold(near, given):
    half = near.shape[0] // 2
    send = add(near[half:], given[half:]).astype(BF)
    return add(near[:half], given[:half]).astype(BF), send


def last_sum(joined):
    half = joined.shape[0] // 2
    low, high = joined[:half], joined[half:]
    at_low = lax.axis_index("fsdp_x") == 0
    given = swap(jnp.where(at_low, high, low).astype(BF), "fsdp_x")
    return jnp.where(at_low, low, high) + given.astype(F32)


def split_rows(where_rows, send_ref, keep_ref, value_of):
    half = where_rows // 2
    send_ref[...] = value_of(slice(half, None)).astype(BF)
    keep_ref[...] = value_of(slice(None, half))


def attend_probs(queries, keys):
    factor = temper / math.sqrt(HEAD_DIM)
    scores = dot_nt(queries, keys) * factor
    lifted = jnp.exp(scores - jnp.max(scores, axis=-1, keepdims=True))
    return lifted / jnp.sum(lifted, axis=-1, keepdims=True)


def held_scratch(held):
    return pltpu.VMEM((2 * held[0].shape[0], held[0].shape[1]), BF)


def attention(rows, held_qk, held_vo, where):
    width = held_vo[0].shape[1] // 2
    count = 2 * rows[0].shape[0]
    model = rows[0].shape[1]

    def kernel(where_ref, upper, lower, near0, far0, near1, far1, *refs):
        qk_ref, v_ref, o_ref, send_ref, keep_ref, w0, w1 = refs
        half = count // 2
        put_in_place(where_ref, (near0, far0), w0, 0)
        qk_ref[:half, :] = dot_nn(upper[...], w0[...]).astype(BF)
        qk_ref[half:, :] = dot_nn(lower[...], w0[...]).astype(BF)
        put_in_place(where_ref, (near1, far1), w1, 1)
        v_ref[:half, :] = dot_nn(upper[...], w1[:, :width]).astype(BF)
        v_ref[half:, :] = dot_nn(lower[...], w1[:, :width]).astype(BF)
        for at in range(0, width, HEAD_DIM):
            head = slice(at, at + HEAD_DIM)
            probs = attend_probs(qk_ref[:, head], qk_ref[:, width + at : width + at + HEAD_DIM])
            o_ref[:, head] = dot_nn(probs.astype(BF), v_ref[:, head]).astype(BF)
        split_rows(count, send_ref, keep_ref, lambda span: dot_nt(o_ref[span, :], w1[:, width:]))

    outs = [
        ((count, 2 * width), BF),
        ((count, width), BF),
        ((count, width), BF),
        ((count // 2, model), BF),
        ((count // 2, model), F32),
    ]
    scratch = [held_scratch(held_qk), held_scratch(held_vo)]
    arrays = (*rows, *held_qk, *held_vo)
    return local_call(kernel, outs, scratch, where, arrays, 28)


def attention_back(rows, queries_keys, values, held_qk, held_vo, where):
    width = values.shape[1]
    count = values.shape[0]
    model = rows[0].shape[1]
    factor = temper / math.sqrt(HEAD_DIM)

    def kernel(where_ref, upper, lower, qk_ref, v_ref, near0, far0, near1, far1, *refs):
        dqk_ref, dv_ref, send_ref, keep_ref, mixed, w0, w1 = refs
        half = count // 2
        put_in_place(where_ref, (near1, far1), w1, 1)
        put_in_place(where_ref, (near0, far0), w0, 0)
        mixed[:half, :] = dot_nn(upper[...], w1[:, width:]).astype(BF)
        mixed[half:, :] = dot_nn(lower[...], w1[:, width:]).astype(BF)
        for at in range(0, width, HEAD_DIM):
            head = slice(at, at + HEAD_DIM)
            key_head = slice(width + at, width + at + HEAD_DIM)
            upstream = mixed[:, head]
            probs = attend_probs(qk_ref[:, head], qk_ref[:, key_head])
            dprobs = dot_nt(upstream, v_ref[:, head])
            inner = jnp.sum(probs * dprobs, axis=-1, keepdims=True)
            dscores = (probs * (dprobs - inner) * factor).astype(BF)
            dqk_ref[:, head] = dot_nn(dscores, qk_ref[:, key_head]).astype(BF)
            dqk_ref[:, key_head] = dot_tn(dscores, qk_ref[:, head]).astype(BF)
            dv_ref[:, head] = dot_tn(probs.astype(BF), upstream).astype(BF)

        def part(span):
            return dot_nt(dqk_ref[span, :], w0[...]) + dot_nt(dv_ref[span, :], w1[:, :width])

        split_rows(count, send_ref, keep_ref, part)

    outs = [
        ((count, 2 * width), BF),
        ((count, width), BF),
        ((count // 2, model), BF),
        ((count // 2, model), F32),
    ]
    scratch = [pltpu.VMEM((count, width), BF), held_scratch(held_qk), held_scratch(held_vo)]
    arrays = (*rows, queries_keys, values, *held_qk, *held_vo)
    return local_call(kernel, outs, scratch, where, arrays, 28)


def gelu_pair(hidden):
    root, cube = math.sqrt(2.0 / math.pi), 0.044715
    square = hidden * hidden
    curve = jnp.tanh(root * (hidden + cube * (square * hidden)))
    rise = 0.5 * (1.0 + curve)
    slope = 0.5 * hidden * (1.0 - curve * curve) * (root * (1.0 + 3.0 * cube * square))
    return hidden * rise, rise + slope


def feed_forward(rows, down_rows, held_in, held_back, where):
    width = held_in[0].shape[1]
    count = 2 * rows[0].shape[0]
    model = rows[0].shape[1]
    strip = width // 4

    def kernel(where_ref, upper, lower, d_upper, d_lower, near0, far0, near1, far1, *refs):
        act_ref, up_ref, send_ref, keep_ref, w0, w1 = refs
        half = count // 2
        put_in_place(where_ref, (near0, far0), w0, 0, True)
        put_in_place(where_ref, (near1, far1), w1, 1, True)
        for k in range(4):
            part = slice(k * strip, (k + 1) * strip)
            for at, left, down in ((0, upper, d_upper), (half, lower, d_lower)):
                active, slope = gelu_pair(dot_nn(left[...], w0[:, part]))
                act_ref[at : at + half, part] = active.astype(BF)
                grad = slope * dot_nn(down[...], w1[:, part])
                up_ref[at : at + half, part] = grad.astype(BF)
        split_rows(count, send_ref, keep_ref, lambda span: dot_nt(up_ref[span, :], w0[...]))

    outs = [
        ((count, width), BF),
        ((count, width), BF),
        ((count // 2, model), BF),
        ((count // 2, model), F32),
    ]
    scratch = [held_scratch(held_in), held_scratch(held_back)]
    arrays = (*rows, *down_rows, *held_in, *held_back)
    return local_call(kernel, outs, scratch, where, arrays, 32)


def down_project(activated, held_back, where):
    count = activated.shape[0]
    model = 2 * held_back[0].shape[0]

    def kernel(where_ref, act_ref, near, far, send_ref, keep_ref, w1):
        put_in_place(where_ref, (near, far), w1, 1, True)
        split_rows(count, send_ref, keep_ref, lambda span: dot_nt(act_ref[span, :], w1[...]))

    outs = [((count // 2, model), BF), ((count // 2, model), F32)]
    scratch = [held_scratch(held_back)]
    arrays = (activated, *held_back)
    return local_call(kernel, outs, scratch, where, arrays, 20)


def pair_up(own):
    return ordered(own, swap(own, "fsdp_x"), "fsdp_x")


def block_pass(tokens, layer_mod, w_qkv, w_out, w_in, w_back, out_grad, grad_scale):
    own_width, ffn_width = w_out.shape[0], w_in.shape[1]
    where = jnp.stack([lax.axis_index(ZY), lax.axis_index("sp_core")]).astype(jnp.int32)
    cut = 2 * own_width
    attn_pair = pair_up(jnp.concatenate([w_qkv, w_out.T], axis=1))
    ffn_own = jnp.concatenate([w_in, w_back.T], axis=1)
    ffn_given = after(swap(ffn_own, "fsdp_x"), attn_pair)
    ffn_pair = ordered(ffn_own, ffn_given, "fsdp_x")

    stream = tokens.astype(F32)
    normed_first, rstd_first = normalize(stream)
    input_first = (normed_first * (1.0 + layer_mod[1]) + layer_mod[0]).astype(BF)

    attn_cuts = column_cuts((cut, 2 * own_width))
    ffn_cuts = column_cuts((ffn_width, ffn_width))
    ffn_held = [ffn_pair[:, part] for part in ffn_cuts]
    ffn_given = [hop(held, 0, k, True) for k, held in enumerate(ffn_held)]
    attn_held = join(attn_pair, hop(attn_pair, 0))
    attn_given = hop(attn_held, 1)
    ffn_given = after(ffn_given, attn_held)
    ffn_held = [join(*pair) for pair in zip(ffn_held, ffn_given)]
    ffn_given = [hop(held, 1, k, True) for k, held in enumerate(ffn_held)]
    input_first = after(input_first, attn_pair)
    attn_held = part_join(attn_held, attn_given, attn_cuts)
    attn_given = [hop(held, 2, k) for k, held in enumerate(attn_held)]
    attn_held = [join(*pair) for pair in zip(attn_held, attn_given)]
    first_rows = spread(input_first, attn_held)
    attn_far = [hop(held, 3, k) for k, held in enumerate(attn_held)]
    ffn_given = after(ffn_given, attn_far)
    ffn_held = [join(*pair) for pair in zip(ffn_held, ffn_given)]
    ffn_given = [hop(held, 2, k, True) for k, held in enumerate(ffn_held)]

    out_grad = after(out_grad, first_rows)
    stream_grad = out_grad.astype(F32)
    down_grad = (layer_mod[5] * stream_grad).astype(BF)
    down_rows = spread(down_grad)

    held_qk, held_vo = tuple(zip(attn_held, attn_far))
    queries_keys, values, attended, send, keep = attention(first_rows, held_qk, held_vo, where)
    send, mine = collect(keep, send)
    ffn_given = after(ffn_given, send)
    ffn_held = [join(*pair) for pair in zip(ffn_held, ffn_given)]
    ffn_far = [hop(held, 3, k, True) for k, held in enumerate(ffn_held)]
    given = swap(send, "sp_x")
    middle = stream + layer_mod[2] * (mine + given.astype(F32))
    normed_second, rstd_second = normalize(middle)
    input_second = (normed_second * (1.0 + layer_mod[4]) + layer_mod[3]).astype(BF)
    second_rows = spread(input_second)
    ffn_far = after(ffn_far, second_rows)
    held_in, held_back = tuple(zip(ffn_held, ffn_far))

    activated, up_grad, send, keep = feed_forward(second_rows, down_rows, held_in, held_back, where)
    send, mine = collect(keep, send)
    up_rows = after(up_grad, send)
    near_in, far_in = term_blocks([(second_rows, up_rows)], where, 0, grad_scale, True)
    given_in = hop(far_in, 3, 0, True)
    act_rows = after(activated, far_in)
    near_back, far_back = term_blocks([(down_rows, act_rows)], where, 1, grad_scale, True)
    given_back = hop(far_back, 3, 1, True)
    back_second = mine + after(swap(send, "sp_x"), far_back).astype(F32)
    stream_grad = stream_grad + norm_back(
        normed_second, rstd_second, back_second * (1.0 + layer_mod[4])
    )
    attn_grad = (layer_mod[2] * stream_grad).astype(BF)
    out_send, out_keep = down_project(after(activated, attn_grad), held_back, where)
    attn_rows = spread(attn_grad, out_keep)
    grad_qk, grad_v, send, keep = attention_back(
        attn_rows, queries_keys, values, held_qk, held_vo, where
    )
    near_qk, far_qk = term_blocks([(first_rows, grad_qk)], where, 0, grad_scale, True)
    given_qk = hop(far_qk, 3, 0, True)
    grad_v, attended = after((grad_v, attended), far_qk)
    products = [(first_rows, grad_v), (attn_rows, attended)]
    near_vo, far_vo = term_blocks(products, where, 1, grad_scale, True)
    given_vo = hop(far_vo, 3, 1, True)

    def fold_on(twos, givens, step):
        twos = [fold(two, given) for two, given in zip(twos, givens)]
        hops = [hop(two[1], step, k, True) for k, two in enumerate(twos)]
        return [two[0] for two in twos], [two[1] for two in twos], hops

    givens = after((given_in, given_back), far_vo)
    near_ffn, sent_ffn, given_ffn = fold_on((near_in, near_back), givens, 2)
    send, mine = collect(keep, after(send, sent_ffn))
    given_first = swap(send, "sp_x")
    givens = after((given_qk, given_vo), send)
    near_attn, sent_attn, given_attn = fold_on((near_qk, near_vo), givens, 2)
    out_send, out_mine = collect(out_keep, after(out_send, sent_attn))
    near_ffn, sent_ffn, given_ffn = fold_on(near_ffn, after(given_ffn, out_send), 1)
    back_first = mine + after(given_first, sent_ffn).astype(F32)
    input_grad = stream_grad + norm_back(
        normed_first, rstd_first, back_first * (1.0 + layer_mod[1])
    )
    givens = after(given_attn, input_grad)
    near_attn, sent_attn, given_attn = fold_on(near_attn, givens, 1)
    near_ffn, sent_ffn, given_ffn = fold_on(near_ffn, after(given_ffn, sent_attn), 0)
    given = after(swap(out_send, "sp_x"), sent_ffn)
    final_out = (middle + layer_mod[5] * (out_mine + given.astype(F32))).astype(BF)
    givens = after(given_attn, final_out)
    near_attn, sent_attn, given_attn = fold_on(near_attn, givens, 0)

    def total(nears, givens):
        return jnp.concatenate([add(near, given) for near, given in zip(nears, givens)], axis=1)

    total_ffn = total(near_ffn, after(given_ffn, sent_attn))
    sum_ffn = last_sum(total_ffn)
    sum_attn = last_sum(total(near_attn, after(given_attn, total_ffn)))
    return (
        final_out,
        input_grad,
        sum_attn[:, : 3 * own_width],
        sum_attn[:, 3 * own_width :].T,
        sum_ffn[:, :ffn_width],
        sum_ffn[:, ffn_width:].T,
    )


def body(tokens, modulation, w_qkv, w_out, w_in, w_back, out_grad):
    local_seq = tokens.shape[1]
    own_width = w_qkv.shape[3]
    grad_scale = 1.0 / math.sqrt(local_seq * lax.axis_size(FSDP) * lax.axis_size(SP))
    final_out, input_grad, grad_qkv, grad_out, grad_in, grad_back = block_pass(
        tokens[0],
        modulation[0, 0],
        w_qkv[0].reshape(-1, 3 * own_width),
        w_out[0],
        w_in[0],
        w_back[0],
        out_grad[0],
        grad_scale,
    )
    return (
        final_out[None],
        input_grad[None],
        grad_qkv.reshape(1, -1, 3, own_width),
        grad_out[None],
        grad_in[None],
        grad_back[None],
    )


def solution(mesh):
    torus = Mesh(
        mesh.devices.reshape(4, 4, 2, 2, 2),
        (*FSDP, *SP),
    )
    return jax.shard_map(
        body,
        mesh=torus,
        in_specs=(
            P(FSDP, SP, None),
            P(FSDP, None, None, None),
            P(None, FSDP, None, SP),
            P(None, SP, FSDP),
            P(None, FSDP, SP),
            P(None, SP, FSDP),
            P(FSDP, SP, None),
        ),
        out_specs=(
            P(FSDP, SP, None),
            P(FSDP, SP, None),
            P(None, FSDP, None, SP),
            P(None, SP, FSDP),
            P(None, FSDP, SP),
            P(None, SP, FSDP),
        ),
        check_vma=False,
    )
```

```python
import math

import jax
import jax.numpy as jnp
from jax import lax
from jax.experimental import pallas as pl
from jax.experimental.pallas import tpu as pltpu
from jax.sharding import Mesh
from jax.sharding import PartitionSpec as P

HEAD_DIM = 128
ZY, FSDP_X = ("fsdp_z", "fsdp_y"), "fsdp_x"
FSDP = (*ZY, FSDP_X)
SP = SP_X, SP_CORE = "sp_x", "sp_core"
SWAP = ((0, 1), (1, 0))
GRID = (*ZY, SP_CORE)
PLACES = 16
FLIPS = (1, 4, 3, 12)
STEPS = 4

ln_eps = 1e-06
temper = 2.5
BF = jnp.bfloat16
F32 = jnp.float32


def normalize(stream):
    mean_part = jnp.mean(stream, axis=-1, keepdims=True)
    centred = stream - mean_part
    rstd = lax.rsqrt(jnp.mean(centred * centred, axis=-1, keepdims=True) + ln_eps)
    return (centred * rstd, rstd)


def norm_back(normed, rstd, incoming):
    first = jnp.mean(incoming, axis=-1, keepdims=True)
    second = jnp.mean(incoming * normed, axis=-1, keepdims=True)
    return rstd * (incoming - first - normed * second)


def dot_nn(left, right):
    return jnp.dot(left, right, preferred_element_type=F32)


def dot_nt(left, right):
    return lax.dot_general(left, right, (((1,), (1,)), ((), ())), preferred_element_type=F32)


def dot_tn(left, right):
    return lax.dot_general(left, right, (((0,), (0,)), ((), ())), preferred_element_type=F32)


def swap(value, axis):
    return lax.ppermute(value, axis, SWAP)


def after(value, *earlier):
    return lax.optimization_barrier((value, earlier))[0]


def spread(own, *earlier):
    across = after(swap(own, SP_X), earlier)
    pair = jnp.concatenate([own, across], axis=0)
    return pair, swap(pair, SP_CORE)


def collect(keep, give):
    rows = keep.shape[0] // 2
    given = swap(give, SP_CORE)
    send = (keep[rows:] + given[rows:].astype(F32)).astype(BF)
    return send, keep[:rows] + given[:rows].astype(F32)


def ordered(own, other, axis):
    first = jnp.concatenate([own, other], axis=0)
    second = jnp.concatenate([other, own], axis=0)
    return jnp.where(lax.axis_index(axis) == 0, first, second)


def flip_of(turning, step, stream, core):
    if turning:
        return FLIPS[(2 * stream + core + step) % STEPS]
    inner = FLIPS[:2] if core == (step >= 2) else FLIPS[2:]
    return inner[(step % 2) ^ (stream if step >= 2 else 0)]


def hop(value, step, stream=0, turning=False):
    pairs = []
    for place in range(PLACES):
        for core in range(2):
            other = place ^ flip_of(turning, step, stream, core)
            pairs.append((2 * place + core, 2 * other + core))
    return lax.ppermute(value, GRID, pairs)


def place_of(where_ref, stream, turning):
    flips = []
    for step in range(STEPS):
        first, second = (flip_of(turning, step, stream, core) for core in range(2))
        flips.append(jnp.where(where_ref[1] == 0, first, second))

    def at(rank):
        place = where_ref[0]
        for step in range(STEPS):
            if rank >> step & 1:
                place = place ^ flips[step]
        return place

    return at


def local_call(kernel, outs, scratch, where, arrays, limit):
    vmem = pl.BlockSpec(memory_space=pltpu.VMEM)
    return pl.pallas_call(
        kernel,
        in_specs=[pl.BlockSpec(memory_space=pltpu.SMEM)] + [vmem] * len(arrays),
        out_specs=[vmem] * len(outs),
        out_shape=[jax.ShapeDtypeStruct(shape, kind) for shape, kind in outs],
        scratch_shapes=scratch,
        compiler_params=pltpu.CompilerParams(vmem_limit_bytes=limit * 1024 * 1024),
    )(where, *arrays)


def put_in_place(where_ref, held, target, stream, turning=False):
    near, far = held
    half = PLACES // 2
    block = target.shape[0] // PLACES
    at = place_of(where_ref, stream, turning)
    for rank in range(PLACES):
        source = near if rank < half else far
        rows = pl.ds(pl.multiple_of(at(rank) * block, block), block)
        target[rows, :] = source[rank % half * block : (rank % half + 1) * block, :]


def column_cuts(widths):
    at, cuts = 0, []
    for width in widths:
        cuts.append(slice(at, at + width))
        at += width
    return cuts


def join(held, given):
    return jnp.concatenate([held, given], axis=0)


def part_join(held, given, cuts):
    return [join(held[:, cut], given[:, cut]) for cut in cuts]


def term_blocks(products, where, stream, grad_scale, turning=False):
    lefts = [half for left, _ in products for half in left]
    rights = [right for _, right in products]
    height = lefts[0].shape[1]
    cuts = column_cuts([right.shape[1] for right in rights])
    width = cuts[-1].stop
    block = height // PLACES
    half = PLACES // 2
    strip = height // 4

    def kernel(where_ref, *refs):
        left_refs, refs = refs[: len(lefts)], refs[len(lefts) :]
        right_refs, (near_ref, far_ref, whole) = refs[: len(rights)], refs[len(rights) :]
        at = place_of(where_ref, stream, turning)
        for number, cut in enumerate(cuts):
            upper, lower = left_refs[2 * number : 2 * number + 2]
            rows = upper.shape[0]
            for k in range(4):
                part = slice(k * strip, (k + 1) * strip)
                total = dot_tn(upper[:, part], right_refs[number][:rows, :])
                total = total + dot_tn(lower[:, part], right_refs[number][rows:, :])
                whole[part, cut] = (total * grad_scale).astype(BF)
        for rank in range(PLACES):
            source = pl.ds(pl.multiple_of(at(rank) * block, block), block)
            out = near_ref if rank < half else far_ref
            out[pl.ds(rank % half * block, block), :] = whole[source, :]

    outs = [((height // 2, width), BF)] * 2
    scratch = [pltpu.VMEM((height, width), BF)]
    return local_call(kernel, outs, scratch, where, (*lefts, *rights), 20)


def add(near, given):
    return near.astype(F32) + given.astype(F32)


def fold(near, given):
    half = near.shape[0] // 2
    send = add(near[half:], given[half:]).astype(BF)
    return add(near[:half], given[:half]).astype(BF), send


def last_sum(joined):
    half = joined.shape[0] // 2
    low, high = joined[:half], joined[half:]
    at_low = lax.axis_index(FSDP_X) == 0
    given = swap(jnp.where(at_low, high, low).astype(BF), FSDP_X)
    return jnp.where(at_low, low, high) + given.astype(F32)


def split_rows(where_rows, send_ref, keep_ref, value_of):
    half = where_rows // 2
    send_ref[...] = value_of(slice(half, None)).astype(BF)
    keep_ref[...] = value_of(slice(None, half))


def attend_probs(queries, keys):
    factor = temper / math.sqrt(HEAD_DIM)
    scores = dot_nt(queries, keys) * factor
    lifted = jnp.exp(scores - jnp.max(scores, axis=-1, keepdims=True))
    return lifted / jnp.sum(lifted, axis=-1, keepdims=True)


def held_scratch(held):
    return pltpu.VMEM((2 * held[0].shape[0], held[0].shape[1]), BF)


def attention(rows, held_qk, held_vo, where):
    width = held_vo[0].shape[1] // 2
    count = 2 * rows[0].shape[0]
    model = rows[0].shape[1]

    def kernel(where_ref, upper, lower, near0, far0, near1, far1, *refs):
        qk_ref, v_ref, o_ref, send_ref, keep_ref, w0, w1 = refs
        half = count // 2
        put_in_place(where_ref, (near0, far0), w0, 0)
        qk_ref[:half, :] = dot_nn(upper[...], w0[...]).astype(BF)
        qk_ref[half:, :] = dot_nn(lower[...], w0[...]).astype(BF)
        put_in_place(where_ref, (near1, far1), w1, 1)
        v_ref[:half, :] = dot_nn(upper[...], w1[:, :width]).astype(BF)
        v_ref[half:, :] = dot_nn(lower[...], w1[:, :width]).astype(BF)
        for at in range(0, width, HEAD_DIM):
            head = slice(at, at + HEAD_DIM)
            probs = attend_probs(qk_ref[:, head], qk_ref[:, width + at : width + at + HEAD_DIM])
            o_ref[:, head] = dot_nn(probs.astype(BF), v_ref[:, head]).astype(BF)
        split_rows(count, send_ref, keep_ref, lambda span: dot_nt(o_ref[span, :], w1[:, width:]))

    outs = [
        ((count, 2 * width), BF),
        ((count, width), BF),
        ((count, width), BF),
        ((count // 2, model), BF),
        ((count // 2, model), F32),
    ]
    scratch = [held_scratch(held_qk), held_scratch(held_vo)]
    arrays = (*rows, *held_qk, *held_vo)
    return local_call(kernel, outs, scratch, where, arrays, 28)


def attention_back(rows, queries_keys, values, held_qk, held_vo, where):
    width = values.shape[1]
    count = values.shape[0]
    model = rows[0].shape[1]
    factor = temper / math.sqrt(HEAD_DIM)

    def kernel(where_ref, upper, lower, qk_ref, v_ref, near0, far0, near1, far1, *refs):
        dqk_ref, dv_ref, send_ref, keep_ref, mixed, w0, w1 = refs
        half = count // 2
        put_in_place(where_ref, (near1, far1), w1, 1)
        put_in_place(where_ref, (near0, far0), w0, 0)
        mixed[:half, :] = dot_nn(upper[...], w1[:, width:]).astype(BF)
        mixed[half:, :] = dot_nn(lower[...], w1[:, width:]).astype(BF)
        for at in range(0, width, HEAD_DIM):
            head = slice(at, at + HEAD_DIM)
            key_head = slice(width + at, width + at + HEAD_DIM)
            upstream = mixed[:, head]
            probs = attend_probs(qk_ref[:, head], qk_ref[:, key_head])
            dprobs = dot_nt(upstream, v_ref[:, head])
            inner = jnp.sum(probs * dprobs, axis=-1, keepdims=True)
            dscores = (probs * (dprobs - inner) * factor).astype(BF)
            dqk_ref[:, head] = dot_nn(dscores, qk_ref[:, key_head]).astype(BF)
            dqk_ref[:, key_head] = dot_tn(dscores, qk_ref[:, head]).astype(BF)
            dv_ref[:, head] = dot_tn(probs.astype(BF), upstream).astype(BF)

        def part(span):
            return dot_nt(dqk_ref[span, :], w0[...]) + dot_nt(dv_ref[span, :], w1[:, :width])

        split_rows(count, send_ref, keep_ref, part)

    outs = [
        ((count, 2 * width), BF),
        ((count, width), BF),
        ((count // 2, model), BF),
        ((count // 2, model), F32),
    ]
    scratch = [pltpu.VMEM((count, width), BF), held_scratch(held_qk), held_scratch(held_vo)]
    arrays = (*rows, queries_keys, values, *held_qk, *held_vo)
    return local_call(kernel, outs, scratch, where, arrays, 28)


def gelu_pair(hidden):
    root, cube = math.sqrt(2.0 / math.pi), 0.044715
    square = hidden * hidden
    curve = jnp.tanh(root * (hidden + cube * (square * hidden)))
    rise = 0.5 * (1.0 + curve)
    slope = 0.5 * hidden * (1.0 - curve * curve) * (root * (1.0 + 3.0 * cube * square))
    return hidden * rise, rise + slope


def feed_forward(rows, down_rows, held_in, held_back, where):
    width = held_in[0].shape[1]
    count = 2 * rows[0].shape[0]
    model = rows[0].shape[1]
    strip = width // 4

    def kernel(where_ref, upper, lower, d_upper, d_lower, near0, far0, near1, far1, *refs):
        act_ref, up_ref, send_ref, keep_ref, w0, w1 = refs
        half = count // 2
        put_in_place(where_ref, (near0, far0), w0, 0, True)
        put_in_place(where_ref, (near1, far1), w1, 1, True)
        for k in range(4):
            part = slice(k * strip, (k + 1) * strip)
            for at, left, down in ((0, upper, d_upper), (half, lower, d_lower)):
                active, slope = gelu_pair(dot_nn(left[...], w0[:, part]))
                act_ref[at : at + half, part] = active.astype(BF)
                grad = slope * dot_nn(down[...], w1[:, part])
                up_ref[at : at + half, part] = grad.astype(BF)
        split_rows(count, send_ref, keep_ref, lambda span: dot_nt(up_ref[span, :], w0[...]))

    outs = [
        ((count, width), BF),
        ((count, width), BF),
        ((count // 2, model), BF),
        ((count // 2, model), F32),
    ]
    scratch = [held_scratch(held_in), held_scratch(held_back)]
    arrays = (*rows, *down_rows, *held_in, *held_back)
    return local_call(kernel, outs, scratch, where, arrays, 32)


def down_project(activated, held_back, where):
    count = activated.shape[0]
    model = 2 * held_back[0].shape[0]

    def kernel(where_ref, act_ref, near, far, send_ref, keep_ref, w1):
        put_in_place(where_ref, (near, far), w1, 1, True)
        split_rows(count, send_ref, keep_ref, lambda span: dot_nt(act_ref[span, :], w1[...]))

    outs = [((count // 2, model), BF), ((count // 2, model), F32)]
    scratch = [held_scratch(held_back)]
    arrays = (activated, *held_back)
    return local_call(kernel, outs, scratch, where, arrays, 20)


def pair_up(own):
    return ordered(own, swap(own, FSDP_X), FSDP_X)


def block_pass(tokens, layer_mod, w_qkv, w_out, w_in, w_back, out_grad, grad_scale):
    own_width, ffn_width = w_out.shape[0], w_in.shape[1]
    where = jnp.stack([lax.axis_index(ZY), lax.axis_index(SP_CORE)]).astype(jnp.int32)
    cut = 2 * own_width
    attn_pair = pair_up(jnp.concatenate([w_qkv, w_out.T], axis=1))
    ffn_own = jnp.concatenate([w_in, w_back.T], axis=1)
    ffn_given = after(swap(ffn_own, FSDP_X), attn_pair)
    ffn_pair = ordered(ffn_own, ffn_given, FSDP_X)

    stream = tokens.astype(F32)
    normed_first, rstd_first = normalize(stream)
    input_first = (normed_first * (1.0 + layer_mod[1]) + layer_mod[0]).astype(BF)

    attn_cuts = column_cuts((cut, 2 * own_width))
    ffn_cuts = column_cuts((ffn_width, ffn_width))
    ffn_held = [ffn_pair[:, part] for part in ffn_cuts]
    ffn_given = [hop(held, 0, k, True) for k, held in enumerate(ffn_held)]
    attn_held = join(attn_pair, hop(attn_pair, 0))
    attn_given = hop(attn_held, 1)
    ffn_given = after(ffn_given, attn_held)
    ffn_held = [join(*pair) for pair in zip(ffn_held, ffn_given)]
    ffn_given = [hop(held, 1, k, True) for k, held in enumerate(ffn_held)]
    input_first = after(input_first, attn_pair)
    attn_held = part_join(attn_held, attn_given, attn_cuts)
    attn_given = [hop(held, 2, k) for k, held in enumerate(attn_held)]
    attn_held = [join(*pair) for pair in zip(attn_held, attn_given)]
    first_rows = spread(input_first, attn_held)
    attn_far = [hop(held, 3, k) for k, held in enumerate(attn_held)]
    ffn_given = after(ffn_given, attn_far)
    ffn_held = [join(*pair) for pair in zip(ffn_held, ffn_given)]
    ffn_given = [hop(held, 2, k, True) for k, held in enumerate(ffn_held)]

    out_grad = after(out_grad, first_rows)
    stream_grad = out_grad.astype(F32)
    down_grad = (layer_mod[5] * stream_grad).astype(BF)
    down_rows = spread(down_grad)

    held_qk, held_vo = tuple(zip(attn_held, attn_far))
    queries_keys, values, attended, send, keep = attention(first_rows, held_qk, held_vo, where)
    send, mine = collect(keep, send)
    ffn_given = after(ffn_given, send)
    ffn_held = [join(*pair) for pair in zip(ffn_held, ffn_given)]
    ffn_far = [hop(held, 3, k, True) for k, held in enumerate(ffn_held)]
    given = swap(send, SP_X)
    middle = stream + layer_mod[2] * (mine + given.astype(F32))
    normed_second, rstd_second = normalize(middle)
    input_second = (normed_second * (1.0 + layer_mod[4]) + layer_mod[3]).astype(BF)
    second_rows = spread(input_second)
    ffn_far = after(ffn_far, second_rows)
    held_in, held_back = tuple(zip(ffn_held, ffn_far))

    activated, up_grad, send, keep = feed_forward(second_rows, down_rows, held_in, held_back, where)
    send, mine = collect(keep, send)
    up_rows = after(up_grad, send)
    near_in, far_in = term_blocks([(second_rows, up_rows)], where, 0, grad_scale, True)
    given_in = hop(far_in, 3, 0, True)
    act_rows = after(activated, far_in)
    near_back, far_back = term_blocks([(down_rows, act_rows)], where, 1, grad_scale, True)
    given_back = hop(far_back, 3, 1, True)
    back_second = mine + after(swap(send, SP_X), far_back).astype(F32)
    stream_grad = stream_grad + norm_back(
        normed_second, rstd_second, back_second * (1.0 + layer_mod[4])
    )
    attn_grad = (layer_mod[2] * stream_grad).astype(BF)
    out_send, out_keep = down_project(after(activated, attn_grad), held_back, where)
    attn_rows = spread(attn_grad, out_keep)
    grad_qk, grad_v, send, keep = attention_back(
        attn_rows, queries_keys, values, held_qk, held_vo, where
    )
    near_qk, far_qk = term_blocks([(first_rows, grad_qk)], where, 0, grad_scale, True)
    given_qk = hop(far_qk, 3, 0, True)
    grad_v, attended = after((grad_v, attended), far_qk)
    products = [(first_rows, grad_v), (attn_rows, attended)]
    near_vo, far_vo = term_blocks(products, where, 1, grad_scale, True)
    given_vo = hop(far_vo, 3, 1, True)

    def fold_on(twos, givens, step):
        twos = [fold(two, given) for two, given in zip(twos, givens)]
        hops = [hop(two[1], step, k, True) for k, two in enumerate(twos)]
        return [two[0] for two in twos], [two[1] for two in twos], hops

    givens = after((given_in, given_back), far_vo)
    near_ffn, sent_ffn, given_ffn = fold_on((near_in, near_back), givens, 2)
    send, mine = collect(keep, after(send, sent_ffn))
    given_first = swap(send, SP_X)
    out_send, out_mine = collect(out_keep, after(out_send, send))
    given_out = swap(out_send, SP_X)
    back_first = mine + after(given_first, out_send).astype(F32)
    input_grad = stream_grad + norm_back(
        normed_first, rstd_first, back_first * (1.0 + layer_mod[1])
    )
    givens = after((given_qk, given_vo), input_grad)
    near_attn, sent_attn, given_attn = fold_on((near_qk, near_vo), givens, 2)
    near_ffn, sent_ffn, given_ffn = fold_on(near_ffn, after(given_ffn, sent_attn), 1)
    given_out = after(given_out, sent_ffn)
    final_out = (middle + layer_mod[5] * (out_mine + given_out.astype(F32))).astype(BF)
    givens = after(given_attn, final_out)
    near_attn, sent_attn, given_attn = fold_on(near_attn, givens, 1)
    near_ffn, sent_ffn, given_ffn = fold_on(near_ffn, after(given_ffn, sent_attn), 0)
    givens = after(given_attn, sent_ffn)
    near_attn, sent_attn, given_attn = fold_on(near_attn, givens, 0)

    def total(nears, givens):
        return jnp.concatenate([add(near, given) for near, given in zip(nears, givens)], axis=1)

    total_ffn = total(near_ffn, after(given_ffn, sent_attn))
    sum_ffn = last_sum(total_ffn)
    sum_attn = last_sum(total(near_attn, after(given_attn, total_ffn)))
    return (
        final_out,
        input_grad,
        sum_attn[:, : 3 * own_width],
        sum_attn[:, 3 * own_width :].T,
        sum_ffn[:, :ffn_width],
        sum_ffn[:, ffn_width:].T,
    )


def body(tokens, modulation, w_qkv, w_out, w_in, w_back, out_grad):
    local_seq = tokens.shape[1]
    own_width = w_qkv.shape[3]
    grad_scale = 1.0 / math.sqrt(local_seq * lax.axis_size(FSDP) * lax.axis_size(SP))
    final_out, input_grad, grad_qkv, grad_out, grad_in, grad_back = block_pass(
        tokens[0],
        modulation[0, 0],
        w_qkv[0].reshape(-1, 3 * own_width),
        w_out[0],
        w_in[0],
        w_back[0],
        out_grad[0],
        grad_scale,
    )
    return (
        final_out[None],
        input_grad[None],
        grad_qkv.reshape(1, -1, 3, own_width),
        grad_out[None],
        grad_in[None],
        grad_back[None],
    )


def solution(mesh):
    torus = Mesh(
        mesh.devices.reshape(4, 4, 2, 2, 2),
        (*FSDP, *SP),
    )
    return jax.shard_map(
        body,
        mesh=torus,
        in_specs=(
            P(FSDP, SP, None),
            P(FSDP, None, None, None),
            P(None, FSDP, None, SP),
            P(None, SP, FSDP),
            P(None, FSDP, SP),
            P(None, SP, FSDP),
            P(FSDP, SP, None),
        ),
        out_specs=(
            P(FSDP, SP, None),
            P(FSDP, SP, None),
            P(None, FSDP, None, SP),
            P(None, SP, FSDP),
            P(None, FSDP, SP),
            P(None, SP, FSDP),
        ),
        check_vma=False,
    )
```

```python
import math

import jax
import jax.numpy as jnp
from jax import lax
from jax.experimental import pallas as pl
from jax.experimental.pallas import tpu as pltpu
from jax.sharding import Mesh
from jax.sharding import PartitionSpec as P

HEAD_DIM = 128
ZY, FSDP_X = ("fsdp_z", "fsdp_y"), "fsdp_x"
FSDP = (*ZY, FSDP_X)
SP = SP_X, SP_CORE = "sp_x", "sp_core"
SWAP = ((0, 1), (1, 0))
GRID = (*ZY, SP_CORE)
PLACES = 16
G_IN, G_BACK, G_QK, G_VO = "gi", "gb", "gq", "gv"
FLIPS = (1, 4, 3, 12)
STEPS = 4
FFN_TURN, ATTN_TURN = 4, 1

ln_eps = 1e-06
temper = 2.5
BF = jnp.bfloat16
F32 = jnp.float32


def normalize(stream):
    mean_part = jnp.mean(stream, axis=-1, keepdims=True)
    centred = stream - mean_part
    rstd = lax.rsqrt(jnp.mean(centred * centred, axis=-1, keepdims=True) + ln_eps)
    return (centred * rstd, rstd)


def norm_back(normed, rstd, incoming):
    first = jnp.mean(incoming, axis=-1, keepdims=True)
    second = jnp.mean(incoming * normed, axis=-1, keepdims=True)
    return rstd * (incoming - first - normed * second)


def dot_nn(left, right):
    return jnp.dot(left, right, preferred_element_type=F32)


def dot_nt(left, right):
    return lax.dot_general(left, right, (((1,), (1,)), ((), ())), preferred_element_type=F32)


def dot_tn(left, right):
    return lax.dot_general(left, right, (((0,), (0,)), ((), ())), preferred_element_type=F32)


def swap(value, axis):
    return lax.ppermute(value, axis, SWAP)


def after(value, *earlier):
    return lax.optimization_barrier((value, earlier))[0]


def spread(own, *earlier):
    across = after(swap(own, SP_X), earlier)
    pair = jnp.concatenate([own, across], axis=0)
    return pair, swap(pair, SP_CORE)


def collect(keep, give):
    rows = keep.shape[0] // 2
    given = swap(give, SP_CORE)
    send = (keep[rows:] + given[rows:].astype(F32)).astype(BF)
    return send, keep[:rows] + given[:rows].astype(F32)


def ordered(own, other, axis):
    first = jnp.concatenate([own, other], axis=0)
    second = jnp.concatenate([other, own], axis=0)
    return jnp.where(lax.axis_index(axis) == 0, first, second)


def flip_of(turning, step, stream, core):
    if turning == ATTN_TURN:
        inner = FLIPS[0::2] if core != (step >= 2) else FLIPS[1::2]
        return inner[stream ^ (step in (1, 2))]
    if turning:
        return FLIPS[(2 * stream + core + step + turning) % STEPS]
    inner = FLIPS[0::2] if core == (step >= 2) else FLIPS[1::2]
    return inner[(step % 2) ^ (stream if step >= 2 else 0)]


def hop(value, step, stream=0, turning=0):
    pairs = []
    for place in range(PLACES):
        for core in range(2):
            other = place ^ flip_of(turning, step, stream, core)
            pairs.append((2 * place + core, 2 * other + core))
    return lax.ppermute(value, GRID, pairs)


def place_of(where_ref, stream, turning):
    flips = []
    for step in range(STEPS):
        first, second = (flip_of(turning, step, stream, core) for core in range(2))
        flips.append(jnp.where(where_ref[1] == 0, first, second))

    def at(rank):
        place = where_ref[0]
        for step in range(STEPS):
            if rank >> step & 1:
                place = place ^ flips[step]
        return place

    return at


def local_call(kernel, outs, scratch, where, arrays, limit):
    vmem = pl.BlockSpec(memory_space=pltpu.VMEM)
    return pl.pallas_call(
        kernel,
        in_specs=[pl.BlockSpec(memory_space=pltpu.SMEM)] + [vmem] * len(arrays),
        out_specs=[vmem] * len(outs),
        out_shape=[jax.ShapeDtypeStruct(shape, kind) for shape, kind in outs],
        scratch_shapes=scratch,
        compiler_params=pltpu.CompilerParams(vmem_limit_bytes=limit * 1024 * 1024),
    )(where, *arrays)


def put_in_place(where_ref, held, target, stream, turning=0):
    near, far = held
    half = PLACES // 2
    block = target.shape[0] // PLACES
    at = place_of(where_ref, stream, turning)
    for rank in range(PLACES):
        source = near if rank < half else far
        rows = pl.ds(pl.multiple_of(at(rank) * block, block), block)
        target[rows, :] = source[rank % half * block : (rank % half + 1) * block, :]


def column_cuts(widths):
    at, cuts = 0, []
    for width in widths:
        cuts.append(slice(at, at + width))
        at += width
    return cuts


def join(held, given):
    return jnp.concatenate([held, given], axis=0)


def part_join(held, given, cuts):
    return [join(held[:, cut], given[:, cut]) for cut in cuts]


def term_blocks(products, where, stream, grad_scale, turning=0):
    lefts = [half for left, _ in products for half in left]
    rights = [right for _, right in products]
    height = lefts[0].shape[1]
    cuts = column_cuts([right.shape[1] for right in rights])
    width = cuts[-1].stop
    block = height // PLACES
    half = PLACES // 2
    strip = height // 4

    def kernel(where_ref, *refs):
        left_refs, refs = refs[: len(lefts)], refs[len(lefts) :]
        right_refs, (near_ref, far_ref, whole) = refs[: len(rights)], refs[len(rights) :]
        at = place_of(where_ref, stream, turning)
        for number, cut in enumerate(cuts):
            upper, lower = left_refs[2 * number : 2 * number + 2]
            rows = upper.shape[0]
            for k in range(4):
                part = slice(k * strip, (k + 1) * strip)
                total = dot_tn(upper[:, part], right_refs[number][:rows, :])
                total = total + dot_tn(lower[:, part], right_refs[number][rows:, :])
                whole[part, cut] = (total * grad_scale).astype(BF)
        for rank in range(PLACES):
            source = pl.ds(pl.multiple_of(at(rank) * block, block), block)
            out = near_ref if rank < half else far_ref
            out[pl.ds(rank % half * block, block), :] = whole[source, :]

    outs = [((height // 2, width), BF)] * 2
    scratch = [pltpu.VMEM((height, width), BF)]
    return local_call(kernel, outs, scratch, where, (*lefts, *rights), 20)


def add(near, given):
    return near.astype(F32) + given.astype(F32)


def fold(near, given):
    half = near.shape[0] // 2
    send = add(near[half:], given[half:]).astype(BF)
    return add(near[:half], given[:half]).astype(BF), send


def last_sum(joined):
    half = joined.shape[0] // 2
    low, high = joined[:half], joined[half:]
    at_low = lax.axis_index(FSDP_X) == 0
    given = swap(jnp.where(at_low, high, low).astype(BF), FSDP_X)
    return jnp.where(at_low, low, high) + given.astype(F32)


def split_rows(where_rows, send_ref, keep_ref, value_of):
    half = where_rows // 2
    send_ref[...] = value_of(slice(half, None)).astype(BF)
    keep_ref[...] = value_of(slice(None, half))


def attend_lifted(queries, keys):
    factor = temper / math.sqrt(HEAD_DIM)
    scores = dot_nt(queries, keys) * factor
    lifted = jnp.exp(scores - jnp.max(scores, axis=-1, keepdims=True))
    return lifted, 1.0 / jnp.sum(lifted, axis=-1, keepdims=True)


def held_scratch(held):
    return pltpu.VMEM((2 * held[0].shape[0], held[0].shape[1]), BF)


def attention(rows, held_qk, held_vo, where):
    width = held_vo[0].shape[1] // 2
    count = 2 * rows[0].shape[0]
    model = rows[0].shape[1]

    def kernel(where_ref, upper, lower, near0, far0, near1, far1, *refs):
        qk_ref, v_ref, o_ref, send_ref, keep_ref, w0, w1 = refs
        half = count // 2
        put_in_place(where_ref, (near0, far0), w0, 0)
        qk_ref[:half, :] = dot_nn(upper[...], w0[...]).astype(BF)
        qk_ref[half:, :] = dot_nn(lower[...], w0[...]).astype(BF)
        put_in_place(where_ref, (near1, far1), w1, 1)
        v_ref[:half, :] = dot_nn(upper[...], w1[:, :width]).astype(BF)
        v_ref[half:, :] = dot_nn(lower[...], w1[:, :width]).astype(BF)
        for at in range(0, width, HEAD_DIM):
            head = slice(at, at + HEAD_DIM)
            key_head = slice(width + at, width + at + HEAD_DIM)
            lifted, scale = attend_lifted(qk_ref[:, head], qk_ref[:, key_head])
            o_ref[:, head] = (dot_nn(lifted.astype(BF), v_ref[:, head]) * scale).astype(BF)
        split_rows(count, send_ref, keep_ref, lambda span: dot_nt(o_ref[span, :], w1[:, width:]))

    outs = [
        ((count, 2 * width), BF),
        ((count, width), BF),
        ((count, width), BF),
        ((count // 2, model), BF),
        ((count // 2, model), F32),
    ]
    scratch = [held_scratch(held_qk), held_scratch(held_vo)]
    arrays = (*rows, *held_qk, *held_vo)
    return local_call(kernel, outs, scratch, where, arrays, 28)


def attention_back(rows, queries_keys, values, held_qk, held_vo, where):
    width = values.shape[1]
    count = values.shape[0]
    model = rows[0].shape[1]
    factor = temper / math.sqrt(HEAD_DIM)

    def kernel(where_ref, upper, lower, qk_ref, v_ref, near0, far0, near1, far1, *refs):
        dqk_ref, dv_ref, send_ref, keep_ref, mixed, w0, w1 = refs
        half = count // 2
        put_in_place(where_ref, (near1, far1), w1, 1)
        put_in_place(where_ref, (near0, far0), w0, 0)
        mixed[:half, :] = dot_nn(upper[...], w1[:, width:]).astype(BF)
        mixed[half:, :] = dot_nn(lower[...], w1[:, width:]).astype(BF)
        for at in range(0, width, HEAD_DIM):
            head = slice(at, at + HEAD_DIM)
            key_head = slice(width + at, width + at + HEAD_DIM)
            upstream = mixed[:, head]
            lifted, scale = attend_lifted(qk_ref[:, head], qk_ref[:, key_head])
            probs = lifted * scale
            dprobs = dot_nt(upstream, v_ref[:, head])
            inner = jnp.sum(probs * dprobs, axis=-1, keepdims=True)
            dscores = (probs * (dprobs - inner)).astype(BF)
            dqk_ref[:, head] = (dot_nn(dscores, qk_ref[:, key_head]) * factor).astype(BF)
            dqk_ref[:, key_head] = (dot_tn(dscores, qk_ref[:, head]) * factor).astype(BF)
            dv_ref[:, head] = dot_tn(probs.astype(BF), upstream).astype(BF)

        def part(span):
            return dot_nt(dqk_ref[span, :], w0[...]) + dot_nt(dv_ref[span, :], w1[:, :width])

        split_rows(count, send_ref, keep_ref, part)

    outs = [
        ((count, 2 * width), BF),
        ((count, width), BF),
        ((count // 2, model), BF),
        ((count // 2, model), F32),
    ]
    scratch = [pltpu.VMEM((count, width), BF), held_scratch(held_qk), held_scratch(held_vo)]
    arrays = (*rows, queries_keys, values, *held_qk, *held_vo)
    return local_call(kernel, outs, scratch, where, arrays, 28)


def gelu_pair(hidden):
    root, cube = math.sqrt(2.0 / math.pi), 0.044715
    square = hidden * hidden
    curve = jnp.tanh(root * (hidden + cube * (square * hidden)))
    rise = 0.5 * (1.0 + curve)
    slope = 0.5 * hidden * (1.0 - curve * curve) * (root * (1.0 + 3.0 * cube * square))
    return hidden * rise, rise + slope


def feed_forward(rows, down_rows, held_in, held_back, where):
    width = held_in[0].shape[1]
    count = 2 * rows[0].shape[0]
    model = rows[0].shape[1]
    strip = width // 4

    def kernel(where_ref, upper, lower, d_upper, d_lower, near0, far0, near1, far1, *refs):
        act_ref, up_ref, send_ref, keep_ref, w0, w1 = refs
        half = count // 2
        put_in_place(where_ref, (near0, far0), w0, 0, FFN_TURN)
        put_in_place(where_ref, (near1, far1), w1, 1, FFN_TURN)
        for k in range(4):
            part = slice(k * strip, (k + 1) * strip)
            for at, left, down in ((0, upper, d_upper), (half, lower, d_lower)):
                active, slope = gelu_pair(dot_nn(left[...], w0[:, part]))
                act_ref[at : at + half, part] = active.astype(BF)
                grad = slope * dot_nn(down[...], w1[:, part])
                up_ref[at : at + half, part] = grad.astype(BF)
        split_rows(count, send_ref, keep_ref, lambda span: dot_nt(up_ref[span, :], w0[...]))

    outs = [
        ((count, width), BF),
        ((count, width), BF),
        ((count // 2, model), BF),
        ((count // 2, model), F32),
    ]
    scratch = [held_scratch(held_in), held_scratch(held_back)]
    arrays = (*rows, *down_rows, *held_in, *held_back)
    return local_call(kernel, outs, scratch, where, arrays, 32)


def down_project(activated, held_back, where):
    count = activated.shape[0]
    model = 2 * held_back[0].shape[0]

    def kernel(where_ref, act_ref, near, far, send_ref, keep_ref, w1):
        put_in_place(where_ref, (near, far), w1, 1, FFN_TURN)
        split_rows(count, send_ref, keep_ref, lambda span: dot_nt(act_ref[span, :], w1[...]))

    outs = [((count // 2, model), BF), ((count // 2, model), F32)]
    scratch = [held_scratch(held_back)]
    arrays = (activated, *held_back)
    return local_call(kernel, outs, scratch, where, arrays, 20)


def pair_up(own):
    return ordered(own, swap(own, FSDP_X), FSDP_X)


def block_pass(tokens, layer_mod, w_qkv, w_out, w_in, w_back, out_grad, grad_scale):
    own_width, ffn_width = w_out.shape[0], w_in.shape[1]
    where = jnp.stack([lax.axis_index(ZY), lax.axis_index(SP_CORE)]).astype(jnp.int32)
    cut = 2 * own_width
    attn_pair = pair_up(jnp.concatenate([w_qkv, w_out.T], axis=1))
    ffn_own = jnp.concatenate([w_in, w_back.T], axis=1)
    ffn_given = after(swap(ffn_own, FSDP_X), attn_pair)
    ffn_pair = ordered(ffn_own, ffn_given, FSDP_X)

    stream = tokens.astype(F32)
    normed_first, rstd_first = normalize(stream)
    input_first = (normed_first * (1.0 + layer_mod[1]) + layer_mod[0]).astype(BF)

    attn_cuts = column_cuts((cut, 2 * own_width))
    ffn_cuts = column_cuts((ffn_width, ffn_width))
    ffn_held = [ffn_pair[:, part] for part in ffn_cuts]
    ffn_given = [hop(held, 0, k, FFN_TURN) for k, held in enumerate(ffn_held)]
    attn_held = join(attn_pair, hop(attn_pair, 0))
    attn_given = hop(attn_held, 1)
    ffn_given = after(ffn_given, attn_held)
    ffn_held = [join(*pair) for pair in zip(ffn_held, ffn_given)]
    ffn_given = [hop(held, 1, k, FFN_TURN) for k, held in enumerate(ffn_held)]
    input_first = after(input_first, attn_pair)
    attn_held = part_join(attn_held, attn_given, attn_cuts)
    attn_given = [hop(held, 2, k) for k, held in enumerate(attn_held)]
    attn_held = [join(*pair) for pair in zip(attn_held, attn_given)]
    first_rows = spread(input_first, attn_held)
    attn_far = [hop(held, 3, k) for k, held in enumerate(attn_held)]
    ffn_given = after(ffn_given, attn_far)
    ffn_held = [join(*pair) for pair in zip(ffn_held, ffn_given)]
    ffn_given = [hop(held, 2, k, FFN_TURN) for k, held in enumerate(ffn_held)]

    out_grad = after(out_grad, first_rows)
    stream_grad = out_grad.astype(F32)
    down_grad = (layer_mod[5] * stream_grad).astype(BF)
    down_rows = spread(down_grad)

    held_qk, held_vo = tuple(zip(attn_held, attn_far))
    queries_keys, values, attended, send, keep = attention(first_rows, held_qk, held_vo, where)
    send, mine = collect(keep, send)
    ffn_given = after(ffn_given, send)
    ffn_held = [join(*pair) for pair in zip(ffn_held, ffn_given)]
    ffn_far = [hop(held, 3, k, FFN_TURN) for k, held in enumerate(ffn_held)]
    given = swap(send, SP_X)
    middle = stream + layer_mod[2] * (mine + given.astype(F32))
    normed_second, rstd_second = normalize(middle)
    input_second = (normed_second * (1.0 + layer_mod[4]) + layer_mod[3]).astype(BF)
    second_rows = spread(input_second)
    ffn_far = after(ffn_far, second_rows)
    held_in, held_back = tuple(zip(ffn_held, ffn_far))

    activated, up_grad, send, keep = feed_forward(second_rows, down_rows, held_in, held_back, where)
    send, mine = collect(keep, send)
    up_rows = after(up_grad, send)
    near_in, far_in = term_blocks([(second_rows, up_rows)], where, 0, grad_scale, FFN_TURN)
    given_in = hop(far_in, 3, 0, FFN_TURN)
    act_rows = after(activated, far_in)
    near_back, far_back = term_blocks([(down_rows, act_rows)], where, 1, grad_scale, FFN_TURN)
    given_back = hop(far_back, 3, 1, FFN_TURN)
    back_second = mine + after(swap(send, SP_X), far_back).astype(F32)
    stream_grad = stream_grad + norm_back(
        normed_second, rstd_second, back_second * (1.0 + layer_mod[4])
    )
    attn_grad = (layer_mod[2] * stream_grad).astype(BF)
    out_send, out_keep = down_project(after(activated, attn_grad), held_back, where)
    attn_rows = spread(attn_grad, out_keep)
    grad_qk, grad_v, send, keep = attention_back(
        attn_rows, queries_keys, values, held_qk, held_vo, where
    )
    near_qk, far_qk = term_blocks([(first_rows, grad_qk)], where, 0, grad_scale, ATTN_TURN)
    given_qk = hop(far_qk, 3, 0, ATTN_TURN)
    grad_v, attended = after((grad_v, attended), far_qk)
    products = [(first_rows, grad_v), (attn_rows, attended)]
    near_vo, far_vo = term_blocks(products, where, 1, grad_scale, ATTN_TURN)
    given_vo = hop(far_vo, 3, 1, ATTN_TURN)

    def fold_on(twos, givens, names, step):
        turn = FFN_TURN if names == ffn_names else ATTN_TURN
        twos = [fold(two, given) for two, given in zip(twos, givens)]
        hops = [hop(two[1], step, k, turn) for k, two in enumerate(twos)]
        return [two[0] for two in twos], [two[1] for two in twos], hops

    ffn_names, attn_names = (G_IN, G_BACK), (G_QK, G_VO)
    givens = after((given_in, given_back), far_vo)
    near_ffn, sent_ffn, given_ffn = fold_on((near_in, near_back), givens, ffn_names, 2)
    send, mine = collect(keep, after(send, sent_ffn))
    given_first = swap(send, SP_X)
    out_send, out_mine = collect(out_keep, after(out_send, send))
    given_out = swap(out_send, SP_X)
    back_first = mine + after(given_first, out_send).astype(F32)
    input_grad = stream_grad + norm_back(
        normed_first, rstd_first, back_first * (1.0 + layer_mod[1])
    )
    givens = after((given_qk, given_vo), input_grad)
    near_attn, sent_attn, given_attn = fold_on((near_qk, near_vo), givens, attn_names, 2)
    near_ffn, sent_ffn, given_ffn = fold_on(near_ffn, after(given_ffn, sent_attn), ffn_names, 1)
    given_out = after(given_out, sent_ffn)
    final_out = (middle + layer_mod[5] * (out_mine + given_out.astype(F32))).astype(BF)
    givens = after(given_attn, final_out)
    near_attn, sent_attn, given_attn = fold_on(near_attn, givens, attn_names, 1)
    near_ffn, sent_ffn, given_ffn = fold_on(near_ffn, after(given_ffn, sent_attn), ffn_names, 0)
    givens = after(given_attn, sent_ffn)
    near_attn, sent_attn, given_attn = fold_on(near_attn, givens, attn_names, 0)

    def total(nears, givens):
        return jnp.concatenate([add(near, given) for near, given in zip(nears, givens)], axis=1)

    total_ffn = total(near_ffn, after(given_ffn, sent_attn))
    sum_ffn = last_sum(total_ffn)
    sum_attn = last_sum(total(near_attn, after(given_attn, total_ffn)))
    return (
        final_out,
        input_grad,
        sum_attn[:, : 3 * own_width],
        sum_attn[:, 3 * own_width :].T,
        sum_ffn[:, :ffn_width],
        sum_ffn[:, ffn_width:].T,
    )


def body(tokens, modulation, w_qkv, w_out, w_in, w_back, out_grad):
    local_seq = tokens.shape[1]
    own_width = w_qkv.shape[3]
    grad_scale = 1.0 / math.sqrt(local_seq * lax.axis_size(FSDP) * lax.axis_size(SP))
    final_out, input_grad, grad_qkv, grad_out, grad_in, grad_back = block_pass(
        tokens[0],
        modulation[0, 0],
        w_qkv[0].reshape(-1, 3 * own_width),
        w_out[0],
        w_in[0],
        w_back[0],
        out_grad[0],
        grad_scale,
    )
    return (
        final_out[None],
        input_grad[None],
        grad_qkv.reshape(1, -1, 3, own_width),
        grad_out[None],
        grad_in[None],
        grad_back[None],
    )


def solution(mesh):
    torus = Mesh(
        mesh.devices.reshape(4, 4, 2, 2, 2),
        (*FSDP, *SP),
    )
    return jax.shard_map(
        body,
        mesh=torus,
        in_specs=(
            P(FSDP, SP, None),
            P(FSDP, None, None, None),
            P(None, FSDP, None, SP),
            P(None, SP, FSDP),
            P(None, FSDP, SP),
            P(None, SP, FSDP),
            P(FSDP, SP, None),
        ),
        out_specs=(
            P(FSDP, SP, None),
            P(FSDP, SP, None),
            P(None, FSDP, None, SP),
            P(None, SP, FSDP),
            P(None, FSDP, SP),
            P(None, SP, FSDP),
        ),
        check_vma=False,
    )
```
